8 devices in a mesh: dp: 2 (over z, y), fsdp: 4 (over x, core).
Axes of the slice: x: 2, y: 2, z: 1, core: 2. Of those that a mesh axis runs over, the one named last changes fastest.
Arguments:
- g_layer: float32 [8, 6, 256, 3072], P(('dp', 'fsdp'))
- g_down: float32 [8, 256, 8192], P(('dp', 'fsdp'))
- g_norm: float32 [8, 4, 3072], P(('dp', 'fsdp'))
- g_embed: float32 [8, 256, 3072], P(('dp', 'fsdp'))
- layer_w: float32 [6, 256, 3072], P(None, 'fsdp')
- layer_m: float32 [6, 256, 3072], P(None, 'fsdp')
- layer_v: float32 [6, 256, 3072], P(None, 'fsdp')
- down_w: float32 [256, 8192], P('fsdp')
- down_m: float32 [256, 8192], P('fsdp')
- down_v: float32 [256, 8192], P('fsdp')
- norm_w: float32 [4, 3072], P(None, 'fsdp')
- norm_m: float32 [4, 3072], P(None, 'fsdp')
- norm_v: float32 [4, 3072], P(None, 'fsdp')
- embed_w: float32 [256, 3072], P('fsdp')
- embed_m: float32 [256, 3072], P('fsdp')
- embed_v: float32 [256, 3072], P('fsdp')
Outputs:
- output 1: float32 [6, 256, 3072], P(None, 'fsdp')
- output 2: float32 [6, 256, 3072], P(None, 'fsdp')
- output 3: float32 [6, 256, 3072], P(None, 'fsdp')
- output 4: bfloat16 [6, 256, 3072], P(None, 'fsdp')
- output 5: float32 [256, 8192], P('fsdp')
- output 6: float32 [256, 8192], P('fsdp')
- output 7: float32 [256, 8192], P('fsdp')
- output 8: bfloat16 [256, 8192], P('fsdp')
- output 9: float32 [4, 3072], P(None, 'fsdp')
- output 10: float32 [4, 3072], P(None, 'fsdp')
- output 11: float32 [4, 3072], P(None, 'fsdp')
- output 12: bfloat16 [4, 3072], P(None, 'fsdp')
- output 13: float32 [256, 3072], P('fsdp')
- output 14: float32 [256, 3072], P('fsdp')
- output 15: float32 [256, 3072], P('fsdp')
- output 16: bfloat16 [256, 3072], P('fsdp')
All inputs are finite; a program needn't handle non-finite values.
Results may differ from the reference program's by a relative error of at most 0.001.
Values sent between devices are 32-bit elements.
A program may use at most 1 GiB of HBM per device.

```python
import math
import jax
import jax.numpy as jnp

D = 3072
FF = 8192
LAYER_ROWS = 256
EMB_ROWS = 256
DEVICES = 8
OPT_STEP = 20

ADAM_BETA1 = 0.9
ADAM_BETA2 = 0.95
ADAM_EPS = 1e-8
LEARN_RATE = 4e-4
WEIGHT_DECAY = 0.1
CLIP_EPS = 1e-6
BIAS_ONE = 1.0 - ADAM_BETA1 ** OPT_STEP
BIAS_TWO = 1.0 - ADAM_BETA2 ** OPT_STEP
NORM_TARGET = 4.0


def draw_group(key_list, arr_shape, grad_share, init_std, init_mean):
    elem_count = math.prod(arr_shape)
    grad_scale = (grad_share * NORM_TARGET ** 2 * DEVICES / elem_count) ** 0.5
    unit_scale = (grad_share / elem_count) ** 0.5
    grad_all = grad_scale * jax.random.normal(key_list[0], (DEVICES,) + arr_shape, jnp.float32)
    master = init_mean + init_std * jax.random.normal(key_list[1], arr_shape, jnp.float32)
    exp_avg = 0.06 * unit_scale * jax.random.normal(key_list[2], arr_shape, jnp.float32)
    exp_avg_sq = 0.05 * unit_scale * unit_scale * jax.random.uniform(key_list[3], arr_shape, jnp.float32, 0.5, 1.5)
    return grad_all, master, exp_avg, exp_avg_sq


def setup_inputs(seed: int = 0) -> dict:
    key_list = jax.random.split(jax.random.key(seed), 16)
    layer_draw = draw_group(key_list[0:4], (6, LAYER_ROWS, D), 0.45, 0.02, 0.0)
    down_draw = draw_group(key_list[4:8], (LAYER_ROWS, FF), 0.2, 0.02, 0.0)
    norm_draw = draw_group(key_list[8:12], (4, D), 0.05, 0.1, 1.0)
    embed_draw = draw_group(key_list[12:16], (EMB_ROWS, D), 0.3, 0.02, 0.0)
    return {
        "g_layer": layer_draw[0], "g_down": down_draw[0], "g_norm": norm_draw[0], "g_embed": embed_draw[0],
        "layer_w": layer_draw[1], "layer_m": layer_draw[2], "layer_v": layer_draw[3],
        "down_w": down_draw[1], "down_m": down_draw[2], "down_v": down_draw[3],
        "norm_w": norm_draw[1], "norm_m": norm_draw[2], "norm_v": norm_draw[3],
        "embed_w": embed_draw[1], "embed_m": embed_draw[2], "embed_v": embed_draw[3],
    }


def adamw_step(grad_mean, master, exp_avg, exp_avg_sq, clip_coef, decay_rate):
    clipped = clip_coef * grad_mean
    avg_new = ADAM_BETA1 * exp_avg + (1.0 - ADAM_BETA1) * clipped
    sq_new = ADAM_BETA2 * exp_avg_sq + (1.0 - ADAM_BETA2) * clipped * clipped
    step_dir = (avg_new / BIAS_ONE) / (jnp.sqrt(sq_new / BIAS_TWO) + ADAM_EPS)
    master_new = master - LEARN_RATE * (step_dir + decay_rate * master)
    return master_new, avg_new, sq_new, master_new.astype(jnp.bfloat16)


def reference(g_layer, g_down, g_norm, g_embed, layer_w, layer_m, layer_v, down_w, down_m, down_v, norm_w, norm_m, norm_v, embed_w, embed_m, embed_v):
    layer_mean = jnp.sum(g_layer, axis=0) / DEVICES
    down_mean = jnp.sum(g_down, axis=0) / DEVICES
    norm_mean = jnp.sum(g_norm, axis=0) / DEVICES
    embed_mean = jnp.sum(g_embed, axis=0) / DEVICES
    sq_total = (jnp.sum(layer_mean * layer_mean) + jnp.sum(down_mean * down_mean)
                + jnp.sum(norm_mean * norm_mean) + jnp.sum(embed_mean * embed_mean))
    global_norm = jnp.sqrt(sq_total)
    clip_coef = jnp.minimum(1.0, 1.0 / (global_norm + CLIP_EPS))
    layer_new = adamw_step(layer_mean, layer_w, layer_m, layer_v, clip_coef, WEIGHT_DECAY)
    down_new = adamw_step(down_mean, down_w, down_m, down_v, clip_coef, WEIGHT_DECAY)
    norm_new = adamw_step(norm_mean, norm_w, norm_m, norm_v, clip_coef, WEIGHT_DECAY)
    embed_new = adamw_step(embed_mean, embed_w, embed_m, embed_v, clip_coef, 0.0)
    return (layer_new[0], layer_new[1], layer_new[2], layer_new[3],
            down_new[0], down_new[1], down_new[2], down_new[3],
            norm_new[0], norm_new[1], norm_new[2], norm_new[3],
            embed_new[0], embed_new[1], embed_new[2], embed_new[3])
```

```python
import functools

import jax
import jax.numpy as jnp
from jax import lax
from jax.experimental import pallas as pl
from jax.experimental.pallas import tpu as pltpu
from jax.sharding import PartitionSpec as P

ADAM_BETA1 = 0.9
ADAM_BETA2 = 0.95
ADAM_EPS = 1e-8
LEARN_RATE = 4e-4
WEIGHT_DECAY = 0.1
CLIP_EPS = 1e-6
OPT_STEP = 20
BIAS_ONE = 1.0 - ADAM_BETA1 ** OPT_STEP
BIAS_TWO = 1.0 - ADAM_BETA2 ** OPT_STEP

MESH = pl.DeviceIdType.MESH
F32 = jnp.float32

ROWS = 64
WIDTH = 3072
FF = 8192
HALF = FF // 2
NORM = (4, 768)
N_DOWN = 2 * (ROWS // 8)
N_SEVEN = 7 * (ROWS // 8)
N = N_DOWN + N_SEVEN

RING = 8
FETCH = 6
LEAD = 3
LAG = 3


def down_at(k):
    row = pl.multiple_of((k // 2) * 8, 8)
    col = pl.multiple_of((k % 2) * HALF, HALF)
    return row, col


def seven_at(k):
    q = k - N_DOWN
    return q // 8, pl.multiple_of((q % 8) * 8, 8)


def reduce_kernel(g_layer, g_down, g_norm, g_embed, layer_w, layer_m, layer_v, down_w, down_m, down_v,
                  norm_w, norm_m, norm_v, embed_w, embed_m, embed_v,
                  sq_out, g7, gd, gn, w7, m7, v7, wd, md, vd, wn, mn, vn,
                  own_o, par_o, pm7, pmd, x7, xd, y7, yd, own_no, par_no, pmn, xn, yn, acc, sq_all,
                  own_o_sem, own_m_sem, do_send, do_recv, dm_send, dm_recv, x_send, x_recv, y_send, y_recv,
                  st_sem, n_sem, n_send, n_recv, sq_send, sq_recv, credit):
    dp = lax.axis_index("dp")
    f = lax.axis_index("fsdp")
    core = lax.rem(f, 2)
    f_core = f + 1 - 2 * core
    f_x = lax.rem(f + 2, 4)
    f_diag = lax.rem(f_core + 2, 4)
    peer_core = (dp, f_core)
    peer_x = (dp, f_x)
    peer_diag = (dp, f_diag)
    peer_y = (1 - dp, f)

    def remote(src, dst, send, recv, peer):
        return pltpu.make_async_remote_copy(src_ref=src, dst_ref=dst, send_sem=send, recv_sem=recv,
                                            device_id=peer, device_id_type=MESH)

    barrier = pltpu.get_barrier_semaphore()
    for peer in (peer_core, peer_x, peer_diag, peer_y):
        pl.semaphore_signal(barrier, inc=1, device_id=peer, device_id_type=MESH)
    pl.semaphore_wait(barrier, 4)
    acc[...] = jnp.zeros_like(acc)

    def on_chunk(k, on_down, on_seven):
        @pl.when(jnp.logical_and(k >= 0, k < N_DOWN))
        def _():
            on_down()

        @pl.when(jnp.logical_and(k >= N_DOWN, k < N))
        def _():
            on_seven()

    def on_source(k, use):
        def on_down():
            row, col = down_at(k)
            use(lambda q: g_down.at[0, pl.ds(pl.multiple_of(q * ROWS + row, 8), 8), pl.ds(col, HALF)],
                lambda ring, s: ring.at[s],
                lambda seven, down: down.at[pl.ds(row, 8), pl.ds(col, HALF)])

        def on_seven():
            j, row = seven_at(k)

            def view(seven, down):
                return seven.at[j, pl.ds(row, 8), :]

            def ring_view(ring, s):
                return ring.at[s, :, pl.ds(0, WIDTH)]

            @pl.when(j < 6)
            def _():
                use(lambda q: g_layer.at[0, j, pl.ds(pl.multiple_of(q * ROWS + row, 8), 8), :], ring_view, view)

            @pl.when(j == 6)
            def _():
                use(lambda q: g_embed.at[0, pl.ds(pl.multiple_of(q * ROWS + row, 8), 8), :], ring_view, view)

        on_chunk(k, on_down, on_seven)

    def on_view(k, use):
        def on_down():
            row, col = down_at(k)
            use(lambda ring, s: ring.at[s], lambda seven, down: down.at[pl.ds(row, 8), pl.ds(col, HALF)], HALF)

        def on_seven():
            j, row = seven_at(k)
            use(lambda ring, s: ring.at[s, :, pl.ds(0, WIDTH)], lambda seven, down: seven.at[j, pl.ds(row, 8), :],
                WIDTH)

        on_chunk(k, on_down, on_seven)

    def x_copy(k, ring_view, view):
        s = lax.rem(k, RING)
        return remote(ring_view(own_o, s), view(x7, xd), x_send.at[s], x_recv.at[k], peer_x)

    def y_copy(k, view):
        s = lax.rem(k, RING)
        return remote(view(g7, gd), view(y7, yd), y_send.at[s], y_recv.at[k], peer_y)

    def push_other(k, source, ring_view):
        s = lax.rem(k, RING)
        return remote(source(f_diag), ring_view(par_o, s), do_send.at[s], do_recv.at[s], peer_core)

    def push_mine(k, source, view):
        s = lax.rem(k, RING)
        return remote(source(f_core), view(pm7, pmd), dm_send.at[s], dm_recv.at[k], peer_core)

    def fetch(k):
        s = lax.rem(k, RING)

        @pl.when(jnp.logical_and(k >= RING, k < N))
        def _():
            def retire(ring_view, view, width):
                x_copy(k - RING, ring_view, view).wait_send()
                push = remote(ring_view(par_o, s), ring_view(par_o, s), do_send.at[s], do_recv.at[s], peer_core)
                push.wait_send()
                push = remote(view(pm7, pmd), view(pm7, pmd), dm_send.at[s], dm_recv.at[k], peer_core)
                push.wait_send()

            on_view(k - RING, retire)
            pl.semaphore_wait(credit, 1)

        def start(source, ring_view, view):
            push_other(k, source, ring_view).start()
            pltpu.make_async_copy(source(f_x), ring_view(own_o, s), own_o_sem.at[s]).start()
            push_mine(k, source, view).start()
            pltpu.make_async_copy(source(f), view(g7, gd), own_m_sem.at[s]).start()

        on_source(k, start)

    def sum_x(k):
        s = lax.rem(k, RING)

        def use(ring_view, view, width):
            mine = view(g7, gd)
            pltpu.make_async_copy(mine, mine, own_m_sem.at[s]).wait()
            push = remote(view(pm7, pmd), view(pm7, pmd), dm_send.at[s], dm_recv.at[k], peer_core)
            push.wait_recv()
            x_copy(k, ring_view, view).wait_recv()
            mine[...] = (mine[...] + view(pm7, pmd)[...]) + view(x7, xd)[...]

        on_view(k, use)

    def sum_chip(k):
        s = lax.rem(k, RING)

        def use(ring_view, view, width):
            mine = ring_view(own_o, s)
            pltpu.make_async_copy(mine, mine, own_o_sem.at[s]).wait()
            push = remote(ring_view(par_o, s), ring_view(par_o, s), do_send.at[s], do_recv.at[s], peer_core)
            push.wait_recv()
            mine[...] = mine[...] + ring_view(par_o, s)[...]

        on_view(k, use)

    def start_y(k):
        on_view(k, lambda ring_view, view, width: y_copy(k, view).start())

    def start_x(k):
        on_view(k, lambda ring_view, view, width: x_copy(k, ring_view, view).start())

        @pl.when(jnp.logical_and(k >= 0, k < N - RING))
        def _():
            pl.semaphore_signal(credit, inc=1, device_id=peer_core, device_id_type=MESH)

    def state_down(k):
        row, col = down_at(k)
        s = lax.rem(k, RING)
        return [pltpu.make_async_copy(src.at[pl.ds(row, 8), pl.ds(col, HALF)], dst.at[pl.ds(row, 8), pl.ds(col, HALF)],
                                      st_sem.at[i, s])
                for i, (src, dst) in enumerate(((down_w, wd), (down_m, md), (down_v, vd)))]

    def state_layer(k):
        j, row = seven_at(k)
        s = lax.rem(k, RING)
        return [pltpu.make_async_copy(src.at[j, pl.ds(row, 8), :], dst.at[j, pl.ds(row, 8), :], st_sem.at[i, s])
                for i, (src, dst) in enumerate(((layer_w, w7), (layer_m, m7), (layer_v, v7)))]

    def state_embed(k):
        j, row = seven_at(k)
        s = lax.rem(k, RING)
        return [pltpu.make_async_copy(src.at[pl.ds(row, 8), :], dst.at[6, pl.ds(row, 8), :], st_sem.at[i, s])
                for i, (src, dst) in enumerate(((embed_w, w7), (embed_m, m7), (embed_v, v7)))]

    def start_state(k):
        def on_seven():
            j, _ = seven_at(k)

            @pl.when(j < 6)
            def _():
                for copy in state_layer(k):
                    copy.start()

            @pl.when(j == 6)
            def _():
                for copy in state_embed(k):
                    copy.start()

        def on_down():
            for copy in state_down(k):
                copy.start()

        on_chunk(k, on_down, on_seven)

    def sum_y(k):
        s = lax.rem(k, RING)

        def use(ring_view, view, width):
            y_copy(k, view).wait()
            for i, ref in enumerate(((w7, wd), (m7, md), (v7, vd))):
                pltpu.make_async_copy(view(*ref), view(*ref), st_sem.at[i, s]).wait()
            mean = (view(g7, gd)[...] + view(y7, yd)[...]) * 0.125
            view(g7, gd)[...] = mean
            parts = [mean[:, i * 128:(i + 1) * 128] for i in range(width // 128)]
            sums = [p * p for p in parts[:4]]
            for i, p in enumerate(parts[4:]):
                sums[i % 4] = sums[i % 4] + p * p
            acc[...] += (sums[0] + sums[1]) + (sums[2] + sums[3])

        on_view(k, use)

    def norm_source(q):
        return g_norm.at[0, :, pl.ds(pl.multiple_of(q * NORM[1], 128), NORM[1])]

    n_push_other = remote(norm_source(f_diag), par_no, n_send.at[0], n_recv.at[0], peer_core)
    n_push_mine = remote(norm_source(f_core), pmn, n_send.at[1], n_recv.at[1], peer_core)
    n_x = remote(own_no, xn, n_send.at[2], n_recv.at[2], peer_x)
    n_y = remote(gn, yn, n_send.at[3], n_recv.at[3], peer_y)
    n_local = [pltpu.make_async_copy(src, dst, n_sem.at[i]) for i, (src, dst) in enumerate(
        ((norm_source(f_x), own_no), (norm_source(f), gn), (norm_w, wn), (norm_m, mn), (norm_v, vn)))]

    def step(t, _):
        i = t - FETCH
        fetch(i + FETCH)

        @pl.when(i == 0)
        def _():
            n_push_other.start()
            n_push_mine.start()
            for copy in n_local:
                copy.start()

        sum_x(i)
        sum_chip(i + LEAD)
        start_y(i)
        start_x(i + LEAD)
        start_state(i)

        @pl.when(i == 4)
        def _():
            for copy in n_local:
                copy.wait()
            n_push_other.wait()
            n_push_mine.wait()
            own_no[...] = own_no[...] + par_no[...]
            n_x.start()

        @pl.when(i == 10)
        def _():
            n_x.wait()
            gn[...] = (gn[...] + pmn[...]) + xn[...]
            n_y.start()

        @pl.when(i == 16)
        def _():
            n_y.wait()
            mean = (gn[...] + yn[...]) * 0.125
            gn[...] = mean
            square = mean * mean
            total = square[:, 0:128]
            for c in range(1, NORM[1] // 128):
                total = total + square[:, c * 128:(c + 1) * 128]
            acc[0:4, :] += total

        sum_y(i - LAG)
        return 0

    lax.fori_loop(0, FETCH + N + LAG, step, 0)

    sq_all[f] = acc[...]
    copies = [remote(sq_all.at[f], sq_all.at[f], sq_send.at[i], sq_recv.at[i], peer)
              for i, peer in enumerate((peer_core, peer_x, peer_diag))]
    for copy in copies:
        copy.start()

    def drain(k, _):
        s = lax.rem(k, RING)

        def use(ring_view, view, width):
            x_copy(k, ring_view, view).wait_send()
            remote(ring_view(par_o, s), ring_view(par_o, s), do_send.at[s], do_recv.at[s], peer_core).wait_send()
            remote(view(pm7, pmd), view(pm7, pmd), dm_send.at[s], dm_recv.at[k], peer_core).wait_send()

        on_view(k, use)
        return 0

    lax.fori_loop(N - RING, N, drain, 0)
    for copy in copies:
        copy.wait()
    sq_out[...] = (sq_all[0] + sq_all[1]) + (sq_all[2] + sq_all[3])


def update_math(clip, g, w, m, v, decay):
    clipped = clip * g
    avg = ADAM_BETA1 * m + (1.0 - ADAM_BETA1) * clipped
    sq = ADAM_BETA2 * v + (1.0 - ADAM_BETA2) * clipped * clipped
    step_dir = (avg / BIAS_ONE) / (jnp.sqrt(sq / BIAS_TWO) + ADAM_EPS)
    new = w - LEARN_RATE * (step_dir + decay * w)
    return new, avg, sq, new.astype(jnp.bfloat16)


def update_kernel(sq, g7, gd, gn, w7, m7, v7, wd, md, vd, wn, mn, vn,
                  lw, lm, lv, lb, dw, dm, dv, db, nw, nm, nv, nb, ew, em, ev, eb,
                  s7w, s7m, s7v, s7b, sdw, sdm, sdv, sdb, snw, snm, snv, snb, sem7, semd, semn):
    total = jnp.sum(sq[...], keepdims=True)
    clip = jnp.minimum(1.0, 1.0 / (jnp.sqrt(total) + CLIP_EPS))

    def seven_copies(j, row, outs):
        i = row // 16
        return [pltpu.make_async_copy(src.at[j, pl.ds(row, 16), :], dst, sem7.at[a, j, i])
                for a, (src, dst) in enumerate(zip((s7w, s7m, s7v, s7b), outs))]

    def layer_copies(j, row):
        return seven_copies(j, row, [o.at[j, pl.ds(row, 16), :] for o in (lw, lm, lv, lb)])

    def embed_copies(row):
        return seven_copies(6, row, [o.at[pl.ds(row, 16), :] for o in (ew, em, ev, eb)])

    def seven(j, decay, row):
        at = (j, pl.ds(row, 16))
        for c in range(0, WIDTH, 512):
            ix = at + (pl.ds(c, 512),)
            out = update_math(clip, g7[ix], w7[ix], m7[ix], v7[ix], decay)
            for ref, val in zip((s7w, s7m, s7v, s7b), out):
                ref[ix] = val

    def layer_step(t, _):
        j = t // 4
        row = pl.multiple_of((t % 4) * 16, 16)
        seven(j, WEIGHT_DECAY, row)
        for copy in layer_copies(j, row):
            copy.start()
        return 0

    def embed_step(t, _):
        row = pl.multiple_of(t * 16, 16)
        seven(6, 0.0, row)
        for copy in embed_copies(row):
            copy.start()
        return 0

    def down_copies(t):
        row = pl.multiple_of((t // 2) * 16, 16)
        col = pl.multiple_of((t % 2) * HALF, HALF)
        ix = (pl.ds(row, 16), pl.ds(col, HALF))
        return [pltpu.make_async_copy(src.at[ix], dst.at[ix], semd.at[a, t])
                for a, (src, dst) in enumerate(zip((sdw, sdm, sdv, sdb), (dw, dm, dv, db)))]

    def down_step(t, _):
        row = pl.multiple_of((t // 2) * 16, 16)
        col = pl.multiple_of((t % 2) * HALF, HALF)
        for c in range(0, HALF, 512):
            ix = (pl.ds(row, 16), pl.ds(pl.multiple_of(col + c, 512), 512))
            out = update_math(clip, gd[ix], wd[ix], md[ix], vd[ix], WEIGHT_DECAY)
            for ref, val in zip((sdw, sdm, sdv, sdb), out):
                ref[ix] = val
        for copy in down_copies(t):
            copy.start()
        return 0

    lax.fori_loop(0, 8, down_step, 0)
    out = update_math(clip, gn[...], wn[...], mn[...], vn[...], WEIGHT_DECAY)
    for ref, val in zip((snw, snm, snv, snb), out):
        ref[...] = val
    norm_copies = [pltpu.make_async_copy(src, dst, semn.at[a])
                   for a, (src, dst) in enumerate(zip((snw, snm, snv, snb), (nw, nm, nv, nb)))]
    for copy in norm_copies:
        copy.start()
    lax.fori_loop(0, 24, layer_step, 0)
    lax.fori_loop(0, 4, embed_step, 0)

    def layer_wait(t, _):
        for copy in layer_copies(t // 4, pl.multiple_of((t % 4) * 16, 16)):
            copy.wait()
        return 0

    def embed_wait(t, _):
        for copy in embed_copies(pl.multiple_of(t * 16, 16)):
            copy.wait()
        return 0

    def down_wait(t, _):
        for copy in down_copies(t):
            copy.wait()
        return 0

    lax.fori_loop(0, 8, down_wait, 0)
    for copy in norm_copies:
        copy.wait()
    lax.fori_loop(0, 24, layer_wait, 0)
    lax.fori_loop(0, 4, embed_wait, 0)


SEVEN = (7, ROWS, WIDTH)
DOWN = (ROWS, FF)


def local_update(g_layer, g_down, g_norm, g_embed, layer_w, layer_m, layer_v, down_w, down_m, down_v, norm_w, norm_m,
                 norm_v, embed_w, embed_m, embed_v):
    any_spec = pl.BlockSpec(memory_space=pl.ANY)
    vmem_spec = pl.BlockSpec(memory_space=pltpu.VMEM)
    dma = pltpu.SemaphoreType.DMA
    held = [(8, 128)] + [SEVEN, DOWN, NORM] + [SEVEN] * 3 + [DOWN] * 3 + [NORM] * 3
    reduced = pl.pallas_call(
        reduce_kernel,
        out_shape=[pltpu.VMEM(shape, F32) for shape in held],
        in_specs=[any_spec] * 16,
        out_specs=[vmem_spec] * len(held),
        scratch_shapes=[pltpu.VMEM((RING, 8, HALF), F32), pltpu.VMEM((RING, 8, HALF), F32)]
        + [pltpu.VMEM(SEVEN, F32), pltpu.VMEM(DOWN, F32)] * 3
        + [pltpu.VMEM(NORM, F32)] * 5
        + [pltpu.VMEM((8, 128), F32), pltpu.VMEM((4, 8, 128), F32)]
        + [dma((RING,)), dma((RING,)), dma((RING,)), dma((RING,)), dma((RING,)), dma((N,)), dma((RING,)), dma((N,)),
           dma((RING,)), dma((N,)), dma((3, RING)), dma((5,)), dma((4,)), dma((4,)), dma((3,)), dma((3,)),
           pltpu.SemaphoreType.REGULAR],
        compiler_params=pltpu.CompilerParams(collective_id=0, has_side_effects=True,
                                             vmem_limit_bytes=26 * 1024 * 1024),
    )(g_layer, g_down, g_norm, g_embed, layer_w, layer_m, layer_v, down_w, down_m, down_v, norm_w, norm_m, norm_v,
      embed_w, embed_m, embed_v)
    groups = ((6, ROWS, WIDTH), DOWN, NORM, (ROWS, WIDTH))
    out_shape = [jax.ShapeDtypeStruct(s, d) for s in groups for d in (F32, F32, F32, jnp.bfloat16)]
    staged = [pltpu.VMEM(s, d) for s in (SEVEN, DOWN, NORM) for d in (F32, F32, F32, jnp.bfloat16)]
    return pl.pallas_call(
        update_kernel,
        out_shape=out_shape,
        in_specs=[vmem_spec] * len(held),
        out_specs=[any_spec] * 16,
        scratch_shapes=staged + [dma((4, 7, 4)), dma((4, 8)), dma((4,))],
        compiler_params=pltpu.CompilerParams(vmem_limit_bytes=26 * 1024 * 1024),
    )(*[pltpu.with_memory_space_constraint(a, pltpu.VMEM) for a in reduced])


def solution(mesh):
    grad_four = P(("dp", "fsdp"), None, None, None)
    grad_three = P(("dp", "fsdp"), None, None)
    layer_spec = P(None, "fsdp", None)
    down_spec = P("fsdp", None)
    norm_spec = P(None, "fsdp")
    embed_spec = P("fsdp", None)
    in_specs = (grad_four, grad_three, grad_three, grad_three,
                layer_spec, layer_spec, layer_spec, down_spec, down_spec, down_spec,
                norm_spec, norm_spec, norm_spec, embed_spec, embed_spec, embed_spec)
    out_specs = (layer_spec,) * 4 + (down_spec,) * 4 + (norm_spec,) * 4 + (embed_spec,) * 4
    return jax.shard_map(local_update, mesh=mesh, in_specs=in_specs, out_specs=out_specs, check_vma=False)
```

```python
import math

import jax
import jax.numpy as jnp
from jax import lax
from jax.experimental import pallas as pl
from jax.experimental.pallas import tpu as pltpu
from jax.sharding import PartitionSpec as P

ADAM_BETA1 = 0.9
ADAM_BETA2 = 0.95
ADAM_EPS = 1e-8
LEARN_RATE = 4e-4
WEIGHT_DECAY = 0.1
CLIP_EPS = 1e-6
OPT_STEP = 20
BIAS_ONE = 1.0 - ADAM_BETA1 ** OPT_STEP
BIAS_TWO = 1.0 - ADAM_BETA2 ** OPT_STEP
ROOT_TWO = math.sqrt(BIAS_TWO)
SMALLEST = 1.1754944e-38

MESH = pl.DeviceIdType.MESH
F32 = jnp.float32

ROWS = 64
WIDTH = 3072
FF = 8192
PIECE = 2048
NORM = (4, 768)
SEVEN = (7, ROWS, WIDTH)
DOWN = (ROWS, FF)

FIRST = 16
N_SEVEN = 7 * (ROWS // 8) - FIRST // 8
N_DOWN = (FF // PIECE) * (ROWS // 8)
N = N_SEVEN + N_DOWN

RING = 12
FETCH = 8
LEAD = 4
LAG = 4


def seven_at(k):
    return k // 8, pl.multiple_of((k % 8) * 8, 8)


def down_at(k):
    q = k - N_SEVEN
    row = pl.multiple_of((q // 4) * 8, 8)
    col = pl.multiple_of((q % 4) * PIECE, PIECE)
    return row, col


def squares(mean, width):
    parts = [mean[:, i * 128:(i + 1) * 128] for i in range(width // 128)]
    sums = [p * p for p in parts[:4]]
    for i, p in enumerate(parts[4:]):
        sums[i % 4] = sums[i % 4] + p * p
    return (sums[0] + sums[1]) + (sums[2] + sums[3])


def reduce_kernel(g_layer, g_down, g_norm, g_embed, layer_w, layer_m, layer_v, down_w, down_m, down_v,
                  norm_w, norm_m, norm_v, embed_w, embed_m, embed_v,
                  sq_out, g7, gd, gn, w7, m7, v7, wd, md, vd, wn, mn, vn,
                  own_o, par_o, pm7, pmd, x7, xd, y7, yd, own_no, par_no, pmn, xn, yn, acc, sq_all, sq_first,
                  fo_own, fo_par, fm_own, fm_par, f_y, f_x_in, f_out, f_in,
                  own_o_sem, own_m_sem, do_send, do_recv, dm_send, dm_recv, x_send, x_recv, y_send, y_recv,
                  st_sem, n_sem, n_send, n_recv, sq_send, sq_recv, sqf_send, sqf_recv, f_sem, f_send, f_recv, credit):
    dp = lax.axis_index("dp")
    f = lax.axis_index("fsdp")
    core = lax.rem(f, 2)
    f_core = f + 1 - 2 * core
    f_x = lax.rem(f + 2, 4)
    f_diag = lax.rem(f_core + 2, 4)
    peer_core = (dp, f_core)
    peer_x = (dp, f_x)
    peer_diag = (dp, f_diag)
    peer_y = (1 - dp, f)
    peers = (peer_core, peer_x, peer_diag, peer_y, (1 - dp, f_core), (1 - dp, f_x), (1 - dp, f_diag))

    def remote(src, dst, send, recv, peer):
        return pltpu.make_async_remote_copy(src_ref=src, dst_ref=dst, send_sem=send, recv_sem=recv,
                                            device_id=peer, device_id_type=MESH)

    barrier = pltpu.get_barrier_semaphore()
    for peer in peers:
        pl.semaphore_signal(barrier, inc=1, device_id=peer, device_id_type=MESH)
    pl.semaphore_wait(barrier, len(peers))
    acc[...] = jnp.zeros_like(acc)

    def on_chunk(k, on_down, on_seven):
        @pl.when(jnp.logical_and(k >= 0, k < N_SEVEN))
        def _():
            on_seven()

        @pl.when(jnp.logical_and(k >= N_SEVEN, k < N))
        def _():
            on_down()

    def on_source(k, use):
        def on_down():
            row, col = down_at(k)
            use(lambda q: g_down.at[0, pl.ds(pl.multiple_of(q * ROWS + row, 8), 8), pl.ds(col, PIECE)],
                lambda ring, s: ring.at[s, :, pl.ds(0, PIECE)],
                lambda seven, down: down.at[pl.ds(row, 8), pl.ds(col, PIECE)])

        def on_seven():
            j, row = seven_at(k)

            def view(seven, down):
                return seven.at[j, pl.ds(row, 8), :]

            def ring_view(ring, s):
                return ring.at[s]

            @pl.when(j < 6)
            def _():
                use(lambda q: g_layer.at[0, j, pl.ds(pl.multiple_of(q * ROWS + row, 8), 8), :], ring_view, view)

            @pl.when(j == 6)
            def _():
                use(lambda q: g_embed.at[0, pl.ds(pl.multiple_of(q * ROWS + row, 8), 8), :], ring_view, view)

        on_chunk(k, on_down, on_seven)

    def on_view(k, use):
        def on_down():
            row, col = down_at(k)
            use(lambda ring, s: ring.at[s, :, pl.ds(0, PIECE)],
                lambda seven, down: down.at[pl.ds(row, 8), pl.ds(col, PIECE)], PIECE)

        def on_seven():
            j, row = seven_at(k)
            use(lambda ring, s: ring.at[s], lambda seven, down: seven.at[j, pl.ds(row, 8), :], WIDTH)

        on_chunk(k, on_down, on_seven)

    def x_copy(k, ring_view, view):
        s = lax.rem(k, RING)
        return remote(ring_view(own_o, s), view(x7, xd), x_send.at[s], x_recv.at[k], peer_x)

    def y_copy(k, view):
        s = lax.rem(k, RING)
        return remote(view(g7, gd), view(y7, yd), y_send.at[s], y_recv.at[k], peer_y)

    def push_other(k, source, ring_view):
        s = lax.rem(k, RING)
        return remote(source(f_diag), ring_view(par_o, s), do_send.at[s], do_recv.at[s], peer_core)

    def push_mine(k, source, view):
        s = lax.rem(k, RING)
        return remote(source(f_core), view(pm7, pmd), dm_send.at[s], dm_recv.at[k], peer_core)

    def fetch(k):
        s = lax.rem(k, RING)

        @pl.when(jnp.logical_and(k >= RING, k < N))
        def _():
            def retire(ring_view, view, width):
                x_copy(k - RING, ring_view, view).wait_send()
                push = remote(ring_view(par_o, s), ring_view(par_o, s), do_send.at[s], do_recv.at[s], peer_core)
                push.wait_send()
                push = remote(view(pm7, pmd), view(pm7, pmd), dm_send.at[s], dm_recv.at[k], peer_core)
                push.wait_send()

            on_view(k - RING, retire)
            pl.semaphore_wait(credit, 1)

        def start(source, ring_view, view):
            push_other(k, source, ring_view).start()
            pltpu.make_async_copy(source(f_x), ring_view(own_o, s), own_o_sem.at[s]).start()
            push_mine(k, source, view).start()
            pltpu.make_async_copy(source(f), view(g7, gd), own_m_sem.at[s]).start()

        on_source(k, start)

    def sum_x(k):
        s = lax.rem(k, RING)

        def use(ring_view, view, width):
            mine = view(g7, gd)
            pltpu.make_async_copy(mine, mine, own_m_sem.at[s]).wait()
            push = remote(view(pm7, pmd), view(pm7, pmd), dm_send.at[s], dm_recv.at[k], peer_core)
            push.wait_recv()
            x_copy(k, ring_view, view).wait_recv()
            mine[...] = (mine[...] + view(pm7, pmd)[...]) + view(x7, xd)[...]

        on_view(k, use)

    def sum_chip(k):
        s = lax.rem(k, RING)

        def use(ring_view, view, width):
            mine = ring_view(own_o, s)
            pltpu.make_async_copy(mine, mine, own_o_sem.at[s]).wait()
            push = remote(ring_view(par_o, s), ring_view(par_o, s), do_send.at[s], do_recv.at[s], peer_core)
            push.wait_recv()
            mine[...] = mine[...] + ring_view(par_o, s)[...]

        on_view(k, use)

    def start_y(k):
        on_view(k, lambda ring_view, view, width: y_copy(k, view).start())

    def start_x(k):
        on_view(k, lambda ring_view, view, width: x_copy(k, ring_view, view).start())

        @pl.when(jnp.logical_and(k >= 0, k < N - RING))
        def _():
            pl.semaphore_signal(credit, inc=1, device_id=peer_core, device_id_type=MESH)

    def state_down(k):
        row, col = down_at(k)
        s = lax.rem(k, RING)
        return [pltpu.make_async_copy(src.at[pl.ds(row, 8), pl.ds(col, PIECE)], dst.at[pl.ds(row, 8), pl.ds(col, PIECE)],
                                      st_sem.at[i, s])
                for i, (src, dst) in enumerate(((down_w, wd), (down_m, md), (down_v, vd)))]

    def state_layer(k):
        j, row = seven_at(k)
        s = lax.rem(k, RING)
        return [pltpu.make_async_copy(src.at[j, pl.ds(row, 8), :], dst.at[j, pl.ds(row, 8), :], st_sem.at[i, s])
                for i, (src, dst) in enumerate(((layer_w, w7), (layer_m, m7), (layer_v, v7)))]

    def state_embed(k):
        j, row = seven_at(k)
        s = lax.rem(k, RING)
        return [pltpu.make_async_copy(src.at[pl.ds(row, 8), :], dst.at[6, pl.ds(row, 8), :], st_sem.at[i, s])
                for i, (src, dst) in enumerate(((embed_w, w7), (embed_m, m7), (embed_v, v7)))]

    def start_state(k):
        def on_seven():
            j, _ = seven_at(k)

            @pl.when(j < 6)
            def _():
                for copy in state_layer(k):
                    copy.start()

            @pl.when(j == 6)
            def _():
                for copy in state_embed(k):
                    copy.start()

        def on_down():
            for copy in state_down(k):
                copy.start()

        on_chunk(k, on_down, on_seven)

    def sum_y(k):
        s = lax.rem(k, RING)

        def use(ring_view, view, width):
            y_copy(k, view).wait()
            for i, ref in enumerate(((w7, wd), (m7, md), (v7, vd))):
                pltpu.make_async_copy(view(*ref), view(*ref), st_sem.at[i, s]).wait()
            mean = (view(g7, gd)[...] + view(y7, yd)[...]) * 0.125
            view(g7, gd)[...] = mean
            acc[...] += squares(mean, width)

        on_view(k, use)

    def embed_rows(q):
        return g_embed.at[0, pl.ds(pl.multiple_of(q * ROWS + (ROWS - FIRST), 8), FIRST), :]

    f_push = [remote(embed_rows(f_diag), fo_par, f_send.at[0], f_recv.at[0], peer_core),
              remote(embed_rows(f_core), fm_par, f_send.at[1], f_recv.at[1], peer_core)]
    f_local = [pltpu.make_async_copy(src, dst, f_sem.at[i]) for i, (src, dst) in enumerate(
        ((embed_rows(f_x), fo_own), (embed_rows(f), fm_own)))]
    last = pl.ds(ROWS - FIRST, FIRST)
    f_state = [pltpu.make_async_copy(src.at[last, :], dst.at[6, last, :], f_sem.at[2 + i])
               for i, (src, dst) in enumerate(((embed_w, w7), (embed_m, m7), (embed_v, v7)))]
    keep = pl.ds(pl.multiple_of(dp * 8, 8), 8)
    give = pl.ds(pl.multiple_of((1 - dp) * 8, 8), 8)
    keep_out = pl.ds(pl.multiple_of(ROWS - FIRST + dp * 8, 8), 8)
    give_out = pl.ds(pl.multiple_of(ROWS - FIRST + (1 - dp) * 8, 8), 8)
    f_scatter = [remote(fo_own.at[give, :], f_y.at[0], f_send.at[2], f_recv.at[2], peer_y),
                 remote(fm_own.at[give, :], f_y.at[1], f_send.at[3], f_recv.at[3], peer_y)]
    f_cross = remote(fo_own.at[keep, :], f_x_in, f_send.at[4], f_recv.at[4], peer_x)
    f_gather = remote(f_out, f_in, f_send.at[5], f_recv.at[5], peer_y)
    me = dp * 4 + f
    sqf_copies = [remote(sq_first.at[me], sq_first.at[me], sqf_send.at[i], sqf_recv.at[i], peer)
                  for i, peer in enumerate(peers)]

    def norm_source(q):
        return g_norm.at[0, :, pl.ds(pl.multiple_of(q * NORM[1], 128), NORM[1])]

    n_push_other = remote(norm_source(f_diag), par_no, n_send.at[0], n_recv.at[0], peer_core)
    n_push_mine = remote(norm_source(f_core), pmn, n_send.at[1], n_recv.at[1], peer_core)
    n_x = remote(own_no, xn, n_send.at[2], n_recv.at[2], peer_x)
    n_y = remote(gn, yn, n_send.at[3], n_recv.at[3], peer_y)
    n_local = [pltpu.make_async_copy(src, dst, n_sem.at[i]) for i, (src, dst) in enumerate(
        ((norm_source(f_x), own_no), (norm_source(f), gn), (norm_w, wn), (norm_m, mn), (norm_v, vn)))]

    def step(t, _):
        i = t - FETCH
        fetch(i + FETCH)

        @pl.when(i == -FETCH)
        def _():
            for copy in f_push:
                copy.start()
            for copy in f_local:
                copy.start()

        @pl.when(i == -LEAD - 1)
        def _():
            n_push_other.start()
            n_push_mine.start()
            for copy in n_local:
                copy.start()

        sum_x(i)
        sum_chip(i + LEAD)
        start_y(i)
        start_x(i + LEAD)
        start_state(i)

        @pl.when(i == 1 - LEAD)
        def _():
            for copy in f_local:
                copy.wait()
            for copy in f_push:
                copy.wait()
            fo_own[...] = fo_own[...] + fo_par[...]
            fm_own[...] = fm_own[...] + fm_par[...]
            for copy in f_scatter:
                copy.start()
            for copy in f_state:
                copy.start()

        @pl.when(i == 2)
        def _():
            for copy in n_local:
                copy.wait()
            n_push_other.wait()
            n_push_mine.wait()
            own_no[...] = own_no[...] + par_no[...]
            n_x.start()

        @pl.when(i == 10)
        def _():
            n_x.wait()
            gn[...] = (gn[...] + pmn[...]) + xn[...]
            n_y.start()
            for copy in f_scatter:
                copy.wait()
            fo_own[keep, :] = fo_own[keep, :] + f_y[0]
            fm_own[keep, :] = fm_own[keep, :] + f_y[1]

        @pl.when(i == 20)
        def _():
            n_y.wait()
            mean = (gn[...] + yn[...]) * 0.125
            gn[...] = mean
            square = mean * mean
            total = square[:, 0:128]
            for c in range(1, NORM[1] // 128):
                total = total + square[:, c * 128:(c + 1) * 128]
            acc[0:4, :] += total

        @pl.when(i == N - LEAD)
        def _():
            f_cross.start()

        @pl.when(i == N + LAG - 2)
        def _():
            f_cross.wait()
            mean = (fm_own[keep, :] + f_x_in[...]) * 0.125
            f_out[...] = mean
            g7[6, keep_out, :] = mean
            sq_first[me] = squares(mean, WIDTH)
            f_gather.start()
            for copy in sqf_copies:
                copy.start()

        sum_y(i - LAG)
        return 0

    lax.fori_loop(0, FETCH + N + LAG, step, 0)

    sq_all[f] = acc[...]
    copies = [remote(sq_all.at[f], sq_all.at[f], sq_send.at[i], sq_recv.at[i], peer)
              for i, peer in enumerate((peer_core, peer_x, peer_diag))]
    for copy in copies:
        copy.start()

    def drain(k, _):
        s = lax.rem(k, RING)

        def use(ring_view, view, width):
            x_copy(k, ring_view, view).wait_send()
            remote(ring_view(par_o, s), ring_view(par_o, s), do_send.at[s], do_recv.at[s], peer_core).wait_send()
            remote(view(pm7, pmd), view(pm7, pmd), dm_send.at[s], dm_recv.at[k], peer_core).wait_send()

        on_view(k, use)
        return 0

    lax.fori_loop(N - RING, N, drain, 0)
    for copy in f_state:
        copy.wait()
    f_gather.wait()
    g7[6, give_out, :] = f_in[...]
    for copy in sqf_copies:
        copy.wait()
    total = sq_first[0]
    for i in range(1, 8):
        total = total + sq_first[i]
    for copy in copies:
        copy.wait()
    sq_out[...] = ((sq_all[0] + sq_all[1]) + (sq_all[2] + sq_all[3])) + total


def update_math(avg_scale, sq_scale, g, w, m, v, decay):
    avg = ADAM_BETA1 * m + avg_scale * g
    root = sq_scale * g
    sq = ADAM_BETA2 * v + root * root
    dev = sq * lax.rsqrt(jnp.maximum(sq, SMALLEST))
    step_dir = avg / (dev + ADAM_EPS * ROOT_TWO)
    new = (1.0 - LEARN_RATE * decay) * w - (LEARN_RATE * ROOT_TWO / BIAS_ONE) * step_dir
    return new, avg, sq, new.astype(jnp.bfloat16)


def update_kernel(sq, g7, gd, gn, w7, m7, v7, wd, md, vd, wn, mn, vn,
                  lw, lm, lv, lb, dw, dm, dv, db, nw, nm, nv, nb, ew, em, ev, eb,
                  s7w, s7m, s7v, s7b, sdw, sdm, sdv, sdb, snw, snm, snv, snb, sem7, semd, semn):
    total = jnp.sum(sq[...], keepdims=True)
    clip = jnp.minimum(1.0, 1.0 / (jnp.sqrt(total) + CLIP_EPS))
    scales = ((1.0 - ADAM_BETA1) * clip, math.sqrt(1.0 - ADAM_BETA2) * clip)

    def seven_copies(j, row, outs):
        i = row // 16
        return [pltpu.make_async_copy(src.at[j, pl.ds(row, 16), :], dst, sem7.at[a, j, i])
                for a, (src, dst) in enumerate(zip((s7w, s7m, s7v, s7b), outs))]

    def layer_copies(j, row):
        return seven_copies(j, row, [o.at[j, pl.ds(row, 16), :] for o in (lw, lm, lv, lb)])

    def embed_copies(row):
        return seven_copies(6, row, [o.at[pl.ds(row, 16), :] for o in (ew, em, ev, eb)])

    def seven(j, decay, row):
        at = (j, pl.ds(row, 16))
        for c in range(0, WIDTH, 512):
            ix = at + (pl.ds(c, 512),)
            out = update_math(*scales, g7[ix], w7[ix], m7[ix], v7[ix], decay)
            for ref, val in zip((s7w, s7m, s7v, s7b), out):
                ref[ix] = val

    def layer_step(t, _):
        j = t // 4
        row = pl.multiple_of((t % 4) * 16, 16)
        seven(j, WEIGHT_DECAY, row)
        for copy in layer_copies(j, row):
            copy.start()
        return 0

    def embed_step(t, _):
        row = pl.multiple_of(t * 16, 16)
        seven(6, 0.0, row)
        for copy in embed_copies(row):
            copy.start()
        return 0

    def down_copies(t):
        row = pl.multiple_of((t // 2) * 16, 16)
        col = pl.multiple_of((t % 2) * (FF // 2), FF // 2)
        ix = (pl.ds(row, 16), pl.ds(col, FF // 2))
        return [pltpu.make_async_copy(src.at[ix], dst.at[ix], semd.at[a, t])
                for a, (src, dst) in enumerate(zip((sdw, sdm, sdv, sdb), (dw, dm, dv, db)))]

    def down_step(t, _):
        row = pl.multiple_of((t // 2) * 16, 16)
        col = pl.multiple_of((t % 2) * (FF // 2), FF // 2)
        for c in range(0, FF // 2, 512):
            ix = (pl.ds(row, 16), pl.ds(pl.multiple_of(col + c, 512), 512))
            out = update_math(*scales, gd[ix], wd[ix], md[ix], vd[ix], WEIGHT_DECAY)
            for ref, val in zip((sdw, sdm, sdv, sdb), out):
                ref[ix] = val
        for copy in down_copies(t):
            copy.start()
        return 0

    lax.fori_loop(0, 8, down_step, 0)
    out = update_math(*scales, gn[...], wn[...], mn[...], vn[...], WEIGHT_DECAY)
    for ref, val in zip((snw, snm, snv, snb), out):
        ref[...] = val
    norm_copies = [pltpu.make_async_copy(src, dst, semn.at[a])
                   for a, (src, dst) in enumerate(zip((snw, snm, snv, snb), (nw, nm, nv, nb)))]
    for copy in norm_copies:
        copy.start()
    lax.fori_loop(0, 24, layer_step, 0)
    lax.fori_loop(0, 4, embed_step, 0)

    def layer_wait(t, _):
        for copy in layer_copies(t // 4, pl.multiple_of((t % 4) * 16, 16)):
            copy.wait()
        return 0

    def embed_wait(t, _):
        for copy in embed_copies(pl.multiple_of(t * 16, 16)):
            copy.wait()
        return 0

    def down_wait(t, _):
        for copy in down_copies(t):
            copy.wait()
        return 0

    lax.fori_loop(0, 8, down_wait, 0)
    for copy in norm_copies:
        copy.wait()
    lax.fori_loop(0, 24, layer_wait, 0)
    lax.fori_loop(0, 4, embed_wait, 0)


def local_update(g_layer, g_down, g_norm, g_embed, layer_w, layer_m, layer_v, down_w, down_m, down_v, norm_w, norm_m,
                 norm_v, embed_w, embed_m, embed_v):
    any_spec = pl.BlockSpec(memory_space=pl.ANY)
    vmem_spec = pl.BlockSpec(memory_space=pltpu.VMEM)
    dma = pltpu.SemaphoreType.DMA
    held = [(8, 128)] + [SEVEN, DOWN, NORM] + [SEVEN] * 3 + [DOWN] * 3 + [NORM] * 3
    reduced = pl.pallas_call(
        reduce_kernel,
        out_shape=[pltpu.VMEM(shape, F32) for shape in held],
        in_specs=[any_spec] * 16,
        out_specs=[vmem_spec] * len(held),
        scratch_shapes=[pltpu.VMEM((RING, 8, WIDTH), F32), pltpu.VMEM((RING, 8, WIDTH), F32)]
        + [pltpu.VMEM(SEVEN, F32), pltpu.VMEM(DOWN, F32)] * 3
        + [pltpu.VMEM(NORM, F32)] * 5
        + [pltpu.VMEM((8, 128), F32), pltpu.VMEM((4, 8, 128), F32), pltpu.VMEM((8, 8, 128), F32)]
        + [pltpu.VMEM((FIRST, WIDTH), F32)] * 4
        + [pltpu.VMEM((2, 8, WIDTH), F32)] + [pltpu.VMEM((8, WIDTH), F32)] * 3
        + [dma((RING,)), dma((RING,)), dma((RING,)), dma((RING,)), dma((RING,)), dma((N,)), dma((RING,)), dma((N,)),
           dma((RING,)), dma((N,)), dma((3, RING)), dma((5,)), dma((4,)), dma((4,)), dma((3,)), dma((3,)),
           dma((7,)), dma((7,)), dma((5,)), dma((6,)), dma((6,)),
           pltpu.SemaphoreType.REGULAR],
        compiler_params=pltpu.CompilerParams(collective_id=0, has_side_effects=True,
                                             vmem_limit_bytes=26 * 1024 * 1024),
    )(g_layer, g_down, g_norm, g_embed, layer_w, layer_m, layer_v, down_w, down_m, down_v, norm_w, norm_m, norm_v,
      embed_w, embed_m, embed_v)
    groups = ((6, ROWS, WIDTH), DOWN, NORM, (ROWS, WIDTH))
    out_shape = [jax.ShapeDtypeStruct(s, d) for s in groups for d in (F32, F32, F32, jnp.bfloat16)]
    staged = [pltpu.VMEM(s, d) for s in (SEVEN, DOWN, NORM) for d in (F32, F32, F32, jnp.bfloat16)]
    return pl.pallas_call(
        update_kernel,
        out_shape=out_shape,
        in_specs=[vmem_spec] * len(held),
        out_specs=[any_spec] * 16,
        scratch_shapes=staged + [dma((4, 7, 4)), dma((4, 8)), dma((4,))],
        compiler_params=pltpu.CompilerParams(vmem_limit_bytes=26 * 1024 * 1024),
    )(*[pltpu.with_memory_space_constraint(a, pltpu.VMEM) for a in reduced])


def solution(mesh):
    grad_four = P(("dp", "fsdp"), None, None, None)
    grad_three = P(("dp", "fsdp"), None, None)
    layer_spec = P(None, "fsdp", None)
    down_spec = P("fsdp", None)
    norm_spec = P(None, "fsdp")
    embed_spec = P("fsdp", None)
    in_specs = (grad_four, grad_three, grad_three, grad_three,
                layer_spec, layer_spec, layer_spec, down_spec, down_spec, down_spec,
                norm_spec, norm_spec, norm_spec, embed_spec, embed_spec, embed_spec)
    out_specs = (layer_spec,) * 4 + (down_spec,) * 4 + (norm_spec,) * 4 + (embed_spec,) * 4
    return jax.shard_map(local_update, mesh=mesh, in_specs=in_specs, out_specs=out_specs, check_vma=False)
```

```python
import math

import jax
import jax.numpy as jnp
from jax import lax
from jax.experimental import pallas as pl
from jax.experimental.pallas import tpu as pltpu
from jax.sharding import PartitionSpec as P

ADAM_BETA1 = 0.9
ADAM_BETA2 = 0.95
ADAM_EPS = 1e-8
LEARN_RATE = 4e-4
WEIGHT_DECAY = 0.1
CLIP_EPS = 1e-6
OPT_STEP = 20
BIAS_ONE = 1.0 - ADAM_BETA1 ** OPT_STEP
BIAS_TWO = 1.0 - ADAM_BETA2 ** OPT_STEP
ROOT_TWO = math.sqrt(BIAS_TWO)
SMALLEST = 1.1754944e-38

MESH = pl.DeviceIdType.MESH
F32 = jnp.float32

ROWS = 64
WIDTH = 3072
FF = 8192
PIECE = 2048
NORM = (4, 768)
SEVEN = (7, ROWS, WIDTH)
DOWN = (ROWS, FF)

FIRST = 16
N_EMBED = (ROWS - FIRST) // 8
N_LAYER = N_EMBED + 6 * (ROWS // 16)
N_WIDE = N_LAYER + (FF // PIECE) * (ROWS // 16 - 1)
N = N_WIDE + (FF // PIECE) * 2

RING = 7
FETCH = 5
LEAD = 3
LAG = 3


class Chunk:
    def __init__(self, kind, k):
        self.kind = kind
        if kind == "embed":
            self.rows, self.width = 8, WIDTH
            self.row = pl.multiple_of(k * 8, 8)
        elif kind == "layer":
            q = k - N_EMBED
            self.rows, self.width = 16, WIDTH
            self.j = q // 4
            self.row = pl.multiple_of((q % 4) * 16, 16)
        else:
            wide = kind == "wide"
            q = k - (N_LAYER if wide else N_WIDE)
            self.rows, self.width = (16, PIECE) if wide else (8, PIECE)
            start = 0 if wide else ROWS - 16
            self.row = pl.multiple_of(start + (q // 4) * self.rows, 8)
            self.cols = pl.ds(pl.multiple_of((q % 4) * PIECE, PIECE), PIECE)

    def source(self, grads, q):
        g_layer, g_down, g_embed = grads
        rows = pl.ds(pl.multiple_of(q * ROWS + self.row, 8), self.rows)
        if self.kind == "embed":
            return g_embed.at[0, rows, :]
        if self.kind == "layer":
            return g_layer.at[0, self.j, rows, :]
        return g_down.at[0, rows, self.cols]

    def state(self, layer, down, embed):
        rows = pl.ds(self.row, self.rows)
        if self.kind == "embed":
            return embed.at[rows, :]
        if self.kind == "layer":
            return layer.at[self.j, rows, :]
        return down.at[rows, self.cols]

    def held(self, seven, down):
        rows = pl.ds(self.row, self.rows)
        if self.kind == "embed":
            return seven.at[6, rows, :]
        if self.kind == "layer":
            return seven.at[self.j, rows, :]
        return down.at[rows, self.cols]

    def ring(self, ring, s):
        return ring.at[s, pl.ds(0, self.rows), pl.ds(0, self.width)]


def on_chunk(k, use):
    bounds = (0, N_EMBED, N_LAYER, N_WIDE, N)
    for i, kind in enumerate(("embed", "layer", "wide", "down")):
        @pl.when(jnp.logical_and(k >= bounds[i], k < bounds[i + 1]))
        def _():
            use(Chunk(kind, k))


def squares(mean, width):
    parts = [mean[r:r + 8, i * 128:(i + 1) * 128] for r in range(0, mean.shape[0], 8) for i in range(width // 128)]
    sums = [p * p for p in parts[:4]]
    for i, p in enumerate(parts[4:]):
        sums[i % 4] = sums[i % 4] + p * p
    return (sums[0] + sums[1]) + (sums[2] + sums[3])


def reduce_kernel(g_layer, g_down, g_norm, g_embed, layer_w, layer_m, layer_v, down_w, down_m, down_v,
                  norm_w, norm_m, norm_v, embed_w, embed_m, embed_v,
                  sq_out, g7, gd, gn, w7, m7, v7, wd, md, vd, wn, mn, vn,
                  own_o, par_o, pm7, pmd, x7, xd, y7, yd, own_no, par_no, pmn, xn, yn, acc, sq_all, sq_first,
                  pre, fo_own, fo_par, fm_own, fm_par, f_y, f_x_in, f_out, f_in,
                  own_o_sem, own_m_sem, do_send, do_recv, dm_send, dm_recv, x_send, x_recv, y_send, y_recv,
                  st_sem, n_sem, n_send, n_recv, sq_send, sq_recv, sqf_send, sqf_recv, f_sem, f_send, f_recv, pre_sem, credit):
    dp = lax.axis_index("dp")
    f = lax.axis_index("fsdp")
    core = lax.rem(f, 2)
    f_core = f + 1 - 2 * core
    f_x = lax.rem(f + 2, 4)
    f_diag = lax.rem(f_core + 2, 4)
    peer_core = (dp, f_core)
    peer_x = (dp, f_x)
    peer_diag = (dp, f_diag)
    peer_y = (1 - dp, f)
    peers = (peer_core, peer_x, peer_diag, peer_y, (1 - dp, f_core), (1 - dp, f_x), (1 - dp, f_diag))

    def remote(src, dst, send, recv, peer):
        return pltpu.make_async_remote_copy(src_ref=src, dst_ref=dst, send_sem=send, recv_sem=recv,
                                            device_id=peer, device_id_type=MESH)

    grads = (g_layer, g_down, g_embed)

    def x_copy(k, chunk):
        s = lax.rem(k, RING)
        return remote(chunk.ring(own_o, s), chunk.held(x7, xd), x_send.at[s], x_recv.at[k], peer_x)

    def y_copy(k, chunk):
        s = lax.rem(k, RING)
        return remote(chunk.held(g7, gd), chunk.held(y7, yd), y_send.at[s], y_recv.at[k], peer_y)

    def push_other(k, chunk, source):
        s = lax.rem(k, RING)
        return remote(source, chunk.ring(par_o, s), do_send.at[s], do_recv.at[s], peer_core)

    def push_mine(k, chunk, source):
        s = lax.rem(k, RING)
        return remote(source, chunk.held(pm7, pmd), dm_send.at[s], dm_recv.at[k], peer_core)

    def own_loads(k, chunk):
        s = lax.rem(k, RING)
        return [pltpu.make_async_copy(chunk.source(grads, f_x), chunk.ring(own_o, s), own_o_sem.at[s]),
                pltpu.make_async_copy(chunk.source(grads, f), chunk.held(g7, gd), own_m_sem.at[s])]

    def retire(k, chunk):
        s = lax.rem(k, RING)
        x_copy(k, chunk).wait_send()
        push_other(k, chunk, chunk.ring(par_o, s)).wait_send()
        push_mine(k, chunk, chunk.held(pm7, pmd)).wait_send()

    def fetch(k):
        @pl.when(jnp.logical_and(k >= RING, k < N))
        def _():
            on_chunk(k - RING, lambda chunk: retire(k - RING, chunk))
            pl.semaphore_wait(credit, 1)

        def start(chunk):
            push_other(k, chunk, chunk.source(grads, f_diag)).start()
            for copy in own_loads(k, chunk):
                copy.start()
            push_mine(k, chunk, chunk.source(grads, f_core)).start()

        on_chunk(k, start)

    def sum_x(k):
        s = lax.rem(k, RING)

        def use(chunk):
            mine = chunk.held(g7, gd)
            theirs = chunk.held(pm7, pmd)
            pltpu.make_async_copy(mine, mine, own_m_sem.at[s]).wait()
            push_mine(k, chunk, theirs).wait_recv()
            x_copy(k, chunk).wait_recv()
            mine[...] = (mine[...] + theirs[...]) + chunk.held(x7, xd)[...]

        on_chunk(k, use)

    def sum_chip(k):
        s = lax.rem(k, RING)

        def use(chunk):
            mine = chunk.ring(own_o, s)
            theirs = chunk.ring(par_o, s)
            pltpu.make_async_copy(mine, mine, own_o_sem.at[s]).wait()
            push_other(k, chunk, theirs).wait_recv()
            mine[...] = mine[...] + theirs[...]

        on_chunk(k, use)

    def start_x(k):
        on_chunk(k, lambda chunk: x_copy(k, chunk).start())

        @pl.when(jnp.logical_and(k >= 0, k < N - RING))
        def _():
            pl.semaphore_signal(credit, inc=1, device_id=peer_core, device_id_type=MESH)

    def start_y(k):
        s = lax.rem(k, RING)

        def use(chunk):
            y_copy(k, chunk).start()
            for i, (src, dst) in enumerate((((layer_w, down_w, embed_w), (w7, wd)), ((layer_m, down_m, embed_m), (m7, md)),
                                            ((layer_v, down_v, embed_v), (v7, vd)))):
                pltpu.make_async_copy(chunk.state(*src), chunk.held(*dst), st_sem.at[i, s]).start()

        on_chunk(k, use)

    def sum_y(k):
        s = lax.rem(k, RING)

        def use(chunk):
            y_copy(k, chunk).wait()
            for i, pair in enumerate(((w7, wd), (m7, md), (v7, vd))):
                ref = chunk.held(*pair)
                pltpu.make_async_copy(ref, ref, st_sem.at[i, s]).wait()
            mine = chunk.held(g7, gd)
            mean = (mine[...] + chunk.held(y7, yd)[...]) * 0.125
            mine[...] = mean
            acc[...] += squares(mean, chunk.width)

        on_chunk(k, use)

    def embed_rows(q):
        return g_embed.at[0, pl.ds(pl.multiple_of(q * ROWS + (ROWS - FIRST), 8), FIRST), :]

    f_give = [pltpu.make_async_copy(embed_rows(q), own_o.at[RING - 2 + i], f_sem.at[5 + i])
              for i, q in enumerate((f_diag, f_core))]
    f_push = [remote(own_o.at[RING - 2], fo_par, f_send.at[0], f_recv.at[0], peer_core),
              remote(own_o.at[RING - 1], fm_par, f_send.at[1], f_recv.at[1], peer_core)]
    f_local = [pltpu.make_async_copy(src, dst, f_sem.at[i]) for i, (src, dst) in enumerate(
        ((embed_rows(f_x), fo_own), (embed_rows(f), fm_own)))]
    last = pl.ds(ROWS - FIRST, FIRST)
    f_state = [pltpu.make_async_copy(src.at[last, :], dst.at[6, last, :], f_sem.at[2 + i])
               for i, (src, dst) in enumerate(((embed_w, w7), (embed_m, m7), (embed_v, v7)))]
    keep = pl.ds(pl.multiple_of(dp * 8, 8), 8)
    give = pl.ds(pl.multiple_of((1 - dp) * 8, 8), 8)
    keep_out = pl.ds(pl.multiple_of(ROWS - FIRST + dp * 8, 8), 8)
    give_out = pl.ds(pl.multiple_of(ROWS - FIRST + (1 - dp) * 8, 8), 8)
    f_scatter = [remote(fo_own.at[give, :], f_y.at[0], f_send.at[2], f_recv.at[2], peer_y),
                 remote(fm_own.at[give, :], f_y.at[1], f_send.at[3], f_recv.at[3], peer_y)]
    f_cross = remote(fo_own.at[keep, :], f_x_in, f_send.at[4], f_recv.at[4], peer_x)
    f_gather = remote(f_out, f_in, f_send.at[5], f_recv.at[5], peer_y)
    me = dp * 4 + f
    sqf_copies = [remote(sq_first.at[me], sq_first.at[me], sqf_send.at[i], sqf_recv.at[i], peer)
                  for i, peer in enumerate(peers)]

    def norm_source(q):
        return g_norm.at[0, :, pl.ds(pl.multiple_of(q * NORM[1], 128), NORM[1])]

    n_push_other = remote(norm_source(f_diag), par_no, n_send.at[0], n_recv.at[0], peer_core)
    n_push_mine = remote(norm_source(f_core), pmn, n_send.at[1], n_recv.at[1], peer_core)
    n_x = remote(own_no, xn, n_send.at[2], n_recv.at[2], peer_x)
    n_y = remote(gn, yn, n_send.at[3], n_recv.at[3], peer_y)
    n_local = [pltpu.make_async_copy(src, dst, n_sem.at[i]) for i, (src, dst) in enumerate(
        ((norm_source(f_x), own_no), (norm_source(f), gn), (norm_w, wn), (norm_m, mn), (norm_v, vn)))]

    zero = Chunk("embed", 0)
    ahead = pltpu.make_async_copy(zero.source(grads, f_diag), pre, pre_sem)
    ahead.start()
    for copy in own_loads(0, zero):
        copy.start()
    for copy in f_give + f_local:
        copy.start()
    acc[...] = jnp.zeros_like(acc)

    barrier = pltpu.get_barrier_semaphore()
    for peer in peers:
        pl.semaphore_signal(barrier, inc=1, device_id=peer, device_id_type=MESH)
    ahead.wait()
    pl.semaphore_wait(barrier, len(peers))
    push_other(0, zero, pre).start()
    for copy, push in zip(f_give, f_push):
        copy.wait()
        push.start()
    push_mine(0, zero, zero.source(grads, f_core)).start()

    def step(t, _):
        i = t - FETCH
        fetch(i + FETCH)

        @pl.when(i == 0)
        def _():
            n_push_other.start()
            n_push_mine.start()
            for copy in n_local:
                copy.start()

        sum_x(i)
        sum_chip(i + LEAD)
        start_y(i)
        start_x(i + LEAD)

        @pl.when(i == 1 - LEAD)
        def _():
            for copy in f_local:
                copy.wait()
            for copy in f_push:
                copy.wait()
            fo_own[...] = fo_own[...] + fo_par[...]
            fm_own[...] = fm_own[...] + fm_par[...]
            for copy in f_scatter:
                copy.start()
            for copy in f_state:
                copy.start()

        @pl.when(i == 3)
        def _():
            for copy in n_local:
                copy.wait()
            n_push_other.wait()
            n_push_mine.wait()
            own_no[...] = own_no[...] + par_no[...]
            n_x.start()

        @pl.when(i == 10)
        def _():
            n_x.wait()
            gn[...] = (gn[...] + pmn[...]) + xn[...]
            n_y.start()
            for copy in f_scatter:
                copy.wait()
            fo_own[keep, :] = fo_own[keep, :] + f_y[0]
            fm_own[keep, :] = fm_own[keep, :] + f_y[1]

        @pl.when(i == 20)
        def _():
            n_y.wait()
            mean = (gn[...] + yn[...]) * 0.125
            gn[...] = mean
            square = mean * mean
            total = square[:, 0:128]
            for c in range(1, NORM[1] // 128):
                total = total + square[:, c * 128:(c + 1) * 128]
            acc[0:4, :] += total

        @pl.when(i == N - LEAD)
        def _():
            f_cross.start()

        @pl.when(i == N + LAG - 2)
        def _():
            f_cross.wait()
            mean = (fm_own[keep, :] + f_x_in[...]) * 0.125
            f_out[...] = mean
            g7[6, keep_out, :] = mean
            sq_first[me] = squares(mean, WIDTH)
            f_gather.start()
            for copy in sqf_copies:
                copy.start()

        sum_y(i - LAG)
        return 0

    lax.fori_loop(1, FETCH + N + LAG, step, 0)

    sq_all[f] = acc[...]
    copies = [remote(sq_all.at[f], sq_all.at[f], sq_send.at[i], sq_recv.at[i], peer)
              for i, peer in enumerate((peer_core, peer_x, peer_diag))]
    for copy in copies:
        copy.start()

    def drain(k, _):
        on_chunk(k, lambda chunk: retire(k, chunk))
        return 0

    lax.fori_loop(N - RING, N, drain, 0)
    for copy in f_state:
        copy.wait()
    f_gather.wait()
    g7[6, give_out, :] = f_in[...]
    for copy in sqf_copies:
        copy.wait()
    total = sq_first[0]
    for i in range(1, 8):
        total = total + sq_first[i]
    for copy in copies:
        copy.wait()
    sq_out[...] = ((sq_all[0] + sq_all[1]) + (sq_all[2] + sq_all[3])) + total


def update_math(avg_scale, sq_scale, g, w, m, v, decay):
    avg = ADAM_BETA1 * m + avg_scale * g
    root = sq_scale * g
    sq = ADAM_BETA2 * v + root * root
    dev = sq * lax.rsqrt(jnp.maximum(sq, SMALLEST))
    step_dir = avg / (dev + ADAM_EPS * ROOT_TWO)
    new = (1.0 - LEARN_RATE * decay) * w - (LEARN_RATE * ROOT_TWO / BIAS_ONE) * step_dir
    return new, avg, sq, new.astype(jnp.bfloat16)


def update_kernel(sq, g7, gd, gn, w7, m7, v7, wd, md, vd, wn, mn, vn,
                  lw, lm, lv, lb, dw, dm, dv, db, nw, nm, nv, nb, ew, em, ev, eb,
                  s7w, s7m, s7v, s7b, sdw, sdm, sdv, sdb, snw, snm, snv, snb, sem7, semd, semn):
    total = jnp.sum(sq[...], keepdims=True)
    clip = jnp.minimum(1.0, 1.0 / (jnp.sqrt(total) + CLIP_EPS))
    scales = ((1.0 - ADAM_BETA1) * clip, math.sqrt(1.0 - ADAM_BETA2) * clip)

    outs = ((lw, lm, lv, lb), (dw, dm, dv, db), (nw, nm, nv, nb), (ew, em, ev, eb))
    seven_staged = (s7w, s7m, s7v, s7b)
    down_staged = (sdw, sdm, sdv, sdb)

    def layer_copies(j, row, rows):
        at = pl.ds(row, rows)
        return [pltpu.make_async_copy(src.at[j, at, :], dst.at[j, at, :], sem7.at[a, j, row // 16])
                for a, (src, dst) in enumerate(zip(seven_staged, outs[0]))]

    def embed_copies():
        return [pltpu.make_async_copy(src.at[6], dst, sem7.at[a, 6, 0])
                for a, (src, dst) in enumerate(zip(seven_staged, outs[3]))]

    def down_copies(t):
        at = pl.ds(pl.multiple_of(t * 16, 16), 16)
        return [pltpu.make_async_copy(src.at[at, :], dst.at[at, :], semd.at[a, t])
                for a, (src, dst) in enumerate(zip(down_staged, outs[1]))]

    def start(copies):
        for copy in copies:
            copy.start()

    def wait(copies):
        for copy in copies:
            copy.wait()

    def seven(j, row, decay):
        for c in range(0, WIDTH, 512):
            ix = (j, pl.ds(row, 16), pl.ds(c, 512))
            out = update_math(*scales, g7[ix], w7[ix], m7[ix], v7[ix], decay)
            for ref, val in zip(seven_staged, out):
                ref[ix] = val

    def block(j, decay):
        def rows(t, _):
            seven(j, pl.multiple_of(t * 16, 16), decay)
            return 0

        lax.fori_loop(0, 4, rows, 0)

    def first_step(t, _):
        row = pl.multiple_of(t * 16, 16)
        seven(0, row, WEIGHT_DECAY)
        start(layer_copies(0, row, 16))
        return 0

    def layer_step(j, _):
        block(j, WEIGHT_DECAY)
        start(layer_copies(j, 0, ROWS))
        return 0

    def down_step(t, _):
        row = pl.multiple_of(t * 16, 16)

        def cols(u, _):
            ix = (pl.ds(row, 16), pl.ds(pl.multiple_of(u * 1024, 1024), 1024))
            out = update_math(*scales, gd[ix], wd[ix], md[ix], vd[ix], WEIGHT_DECAY)
            for ref, val in zip(down_staged, out):
                ref[ix] = val
            return 0

        lax.fori_loop(0, FF // 1024, cols, 0)
        start(down_copies(t))
        return 0

    lax.fori_loop(0, 4, first_step, 0)
    lax.fori_loop(1, 6, layer_step, 0)
    out = update_math(*scales, gn[...], wn[...], mn[...], vn[...], WEIGHT_DECAY)
    for ref, val in zip((snw, snm, snv, snb), out):
        ref[...] = val
    norm_copies = [pltpu.make_async_copy(src, dst, semn.at[a])
                   for a, (src, dst) in enumerate(zip((snw, snm, snv, snb), outs[2]))]
    start(norm_copies)
    block(6, 0.0)
    start(embed_copies())
    lax.fori_loop(0, 4, down_step, 0)

    for row in range(0, ROWS, 16):
        wait(layer_copies(0, row, 16))

    def layer_wait(j, _):
        wait(layer_copies(j, 0, ROWS))
        return 0

    def down_wait(t, _):
        wait(down_copies(t))
        return 0

    lax.fori_loop(1, 6, layer_wait, 0)
    wait(norm_copies)
    wait(embed_copies())
    lax.fori_loop(0, 4, down_wait, 0)


def local_update(g_layer, g_down, g_norm, g_embed, layer_w, layer_m, layer_v, down_w, down_m, down_v, norm_w, norm_m,
                 norm_v, embed_w, embed_m, embed_v):
    any_spec = pl.BlockSpec(memory_space=pl.ANY)
    vmem_spec = pl.BlockSpec(memory_space=pltpu.VMEM)
    dma = pltpu.SemaphoreType.DMA
    held = [(8, 128)] + [SEVEN, DOWN, NORM] + [SEVEN] * 3 + [DOWN] * 3 + [NORM] * 3
    reduced = pl.pallas_call(
        reduce_kernel,
        out_shape=[pltpu.VMEM(shape, F32) for shape in held],
        in_specs=[any_spec] * 16,
        out_specs=[vmem_spec] * len(held),
        scratch_shapes=[pltpu.VMEM((RING, 16, WIDTH), F32), pltpu.VMEM((RING, 16, WIDTH), F32)]
        + [pltpu.VMEM(SEVEN, F32), pltpu.VMEM(DOWN, F32)] * 3
        + [pltpu.VMEM(NORM, F32)] * 5
        + [pltpu.VMEM((8, 128), F32), pltpu.VMEM((4, 8, 128), F32), pltpu.VMEM((8, 8, 128), F32)]
        + [pltpu.VMEM((8, WIDTH), F32)] + [pltpu.VMEM((FIRST, WIDTH), F32)] * 4
        + [pltpu.VMEM((2, 8, WIDTH), F32)] + [pltpu.VMEM((8, WIDTH), F32)] * 3
        + [dma((RING,)), dma((RING,)), dma((RING,)), dma((RING,)), dma((RING,)), dma((N,)), dma((RING,)), dma((N,)),
           dma((RING,)), dma((N,)), dma((3, RING)), dma((5,)), dma((4,)), dma((4,)), dma((3,)), dma((3,)),
           dma((7,)), dma((7,)), dma((7,)), dma((6,)), dma((6,)), dma,
           pltpu.SemaphoreType.REGULAR],
        compiler_params=pltpu.CompilerParams(collective_id=0, has_side_effects=True,
                                             vmem_limit_bytes=26 * 1024 * 1024),
    )(g_layer, g_down, g_norm, g_embed, layer_w, layer_m, layer_v, down_w, down_m, down_v, norm_w, norm_m, norm_v,
      embed_w, embed_m, embed_v)
    groups = ((6, ROWS, WIDTH), DOWN, NORM, (ROWS, WIDTH))
    out_shape = [jax.ShapeDtypeStruct(s, d) for s in groups for d in (F32, F32, F32, jnp.bfloat16)]
    staged = [pltpu.VMEM(s, d) for s in (SEVEN, DOWN, NORM) for d in (F32, F32, F32, jnp.bfloat16)]
    return pl.pallas_call(
        update_kernel,
        out_shape=out_shape,
        in_specs=[vmem_spec] * len(held),
        out_specs=[any_spec] * 16,
        scratch_shapes=staged + [dma((4, 7, 4)), dma((4, 4)), dma((4,))],
        compiler_params=pltpu.CompilerParams(vmem_limit_bytes=26 * 1024 * 1024),
    )(*[pltpu.with_memory_space_constraint(a, pltpu.VMEM) for a in reduced])


def solution(mesh):
    grad_four = P(("dp", "fsdp"), None, None, None)
    grad_three = P(("dp", "fsdp"), None, None)
    layer_spec = P(None, "fsdp", None)
    down_spec = P("fsdp", None)
    norm_spec = P(None, "fsdp")
    embed_spec = P("fsdp", None)
    in_specs = (grad_four, grad_three, grad_three, grad_three,
                layer_spec, layer_spec, layer_spec, down_spec, down_spec, down_spec,
                norm_spec, norm_spec, norm_spec, embed_spec, embed_spec, embed_spec)
    out_specs = (layer_spec,) * 4 + (down_spec,) * 4 + (norm_spec,) * 4 + (embed_spec,) * 4
    return jax.shard_map(local_update, mesh=mesh, in_specs=in_specs, out_specs=out_specs, check_vma=False)
```

```python
import math

import jax
import jax.numpy as jnp
from jax import lax
from jax.experimental import pallas as pl
from jax.experimental.pallas import tpu as pltpu
from jax.sharding import PartitionSpec as P

ADAM_BETA1 = 0.9
ADAM_BETA2 = 0.95
ADAM_EPS = 1e-8
LEARN_RATE = 4e-4
WEIGHT_DECAY = 0.1
CLIP_EPS = 1e-6
OPT_STEP = 20
BIAS_ONE = 1.0 - ADAM_BETA1 ** OPT_STEP
BIAS_TWO = 1.0 - ADAM_BETA2 ** OPT_STEP
ROOT_TWO = math.sqrt(BIAS_TWO)
SMALLEST = 1.1754944e-38

MESH = pl.DeviceIdType.MESH
F32 = jnp.float32

ROWS = 64
WIDTH = 3072
FF = 8192
PIECE = 2048
NORM = (4, 768)
SEVEN = (7, ROWS, WIDTH)
DOWN = (ROWS, FF)

FIRST = 8
SPLIT = FF // 2
N_EMBED = ROWS // 8
N_LAYER = N_EMBED + 6 * (ROWS // 16)
N_WIDE = N_LAYER + (FF // PIECE) * (ROWS // 16 - 1)
N = N_WIDE + (FF // PIECE) * (16 - FIRST) // 8

RING = 7
Y_RING = 8
M_RING = 10
FETCH = 5
LEAD = 3
LAG = 3


class Chunk:
    def __init__(self, kind, k):
        self.kind = kind
        if kind == "embed":
            self.rows, self.width = 8, WIDTH
            self.row = pl.multiple_of(k * 8, 8)
        elif kind == "layer":
            q = k - N_EMBED
            self.rows, self.width = 16, WIDTH
            self.j = q // 4
            self.row = pl.multiple_of((q % 4) * 16, 16)
        else:
            wide = kind == "wide"
            q = k - (N_LAYER if wide else N_WIDE)
            self.rows, self.width = (16, PIECE) if wide else (8, PIECE)
            start = 0 if wide else ROWS - 16
            self.row = pl.multiple_of(start + (q // 4) * self.rows, 8)
            self.cols = pl.ds(pl.multiple_of((q % 4) * PIECE, PIECE), PIECE)

    def source(self, grads, q):
        g_layer, g_down, g_embed = grads
        rows = pl.ds(pl.multiple_of(q * ROWS + self.row, 8), self.rows)
        if self.kind == "embed":
            return g_embed.at[0, rows, :]
        if self.kind == "layer":
            return g_layer.at[0, self.j, rows, :]
        return g_down.at[0, rows, self.cols]

    def state(self, layer, down, embed):
        rows = pl.ds(self.row, self.rows)
        if self.kind == "embed":
            return embed.at[rows, :]
        if self.kind == "layer":
            return layer.at[self.j, rows, :]
        return down.at[rows, self.cols]

    def held(self, seven, down):
        rows = pl.ds(self.row, self.rows)
        if self.kind == "embed":
            return seven.at[6, rows, :]
        if self.kind == "layer":
            return seven.at[self.j, rows, :]
        return down.at[rows, self.cols]

    def ring(self, ring, s):
        return ring.at[s, pl.ds(0, self.rows), pl.ds(0, self.width)]


def on_chunk(k, use):
    if isinstance(k, int):
        use(Chunk("embed", k))
        return
    bounds = (0, N_EMBED, N_LAYER, N_WIDE, N)
    for i, kind in enumerate(("embed", "layer", "wide", "down")):
        @pl.when(jnp.logical_and(k >= bounds[i], k < bounds[i + 1]))
        def _():
            use(Chunk(kind, k))


def start(copies):
    for copy in copies:
        copy.start()


def wait(copies):
    for copy in copies:
        copy.wait()


def squares(mean, width):
    parts = [mean[r:r + 8, i * 128:(i + 1) * 128] for r in range(0, mean.shape[0], 8) for i in range(width // 128)]
    sums = [p * p for p in parts[:4]]
    for i, p in enumerate(parts[4:]):
        sums[i % 4] = sums[i % 4] + p * p
    return (sums[0] + sums[1]) + (sums[2] + sums[3])


def reduce_kernel(g_layer, g_down, g_norm, g_embed, layer_w, layer_m, layer_v, down_w, down_m, down_v,
                  norm_w, norm_m, norm_v, embed_w, embed_m, embed_v,
                  sq_out, g7, gd, gn, w7, m7, v7, wd, md, vd, wn, mn, vn,
                  own_o, par_o, pm7, pmd, x7, xd, y7, yd, own_no, par_no, pmn, xn, yn, acc, sq_all, sq_first,
                  pre, fo_own, fo_par, f_held, f_y,
                  own_o_sem, own_m_sem, do_send, do_recv, dm_send, dm_recv, x_send, x_recv, y_send, y_recv,
                  st_sem, n_sem, n_send, n_recv, sq_send, sq_recv, sqf_send, sqf_recv, f_sem, f_send, f_recv, pre_sem, credit):
    dp = lax.axis_index("dp")
    f = lax.axis_index("fsdp")
    core = lax.rem(f, 2)
    f_core = f + 1 - 2 * core
    f_x = lax.rem(f + 2, 4)
    f_diag = lax.rem(f_core + 2, 4)
    peer_core = (dp, f_core)
    peer_x = (dp, f_x)
    peer_diag = (dp, f_diag)
    peer_y = (1 - dp, f)
    peers = (peer_core, peer_x, peer_diag, peer_y, (1 - dp, f_core), (1 - dp, f_x), (1 - dp, f_diag))

    def remote(src, dst, send, recv, peer):
        return pltpu.make_async_remote_copy(src_ref=src, dst_ref=dst, send_sem=send, recv_sem=recv,
                                            device_id=peer, device_id_type=MESH)

    grads = (g_layer, g_down, g_embed)

    def x_copy(k, chunk):
        s = lax.rem(k, RING)
        return remote(chunk.ring(own_o, s), chunk.held(x7, xd), x_send.at[s], x_recv.at[s], peer_x)

    def y_copy(k, chunk):
        s = lax.rem(k, RING)
        return remote(chunk.held(g7, gd), chunk.held(y7, yd), y_send.at[s], y_recv.at[lax.rem(k, Y_RING)], peer_y)

    def push_other(k, chunk, source):
        s = lax.rem(k, RING)
        return remote(source, chunk.ring(par_o, s), do_send.at[s], do_recv.at[s], peer_core)

    def push_mine(k, chunk, source):
        s = lax.rem(k, RING)
        return remote(source, chunk.held(pm7, pmd), dm_send.at[s], dm_recv.at[lax.rem(k, M_RING)], peer_core)

    def own_loads(k, chunk):
        s = lax.rem(k, RING)
        return [pltpu.make_async_copy(chunk.source(grads, f_x), chunk.ring(own_o, s), own_o_sem.at[s]),
                pltpu.make_async_copy(chunk.source(grads, f), chunk.held(g7, gd), own_m_sem.at[s])]

    def retire(k, chunk):
        s = lax.rem(k, RING)
        x_copy(k, chunk).wait_send()
        push_other(k, chunk, chunk.ring(par_o, s)).wait_send()
        push_mine(k, chunk, chunk.held(pm7, pmd)).wait_send()

    def fetch(k):
        @pl.when(jnp.logical_and(k >= RING, k < N))
        def _():
            on_chunk(k - RING, lambda chunk: retire(k - RING, chunk))
            pl.semaphore_wait(credit, 1)

        def begin(chunk):
            push_other(k, chunk, chunk.source(grads, f_diag)).start()
            for copy in own_loads(k, chunk):
                copy.start()
            push_mine(k, chunk, chunk.source(grads, f_core)).start()

        on_chunk(k, begin)

    def sum_x(k):
        s = lax.rem(k, RING)

        def use(chunk):
            mine = chunk.held(g7, gd)
            theirs = chunk.held(pm7, pmd)
            pltpu.make_async_copy(mine, mine, own_m_sem.at[s]).wait()
            push_mine(k, chunk, theirs).wait_recv()
            x_copy(k, chunk).wait_recv()
            mine[...] = (mine[...] + theirs[...]) + chunk.held(x7, xd)[...]

        on_chunk(k, use)

    def sum_chip(k):
        s = lax.rem(k, RING)

        def use(chunk):
            mine = chunk.ring(own_o, s)
            theirs = chunk.ring(par_o, s)
            pltpu.make_async_copy(mine, mine, own_o_sem.at[s]).wait()
            push_other(k, chunk, theirs).wait_recv()
            mine[...] = mine[...] + theirs[...]

        on_chunk(k, use)

    def start_x(k):
        on_chunk(k, lambda chunk: x_copy(k, chunk).start())

        @pl.when(jnp.logical_and(k >= 0, k < N - RING))
        def _():
            pl.semaphore_signal(credit, inc=1, device_id=peer_core, device_id_type=MESH)

    def start_y(k):
        def use(chunk):
            y_copy(k, chunk).start()
            seven = chunk.kind in ("embed", "layer")
            for i, (src, dst) in enumerate((((layer_w, down_w, embed_w), (w7, wd)), ((layer_m, down_m, embed_m), (m7, md)),
                                            ((layer_v, down_v, embed_v), (v7, vd)))):
                pltpu.make_async_copy(chunk.state(*src), chunk.held(*dst), st_sem.at[i if seven else 3 + i]).start()

        on_chunk(k, use)

    def sum_y(k):
        def use(chunk):
            y_copy(k, chunk).wait()
            mine = chunk.held(g7, gd)
            mean = (mine[...] + chunk.held(y7, yd)[...]) * 0.125
            mine[...] = mean
            acc[...] += squares(mean, chunk.width)

        on_chunk(k, use)

    last = pl.ds(ROWS - FIRST, FIRST)
    keep = pl.ds(pl.multiple_of(dp * SPLIT, SPLIT), SPLIT)
    give = pl.ds(pl.multiple_of((1 - dp) * SPLIT, SPLIT), SPLIT)

    def first_rows(q):
        return g_down.at[0, pl.ds(pl.multiple_of(q * ROWS + (ROWS - FIRST), 8), FIRST), :]

    f_own, f_par = gd.at[last, :], pmd.at[last, :]
    f_give = [pltpu.make_async_copy(first_rows(q), f_held.at[i], f_sem.at[i]) for i, q in enumerate((f_diag, f_core))]
    f_local = [pltpu.make_async_copy(first_rows(f_x), fo_own, f_sem.at[2]),
               pltpu.make_async_copy(first_rows(f), f_own, f_sem.at[3])]
    f_push = [remote(f_held.at[0], fo_par, f_send.at[0], f_recv.at[0], peer_core),
              remote(f_held.at[1], f_par, f_send.at[1], f_recv.at[1], peer_core)]
    f_state = [pltpu.make_async_copy(src.at[last, :], dst.at[last, :], st_sem.at[3 + i])
               for i, (src, dst) in enumerate(((down_w, wd), (down_m, md), (down_v, vd)))]
    f_scatter = [remote(fo_own.at[:, give], f_y, f_send.at[2], f_recv.at[2], peer_y),
                 remote(gd.at[last, give], yd.at[last, give], f_send.at[3], f_recv.at[3], peer_y)]
    f_cross = remote(fo_own.at[:, keep], xd.at[last, keep], f_send.at[4], f_recv.at[4], peer_x)
    f_gather = remote(gd.at[last, keep], yd.at[last, keep], f_send.at[5], f_recv.at[5], peer_y)
    me = dp * 4 + f
    sqf_copies = [remote(sq_first.at[me], sq_first.at[me], sqf_send.at[i], sqf_recv.at[i], peer)
                  for i, peer in enumerate(peers)]

    def norm_source(q):
        return g_norm.at[0, :, pl.ds(pl.multiple_of(q * NORM[1], 128), NORM[1])]

    n_push_other = remote(norm_source(f_diag), par_no, n_send.at[0], n_recv.at[0], peer_core)
    n_push_mine = remote(norm_source(f_core), pmn, n_send.at[1], n_recv.at[1], peer_core)
    n_x = remote(own_no, xn, n_send.at[2], n_recv.at[2], peer_x)
    n_y = remote(gn, yn, n_send.at[3], n_recv.at[3], peer_y)
    n_local = [pltpu.make_async_copy(src, dst, n_sem.at[i]) for i, (src, dst) in enumerate(
        ((norm_source(f_x), own_no), (norm_source(f), gn), (norm_w, wn), (norm_m, mn), (norm_v, vn)))]

    zero = Chunk("embed", 0)
    ahead = pltpu.make_async_copy(zero.source(grads, f_diag), pre, pre_sem)
    ahead.start()
    for copy in own_loads(0, zero):
        copy.start()
    for copy in f_give + f_local:
        copy.start()
    acc[...] = jnp.zeros_like(acc)

    barrier = pltpu.get_barrier_semaphore()
    for peer in peers:
        pl.semaphore_signal(barrier, inc=1, device_id=peer, device_id_type=MESH)
    ahead.wait()
    pl.semaphore_wait(barrier, len(peers))
    push_other(0, zero, pre).start()
    for copy, push in zip(f_give, f_push):
        copy.wait()
        push.start()
    push_mine(0, zero, zero.source(grads, f_core)).start()
    fetch(1)
    fetch(2)
    sum_chip(0)
    start_x(0)
    wait(f_local)
    wait(f_push)
    fo_own[...] = fo_own[...] + fo_par[...]
    f_own[...] = f_own[...] + f_par[...]
    start(f_scatter)
    start(f_state)

    def step(t, _):
        i = t - FETCH
        fetch(i + FETCH)

        @pl.when(i == 0)
        def _():
            n_push_other.start()
            n_push_mine.start()
            for copy in n_local:
                copy.start()

        sum_x(i)
        sum_chip(i + LEAD)
        start_y(i)
        start_x(i + LEAD)

        @pl.when(i == 3)
        def _():
            for copy in n_local:
                copy.wait()
            n_push_other.wait()
            n_push_mine.wait()
            own_no[...] = own_no[...] + par_no[...]
            n_x.start()

        @pl.when(i == 10)
        def _():
            n_x.wait()
            gn[...] = (gn[...] + pmn[...]) + xn[...]
            n_y.start()
            for copy in f_scatter:
                copy.wait()
            fo_own[:, keep] = fo_own[:, keep] + f_y[...]
            gd[last, keep] = gd[last, keep] + yd[last, keep]

        @pl.when(i == 20)
        def _():
            n_y.wait()
            mean = (gn[...] + yn[...]) * 0.125
            gn[...] = mean
            square = mean * mean
            total = square[:, 0:128]
            for c in range(1, NORM[1] // 128):
                total = total + square[:, c * 128:(c + 1) * 128]
            acc[0:4, :] += total

        @pl.when(i == N - LEAD)
        def _():
            f_cross.start()

        @pl.when(i == N + LAG - 2)
        def _():
            f_cross.wait()
            mean = (gd[last, keep] + xd[last, keep]) * 0.125
            gd[last, keep] = mean
            sq_first[me] = squares(mean, SPLIT)
            f_gather.start()
            for copy in sqf_copies:
                copy.start()

        sum_y(i - LAG)
        return 0

    lax.fori_loop(FETCH - LEAD + 1, FETCH + N + LAG, step, 0)

    sq_all[f] = acc[...]
    copies = [remote(sq_all.at[f], sq_all.at[f], sq_send.at[i], sq_recv.at[i], peer)
              for i, peer in enumerate((peer_core, peer_x, peer_diag))]
    for copy in copies:
        copy.start()

    def drain(k, _):
        on_chunk(k, lambda chunk: retire(k, chunk))
        return 0

    lax.fori_loop(N - RING, N, drain, 0)
    for i, ref in enumerate((w7, m7, v7, wd, md, vd)):
        pltpu.make_async_copy(ref, ref, st_sem.at[i]).wait()
    f_gather.wait()
    gd[last, give] = yd[last, give]
    for copy in sqf_copies:
        copy.wait()
    total = sq_first[0]
    for i in range(1, 8):
        total = total + sq_first[i]
    for copy in copies:
        copy.wait()
    sq_out[...] = ((sq_all[0] + sq_all[1]) + (sq_all[2] + sq_all[3])) + total


def update_math(avg_scale, sq_scale, g, w, m, v, decay):
    avg = ADAM_BETA1 * m + avg_scale * g
    root = sq_scale * g
    sq = ADAM_BETA2 * v + root * root
    dev = sq * lax.rsqrt(jnp.maximum(sq, SMALLEST))
    step_dir = avg / (dev + ADAM_EPS * ROOT_TWO)
    new = (1.0 - LEARN_RATE * decay) * w - (LEARN_RATE * ROOT_TWO / BIAS_ONE) * step_dir
    return new, avg, sq, new.astype(jnp.bfloat16)


def update_kernel(sq, g7, gd, gn, w7, m7, v7, wd, md, vd, wn, mn, vn,
                  lw, lm, lv, lb, dw, dm, dv, db, nw, nm, nv, nb, ew, em, ev, eb,
                  s7w, s7m, s7v, s7b, sdw, sdm, sdv, sdb, snw, snm, snv, snb, sem):
    total = jnp.sum(sq[...], keepdims=True)
    clip = jnp.minimum(1.0, 1.0 / (jnp.sqrt(total) + CLIP_EPS))
    scales = ((1.0 - ADAM_BETA1) * clip, math.sqrt(1.0 - ADAM_BETA2) * clip)

    outs = ((lw, lm, lv, lb), (dw, dm, dv, db), (nw, nm, nv, nb), (ew, em, ev, eb))
    seven_staged = (s7w, s7m, s7v, s7b)
    down_staged = (sdw, sdm, sdv, sdb)

    def layer_copies(j, row, rows):
        at = pl.ds(row, rows)
        return [pltpu.make_async_copy(src.at[j, at, :], dst.at[j, at, :], sem.at[0, a])
                for a, (src, dst) in enumerate(zip(seven_staged, outs[0]))]

    def embed_copies():
        return [pltpu.make_async_copy(src.at[6], dst, sem.at[1, a])
                for a, (src, dst) in enumerate(zip(seven_staged, outs[3]))]

    def down_copies(t):
        at = pl.ds(pl.multiple_of(t * 16, 16), 16)
        return [pltpu.make_async_copy(src.at[at, :], dst.at[at, :], sem.at[2, a])
                for a, (src, dst) in enumerate(zip(down_staged, outs[1]))]

    def seven(j, row, decay):
        for c in range(0, WIDTH, 512):
            ix = (j, pl.ds(row, 16), pl.ds(c, 512))
            out = update_math(*scales, g7[ix], w7[ix], m7[ix], v7[ix], decay)
            for ref, val in zip(seven_staged, out):
                ref[ix] = val

    def block(j, decay):
        def rows(t, _):
            seven(j, pl.multiple_of(t * 16, 16), decay)
            return 0

        lax.fori_loop(0, 4, rows, 0)

    def first_step(t, _):
        row = pl.multiple_of(t * 16, 16)
        seven(0, row, WEIGHT_DECAY)
        start(layer_copies(0, row, 16))
        return 0

    def half_step(t, _):
        seven(1, pl.multiple_of(t * 32, 32), WEIGHT_DECAY)
        seven(1, pl.multiple_of(t * 32 + 16, 16), WEIGHT_DECAY)
        start(layer_copies(1, pl.multiple_of(t * 32, 32), 32))
        return 0

    def layer_step(j, _):
        block(j, WEIGHT_DECAY)
        start(layer_copies(j, 0, ROWS))
        return 0

    def down_step(t, _):
        row = pl.multiple_of(t * 16, 16)

        def cols(u, _):
            ix = (pl.ds(row, 16), pl.ds(pl.multiple_of(u * 1024, 1024), 1024))
            out = update_math(*scales, gd[ix], wd[ix], md[ix], vd[ix], WEIGHT_DECAY)
            for ref, val in zip(down_staged, out):
                ref[ix] = val
            return 0

        lax.fori_loop(0, FF // 1024, cols, 0)
        start(down_copies(t))
        return 0

    lax.fori_loop(0, 4, first_step, 0)
    lax.fori_loop(0, 2, half_step, 0)
    lax.fori_loop(2, 6, layer_step, 0)
    out = update_math(*scales, gn[...], wn[...], mn[...], vn[...], WEIGHT_DECAY)
    for ref, val in zip((snw, snm, snv, snb), out):
        ref[...] = val
    norm_copies = [pltpu.make_async_copy(src, dst, sem.at[3, a])
                   for a, (src, dst) in enumerate(zip((snw, snm, snv, snb), outs[2]))]
    start(norm_copies)
    block(6, 0.0)
    start(embed_copies())
    lax.fori_loop(0, 4, down_step, 0)

    for a, staged in enumerate(seven_staged):
        pltpu.make_async_copy(staged.at[pl.ds(0, 6)], outs[0][a], sem.at[0, a]).wait()
    wait(embed_copies())
    wait(norm_copies)
    for a, staged in enumerate(down_staged):
        pltpu.make_async_copy(staged, outs[1][a], sem.at[2, a]).wait()


def local_update(g_layer, g_down, g_norm, g_embed, layer_w, layer_m, layer_v, down_w, down_m, down_v, norm_w, norm_m,
                 norm_v, embed_w, embed_m, embed_v):
    any_spec = pl.BlockSpec(memory_space=pl.ANY)
    vmem_spec = pl.BlockSpec(memory_space=pltpu.VMEM)
    dma = pltpu.SemaphoreType.DMA
    held = [(8, 128)] + [SEVEN, DOWN, NORM] + [SEVEN] * 3 + [DOWN] * 3 + [NORM] * 3
    reduced = pl.pallas_call(
        reduce_kernel,
        out_shape=[pltpu.VMEM(shape, F32) for shape in held],
        in_specs=[any_spec] * 16,
        out_specs=[vmem_spec] * len(held),
        scratch_shapes=[pltpu.VMEM((RING, 16, WIDTH), F32), pltpu.VMEM((RING, 16, WIDTH), F32)]
        + [pltpu.VMEM(SEVEN, F32), pltpu.VMEM(DOWN, F32)] * 3
        + [pltpu.VMEM(NORM, F32)] * 5
        + [pltpu.VMEM((8, 128), F32), pltpu.VMEM((4, 8, 128), F32), pltpu.VMEM((8, 8, 128), F32)]
        + [pltpu.VMEM((8, WIDTH), F32)] + [pltpu.VMEM((FIRST, FF), F32)] * 2
        + [pltpu.VMEM((2, FIRST, FF), F32), pltpu.VMEM((FIRST, SPLIT), F32)]
        + [dma((RING,)), dma((RING,)), dma((RING,)), dma((RING,)), dma((RING,)), dma((M_RING,)), dma((RING,)),
           dma((RING,)), dma((RING,)), dma((Y_RING,)), dma((6,)), dma((5,)), dma((4,)), dma((4,)), dma((3,)), dma((3,)),
           dma((7,)), dma((7,)), dma((4,)), dma((6,)), dma((6,)), dma,
           pltpu.SemaphoreType.REGULAR],
        compiler_params=pltpu.CompilerParams(collective_id=0, has_side_effects=True,
                                             vmem_limit_bytes=26 * 1024 * 1024),
    )(g_layer, g_down, g_norm, g_embed, layer_w, layer_m, layer_v, down_w, down_m, down_v, norm_w, norm_m, norm_v,
      embed_w, embed_m, embed_v)
    groups = ((6, ROWS, WIDTH), DOWN, NORM, (ROWS, WIDTH))
    out_shape = [jax.ShapeDtypeStruct(s, d) for s in groups for d in (F32, F32, F32, jnp.bfloat16)]
    staged = [pltpu.VMEM(s, d) for s in (SEVEN, DOWN, NORM) for d in (F32, F32, F32, jnp.bfloat16)]
    return pl.pallas_call(
        update_kernel,
        out_shape=out_shape,
        in_specs=[vmem_spec] * len(held),
        out_specs=[any_spec] * 16,
        scratch_shapes=staged + [dma((4, 4))],
        compiler_params=pltpu.CompilerParams(vmem_limit_bytes=26 * 1024 * 1024),
    )(*[pltpu.with_memory_space_constraint(a, pltpu.VMEM) for a in reduced])


def solution(mesh):
    grad_four = P(("dp", "fsdp"), None, None, None)
    grad_three = P(("dp", "fsdp"), None, None)
    layer_spec = P(None, "fsdp", None)
    down_spec = P("fsdp", None)
    norm_spec = P(None, "fsdp")
    embed_spec = P("fsdp", None)
    in_specs = (grad_four, grad_three, grad_three, grad_three,
                layer_spec, layer_spec, layer_spec, down_spec, down_spec, down_spec,
                norm_spec, norm_spec, norm_spec, embed_spec, embed_spec, embed_spec)
    out_specs = (layer_spec,) * 4 + (down_spec,) * 4 + (norm_spec,) * 4 + (embed_spec,) * 4
    return jax.shard_map(local_update, mesh=mesh, in_specs=in_specs, out_specs=out_specs, check_vma=False)
```

```python
import math

import jax
import jax.numpy as jnp
from jax import lax
from jax.experimental import pallas as pl
from jax.experimental.pallas import tpu as pltpu
from jax.sharding import PartitionSpec as P

ADAM_BETA1 = 0.9
ADAM_BETA2 = 0.95
ADAM_EPS = 1e-8
LEARN_RATE = 4e-4
WEIGHT_DECAY = 0.1
CLIP_EPS = 1e-6
OPT_STEP = 20
BIAS_ONE = 1.0 - ADAM_BETA1 ** OPT_STEP
BIAS_TWO = 1.0 - ADAM_BETA2 ** OPT_STEP
ROOT_TWO = math.sqrt(BIAS_TWO)
SMALLEST = 1.1754944e-38

MESH = pl.DeviceIdType.MESH
F32 = jnp.float32

ROWS = 64
WIDTH = 3072
FF = 8192
PIECE = 2048
NORM = (4, 768)
SEVEN = (7, ROWS, WIDTH)
DOWN = (ROWS, FF)

FIRST = 8
FIRST_COLS = 8192
SPLIT = FIRST_COLS // 2
LAYER_ROWS = 8
N_EMBED = ROWS // 8
N_LAYER = N_EMBED + 6 * (ROWS // LAYER_ROWS)
N_WIDE = N_LAYER + (FF // PIECE) * (ROWS // 16 - 1)
N = N_WIDE + (FF // PIECE) * 2 - FIRST_COLS // PIECE

RING = 7
Y_RING = 8
M_RING = 10
FETCH = 5
LEAD = 3
LAG = 3


class Chunk:
    def __init__(self, kind, k):
        self.kind = kind
        if kind == "embed":
            self.rows, self.width = 8, WIDTH
            self.row = pl.multiple_of(k * 8, 8)
        elif kind == "layer":
            q = k - N_EMBED
            per = ROWS // LAYER_ROWS
            self.rows, self.width = LAYER_ROWS, WIDTH
            self.j = q // per
            self.row = pl.multiple_of((q % per) * LAYER_ROWS, LAYER_ROWS)
        else:
            wide = kind == "wide"
            q = k - (N_LAYER if wide else N_WIDE)
            self.rows, self.width = (16, PIECE) if wide else (8, PIECE)
            start = 0 if wide else ROWS - 16
            self.row = pl.multiple_of(start + (q // 4) * self.rows, 8)
            self.cols = pl.ds(pl.multiple_of((q % 4) * PIECE, PIECE), PIECE)

    def source(self, grads, q):
        g_layer, g_down, g_embed = grads
        rows = pl.ds(pl.multiple_of(q * ROWS + self.row, 8), self.rows)
        if self.kind == "embed":
            return g_embed.at[0, rows, :]
        if self.kind == "layer":
            return g_layer.at[0, self.j, rows, :]
        return g_down.at[0, rows, self.cols]

    def state(self, layer, down, embed):
        rows = pl.ds(self.row, self.rows)
        if self.kind == "embed":
            return embed.at[rows, :]
        if self.kind == "layer":
            return layer.at[self.j, rows, :]
        return down.at[rows, self.cols]

    def held(self, seven, down):
        rows = pl.ds(self.row, self.rows)
        if self.kind == "embed":
            return seven.at[6, rows, :]
        if self.kind == "layer":
            return seven.at[self.j, rows, :]
        return down.at[rows, self.cols]

    def ring(self, ring, s):
        return ring.at[s, pl.ds(0, self.rows), pl.ds(0, self.width)]


def on_chunk(k, use):
    if isinstance(k, int):
        use(Chunk("embed", k))
        return
    bounds = (0, N_EMBED, N_LAYER, N_WIDE, N)
    for i, kind in enumerate(("embed", "layer", "wide", "down")):
        @pl.when(jnp.logical_and(k >= bounds[i], k < bounds[i + 1]))
        def _():
            use(Chunk(kind, k))


def start(copies):
    for copy in copies:
        copy.start()


def wait(copies):
    for copy in copies:
        copy.wait()


def squares(mean, width):
    parts = [mean[r:r + 8, i * 128:(i + 1) * 128] for r in range(0, mean.shape[0], 8) for i in range(width // 128)]
    sums = [p * p for p in parts[:4]]
    for i, p in enumerate(parts[4:]):
        sums[i % 4] = sums[i % 4] + p * p
    return (sums[0] + sums[1]) + (sums[2] + sums[3])


def reduce_kernel(g_layer, g_down, g_norm, g_embed, layer_w, layer_m, layer_v, down_w, down_m, down_v,
                  norm_w, norm_m, norm_v, embed_w, embed_m, embed_v,
                  sq_out, g7, gd, gn, w7, m7, v7, wd, md, vd, wn, mn, vn,
                  own_o, par_o, pm7, pmd, x7, xd, y7, yd, own_no, par_no, pmn, xn, yn, acc, sq_all, sq_first,
                  pre, fo_own, fo_par, f_held, f_y,
                  own_o_sem, own_m_sem, do_send, do_recv, dm_send, dm_recv, x_send, x_recv, y_send, y_recv,
                  st_sem, n_sem, n_send, n_recv, sq_send, sq_recv, sqf_send, sqf_recv, f_sem, f_send, f_recv, pre_sem, credit):
    dp = lax.axis_index("dp")
    f = lax.axis_index("fsdp")
    core = lax.rem(f, 2)
    f_core = f + 1 - 2 * core
    f_x = lax.rem(f + 2, 4)
    f_diag = lax.rem(f_core + 2, 4)
    peer_core = (dp, f_core)
    peer_x = (dp, f_x)
    peer_diag = (dp, f_diag)
    peer_y = (1 - dp, f)
    peers = (peer_core, peer_x, peer_diag, peer_y, (1 - dp, f_core), (1 - dp, f_x), (1 - dp, f_diag))

    def remote(src, dst, send, recv, peer):
        return pltpu.make_async_remote_copy(src_ref=src, dst_ref=dst, send_sem=send, recv_sem=recv,
                                            device_id=peer, device_id_type=MESH)

    grads = (g_layer, g_down, g_embed)

    def x_copy(k, chunk):
        s = lax.rem(k, RING)
        return remote(chunk.ring(own_o, s), chunk.held(x7, xd), x_send.at[s], x_recv.at[s], peer_x)

    def y_copy(k, chunk):
        s = lax.rem(k, RING)
        return remote(chunk.held(g7, gd), chunk.held(y7, yd), y_send.at[s], y_recv.at[lax.rem(k, Y_RING)], peer_y)

    def push_other(k, chunk, source):
        s = lax.rem(k, RING)
        return remote(source, chunk.ring(par_o, s), do_send.at[s], do_recv.at[s], peer_core)

    def push_mine(k, chunk, source):
        s = lax.rem(k, RING)
        return remote(source, chunk.held(pm7, pmd), dm_send.at[s], dm_recv.at[lax.rem(k, M_RING)], peer_core)

    def own_loads(k, chunk):
        s = lax.rem(k, RING)
        return [pltpu.make_async_copy(chunk.source(grads, f_x), chunk.ring(own_o, s), own_o_sem.at[s]),
                pltpu.make_async_copy(chunk.source(grads, f), chunk.held(g7, gd), own_m_sem.at[s])]

    def retire(k, chunk):
        s = lax.rem(k, RING)
        x_copy(k, chunk).wait_send()
        push_other(k, chunk, chunk.ring(par_o, s)).wait_send()
        push_mine(k, chunk, chunk.held(pm7, pmd)).wait_send()

    def fetch(k):
        @pl.when(jnp.logical_and(k >= RING, k < N))
        def _():
            on_chunk(k - RING, lambda chunk: retire(k - RING, chunk))
            pl.semaphore_wait(credit, 1)

        def begin(chunk):
            push_other(k, chunk, chunk.source(grads, f_diag)).start()
            for copy in own_loads(k, chunk):
                copy.start()
            push_mine(k, chunk, chunk.source(grads, f_core)).start()

        on_chunk(k, begin)

    def sum_x(k):
        s = lax.rem(k, RING)

        def use(chunk):
            mine = chunk.held(g7, gd)
            theirs = chunk.held(pm7, pmd)
            pltpu.make_async_copy(mine, mine, own_m_sem.at[s]).wait()
            push_mine(k, chunk, theirs).wait_recv()
            x_copy(k, chunk).wait_recv()
            mine[...] = (mine[...] + theirs[...]) + chunk.held(x7, xd)[...]

        on_chunk(k, use)

    def sum_chip(k):
        s = lax.rem(k, RING)

        def use(chunk):
            mine = chunk.ring(own_o, s)
            theirs = chunk.ring(par_o, s)
            pltpu.make_async_copy(mine, mine, own_o_sem.at[s]).wait()
            push_other(k, chunk, theirs).wait_recv()
            mine[...] = mine[...] + theirs[...]

        on_chunk(k, use)

    def start_x(k):
        on_chunk(k, lambda chunk: x_copy(k, chunk).start())

        @pl.when(jnp.logical_and(k >= 0, k < N - RING))
        def _():
            pl.semaphore_signal(credit, inc=1, device_id=peer_core, device_id_type=MESH)

    def start_y(k):
        def use(chunk):
            y_copy(k, chunk).start()
            seven = chunk.kind in ("embed", "layer")
            for i, (src, dst) in enumerate((((layer_w, down_w, embed_w), (w7, wd)), ((layer_m, down_m, embed_m), (m7, md)),
                                            ((layer_v, down_v, embed_v), (v7, vd)))):
                pltpu.make_async_copy(chunk.state(*src), chunk.held(*dst), st_sem.at[i if seven else 3 + i]).start()

        on_chunk(k, use)

    def sum_y(k):
        def use(chunk):
            y_copy(k, chunk).wait()
            mine = chunk.held(g7, gd)
            mean = (mine[...] + chunk.held(y7, yd)[...]) * 0.125
            mine[...] = mean
            acc[...] += squares(mean, chunk.width)

        on_chunk(k, use)

    last = pl.ds(ROWS - FIRST, FIRST)
    keep = pl.ds(pl.multiple_of(FF - FIRST_COLS + dp * SPLIT, PIECE // 2), SPLIT)
    give = pl.ds(pl.multiple_of(FF - FIRST_COLS + (1 - dp) * SPLIT, PIECE // 2), SPLIT)
    cols = pl.ds(FF - FIRST_COLS, FIRST_COLS)
    keep_o = pl.ds(pl.multiple_of(dp * SPLIT, PIECE // 2), SPLIT)
    give_o = pl.ds(pl.multiple_of((1 - dp) * SPLIT, PIECE // 2), SPLIT)

    def first_rows(q):
        return g_down.at[0, pl.ds(pl.multiple_of(q * ROWS + (ROWS - FIRST), 8), FIRST), cols]

    f_own = gd.at[last, cols]
    f_give = [pltpu.make_async_copy(first_rows(q), f_held.at[i], f_sem.at[i]) for i, q in enumerate((f_diag, f_core))]
    f_local = [pltpu.make_async_copy(first_rows(f_x), fo_own, f_sem.at[2]),
               pltpu.make_async_copy(first_rows(f), f_own, f_sem.at[3])]
    f_push = []
    for h, (half, half_o) in enumerate(((give, give_o), (keep, keep_o))):
        for i, ref in enumerate((fo_par.at[:, half_o], pmd.at[last, half])):
            f_push.append(remote(f_held.at[i, :, half_o], ref, f_send.at[4 + 2 * h + i], f_recv.at[4 + 2 * h + i],
                                 peer_core))
    f_state = [pltpu.make_async_copy(src.at[last, cols], dst.at[last, cols], st_sem.at[3 + i])
               for i, (src, dst) in enumerate(((down_w, wd), (down_m, md), (down_v, vd)))]
    f_scatter = [remote(fo_own.at[:, give_o], f_y, f_send.at[0], f_recv.at[0], peer_y),
                 remote(gd.at[last, give], yd.at[last, give], f_send.at[1], f_recv.at[1], peer_y)]
    f_cross = remote(fo_own.at[:, keep_o], xd.at[last, keep], f_send.at[2], f_recv.at[2], peer_x)
    f_gather = remote(gd.at[last, keep], yd.at[last, keep], f_send.at[3], f_recv.at[3], peer_y)
    me = dp * 4 + f
    sqf_copies = [remote(sq_first.at[me], sq_first.at[me], sqf_send.at[i], sqf_recv.at[i], peer)
                  for i, peer in enumerate(peers)]

    def norm_source(q):
        return g_norm.at[0, :, pl.ds(pl.multiple_of(q * NORM[1], 128), NORM[1])]

    n_push_other = remote(norm_source(f_diag), par_no, n_send.at[0], n_recv.at[0], peer_core)
    n_push_mine = remote(norm_source(f_core), pmn, n_send.at[1], n_recv.at[1], peer_core)
    n_x = remote(own_no, xn, n_send.at[2], n_recv.at[2], peer_x)
    n_y = remote(gn, yn, n_send.at[3], n_recv.at[3], peer_y)
    n_local = [pltpu.make_async_copy(src, dst, n_sem.at[i]) for i, (src, dst) in enumerate(
        ((norm_source(f_x), own_no), (norm_source(f), gn), (norm_w, wn), (norm_m, mn), (norm_v, vn)))]

    zero = Chunk("embed", 0)
    ahead = pltpu.make_async_copy(zero.source(grads, f_diag), pre, pre_sem)
    ahead.start()
    for copy in own_loads(0, zero):
        copy.start()
    for copy in f_give + f_local:
        copy.start()
    acc[...] = jnp.zeros_like(acc)

    barrier = pltpu.get_barrier_semaphore()
    near = (peer_core, peer_x, peer_y)
    for peer in near:
        pl.semaphore_signal(barrier, inc=1, device_id=peer, device_id_type=MESH)
    wait(f_give)
    pl.semaphore_wait(barrier, len(near))
    start(f_push[:2])
    ahead.wait()
    push_other(0, zero, pre).start()
    start(f_push[2:])
    push_mine(0, zero, zero.source(grads, f_core)).start()
    fetch(1)
    fetch(2)
    wait(f_local)
    wait(f_push[:1])
    fo_own[:, give_o] = fo_own[:, give_o] + fo_par[:, give_o]
    f_scatter[0].start()
    wait(f_push[1:2])
    gd[last, give] = gd[last, give] + pmd[last, give]
    f_scatter[1].start()
    sum_chip(0)
    start_x(0)
    wait(f_push[2:])
    fo_own[:, keep_o] = fo_own[:, keep_o] + fo_par[:, keep_o]
    gd[last, keep] = gd[last, keep] + pmd[last, keep]
    start(f_state)

    def step(t, _):
        i = t - FETCH
        fetch(i + FETCH)

        @pl.when(i == 0)
        def _():
            n_push_other.start()
            n_push_mine.start()
            for copy in n_local:
                copy.start()

        sum_x(i)
        sum_chip(i + LEAD)
        start_y(i)
        start_x(i + LEAD)

        @pl.when(i == 3)
        def _():
            for copy in n_local:
                copy.wait()
            n_push_other.wait()
            n_push_mine.wait()
            own_no[...] = own_no[...] + par_no[...]
            n_x.start()

        @pl.when(i == 10)
        def _():
            n_x.wait()
            gn[...] = (gn[...] + pmn[...]) + xn[...]
            n_y.start()
            for copy in f_scatter:
                copy.wait()
            fo_own[:, keep_o] = fo_own[:, keep_o] + f_y[...]
            gd[last, keep] = gd[last, keep] + yd[last, keep]

        @pl.when(i == 20)
        def _():
            n_y.wait()
            mean = (gn[...] + yn[...]) * 0.125
            gn[...] = mean
            square = mean * mean
            total = square[:, 0:128]
            for c in range(1, NORM[1] // 128):
                total = total + square[:, c * 128:(c + 1) * 128]
            acc[0:4, :] += total

        @pl.when(i == N - LEAD)
        def _():
            f_cross.start()

        @pl.when(i == N + LAG - 2)
        def _():
            f_cross.wait()
            mean = (gd[last, keep] + xd[last, keep]) * 0.125
            gd[last, keep] = mean
            sq_first[me] = squares(mean, SPLIT)
            start(sqf_copies)
            f_gather.start()

        sum_y(i - LAG)
        return 0

    lax.fori_loop(FETCH - LEAD + 1, FETCH + N + LAG, step, 0)

    sq_all[f] = acc[...]
    copies = [remote(sq_all.at[f], sq_all.at[f], sq_send.at[i], sq_recv.at[i], peer)
              for i, peer in enumerate((peer_core, peer_x, peer_diag))]
    for copy in copies:
        copy.start()

    def drain(k, _):
        on_chunk(k, lambda chunk: retire(k, chunk))
        return 0

    lax.fori_loop(N - RING, N, drain, 0)
    for i, ref in enumerate((w7, m7, v7, wd, md, vd)):
        pltpu.make_async_copy(ref, ref, st_sem.at[i]).wait()
    f_gather.wait()
    gd[last, give] = yd[last, give]
    for copy in sqf_copies:
        copy.wait()
    total = sq_first[0]
    for i in range(1, 8):
        total = total + sq_first[i]
    for copy in copies:
        copy.wait()
    sq_out[...] = ((sq_all[0] + sq_all[1]) + (sq_all[2] + sq_all[3])) + total


def update_math(avg_scale, sq_scale, g, w, m, v, decay):
    avg = ADAM_BETA1 * m + avg_scale * g
    root = sq_scale * g
    sq = ADAM_BETA2 * v + root * root
    dev = sq * lax.rsqrt(jnp.maximum(sq, SMALLEST))
    step_dir = avg / (dev + ADAM_EPS * ROOT_TWO)
    new = (1.0 - LEARN_RATE * decay) * w - (LEARN_RATE * ROOT_TWO / BIAS_ONE) * step_dir
    return new, avg, sq, new.astype(jnp.bfloat16)


def update_kernel(sq, g7, gd, gn, w7, m7, v7, wd, md, vd, wn, mn, vn,
                  lw, lm, lv, lb, dw, dm, dv, db, nw, nm, nv, nb, ew, em, ev, eb,
                  s7w, s7m, s7v, s7b, sdw, sdm, sdv, sdb, snw, snm, snv, snb, sem):
    total = jnp.sum(sq[...], keepdims=True)
    clip = jnp.minimum(1.0, 1.0 / (jnp.sqrt(total) + CLIP_EPS))
    scales = ((1.0 - ADAM_BETA1) * clip, math.sqrt(1.0 - ADAM_BETA2) * clip)

    outs = ((lw, lm, lv, lb), (dw, dm, dv, db), (nw, nm, nv, nb), (ew, em, ev, eb))
    seven_staged = (s7w, s7m, s7v, s7b)
    down_staged = (sdw, sdm, sdv, sdb)

    def layer_copies(j, row, rows):
        at = pl.ds(row, rows)
        return [pltpu.make_async_copy(src.at[j, at, :], dst.at[j, at, :], sem.at[0, a])
                for a, (src, dst) in enumerate(zip(seven_staged, outs[0]))]

    def embed_copies():
        return [pltpu.make_async_copy(src.at[6], dst, sem.at[1, a])
                for a, (src, dst) in enumerate(zip(seven_staged, outs[3]))]

    def down_copies(t):
        at = pl.ds(pl.multiple_of(t * 16, 16), 16)
        return [pltpu.make_async_copy(src.at[at, :], dst.at[at, :], sem.at[2, a])
                for a, (src, dst) in enumerate(zip(down_staged, outs[1]))]

    def seven(j, row, decay):
        for c in range(0, WIDTH, 512):
            ix = (j, pl.ds(row, 16), pl.ds(c, 512))
            out = update_math(*scales, g7[ix], w7[ix], m7[ix], v7[ix], decay)
            for ref, val in zip(seven_staged, out):
                ref[ix] = val

    def block(j, decay):
        def rows(t, _):
            seven(j, pl.multiple_of(t * 16, 16), decay)
            return 0

        lax.fori_loop(0, 4, rows, 0)

    def first_step(t, _):
        row = pl.multiple_of(t * 16, 16)
        seven(0, row, WEIGHT_DECAY)
        start(layer_copies(0, row, 16))
        return 0

    def half_step(t, _):
        seven(1, pl.multiple_of(t * 32, 32), WEIGHT_DECAY)
        seven(1, pl.multiple_of(t * 32 + 16, 16), WEIGHT_DECAY)
        start(layer_copies(1, pl.multiple_of(t * 32, 32), 32))
        return 0

    def layer_step(j, _):
        block(j, WEIGHT_DECAY)
        start(layer_copies(j, 0, ROWS))
        return 0

    def down_step(t, _):
        row = pl.multiple_of(t * 16, 16)

        def cols(u, _):
            ix = (pl.ds(row, 16), pl.ds(pl.multiple_of(u * 1024, 1024), 1024))
            out = update_math(*scales, gd[ix], wd[ix], md[ix], vd[ix], WEIGHT_DECAY)
            for ref, val in zip(down_staged, out):
                ref[ix] = val
            return 0

        lax.fori_loop(0, FF // 1024, cols, 0)
        start(down_copies(t))
        return 0

    lax.fori_loop(0, 4, first_step, 0)
    lax.fori_loop(0, 2, half_step, 0)
    lax.fori_loop(2, 6, layer_step, 0)
    out = update_math(*scales, gn[...], wn[...], mn[...], vn[...], WEIGHT_DECAY)
    for ref, val in zip((snw, snm, snv, snb), out):
        ref[...] = val
    norm_copies = [pltpu.make_async_copy(src, dst, sem.at[3, a])
                   for a, (src, dst) in enumerate(zip((snw, snm, snv, snb), outs[2]))]
    start(norm_copies)
    block(6, 0.0)
    start(embed_copies())
    lax.fori_loop(0, 4, down_step, 0)

    for a, staged in enumerate(seven_staged):
        pltpu.make_async_copy(staged.at[pl.ds(0, 6)], outs[0][a], sem.at[0, a]).wait()
    wait(embed_copies())
    wait(norm_copies)
    for a, staged in enumerate(down_staged):
        pltpu.make_async_copy(staged, outs[1][a], sem.at[2, a]).wait()


def local_update(g_layer, g_down, g_norm, g_embed, layer_w, layer_m, layer_v, down_w, down_m, down_v, norm_w, norm_m,
                 norm_v, embed_w, embed_m, embed_v):
    any_spec = pl.BlockSpec(memory_space=pl.ANY)
    vmem_spec = pl.BlockSpec(memory_space=pltpu.VMEM)
    dma = pltpu.SemaphoreType.DMA
    held = [(8, 128)] + [SEVEN, DOWN, NORM] + [SEVEN] * 3 + [DOWN] * 3 + [NORM] * 3
    reduced = pl.pallas_call(
        reduce_kernel,
        out_shape=[pltpu.VMEM(shape, F32) for shape in held],
        in_specs=[any_spec] * 16,
        out_specs=[vmem_spec] * len(held),
        scratch_shapes=[pltpu.VMEM((RING, 16, WIDTH), F32), pltpu.VMEM((RING, 16, WIDTH), F32)]
        + [pltpu.VMEM(SEVEN, F32), pltpu.VMEM(DOWN, F32)] * 3
        + [pltpu.VMEM(NORM, F32)] * 5
        + [pltpu.VMEM((8, 128), F32), pltpu.VMEM((4, 8, 128), F32), pltpu.VMEM((8, 8, 128), F32)]
        + [pltpu.VMEM((8, WIDTH), F32)] + [pltpu.VMEM((FIRST, FIRST_COLS), F32)] * 2
        + [pltpu.VMEM((2, FIRST, FIRST_COLS), F32), pltpu.VMEM((FIRST, SPLIT), F32)]
        + [dma((RING,)), dma((RING,)), dma((RING,)), dma((RING,)), dma((RING,)), dma((M_RING,)), dma((RING,)),
           dma((RING,)), dma((RING,)), dma((Y_RING,)), dma((6,)), dma((5,)), dma((4,)), dma((4,)), dma((3,)), dma((3,)),
           dma((7,)), dma((7,)), dma((4,)), dma((8,)), dma((8,)), dma,
           pltpu.SemaphoreType.REGULAR],
        compiler_params=pltpu.CompilerParams(collective_id=0, has_side_effects=True,
                                             vmem_limit_bytes=26 * 1024 * 1024),
    )(g_layer, g_down, g_norm, g_embed, layer_w, layer_m, layer_v, down_w, down_m, down_v, norm_w, norm_m, norm_v,
      embed_w, embed_m, embed_v)
    groups = ((6, ROWS, WIDTH), DOWN, NORM, (ROWS, WIDTH))
    out_shape = [jax.ShapeDtypeStruct(s, d) for s in groups for d in (F32, F32, F32, jnp.bfloat16)]
    staged = [pltpu.VMEM(s, d) for s in (SEVEN, DOWN, NORM) for d in (F32, F32, F32, jnp.bfloat16)]
    return pl.pallas_call(
        update_kernel,
        out_shape=out_shape,
        in_specs=[vmem_spec] * len(held),
        out_specs=[any_spec] * 16,
        scratch_shapes=staged + [dma((4, 4))],
        compiler_params=pltpu.CompilerParams(vmem_limit_bytes=26 * 1024 * 1024),
    )(*[pltpu.with_memory_space_constraint(a, pltpu.VMEM) for a in reduced])


def solution(mesh):
    grad_four = P(("dp", "fsdp"), None, None, None)
    grad_three = P(("dp", "fsdp"), None, None)
    layer_spec = P(None, "fsdp", None)
    down_spec = P("fsdp", None)
    norm_spec = P(None, "fsdp")
    embed_spec = P("fsdp", None)
    in_specs = (grad_four, grad_three, grad_three, grad_three,
                layer_spec, layer_spec, layer_spec, down_spec, down_spec, down_spec,
                norm_spec, norm_spec, norm_spec, embed_spec, embed_spec, embed_spec)
    out_specs = (layer_spec,) * 4 + (down_spec,) * 4 + (norm_spec,) * 4 + (embed_spec,) * 4
    return jax.shard_map(local_update, mesh=mesh, in_specs=in_specs, out_specs=out_specs, check_vma=False)
```

```python
import math

import jax
import jax.numpy as jnp
from jax import lax
from jax.experimental import pallas as pl
from jax.experimental.pallas import tpu as pltpu
from jax.sharding import PartitionSpec as P

ADAM_BETA1 = 0.9
ADAM_BETA2 = 0.95
ADAM_EPS = 1e-8
LEARN_RATE = 4e-4
WEIGHT_DECAY = 0.1
CLIP_EPS = 1e-6
OPT_STEP = 20
BIAS_ONE = 1.0 - ADAM_BETA1 ** OPT_STEP
BIAS_TWO = 1.0 - ADAM_BETA2 ** OPT_STEP
ROOT_TWO = math.sqrt(BIAS_TWO)
SMALLEST = 1.1754944e-38

MESH = pl.DeviceIdType.MESH
F32 = jnp.float32

ROWS = 64
WIDTH = 3072
FF = 8192
PIECE = 2048
NORM = (4, 768)
SEVEN = (7, ROWS, WIDTH)
DOWN = (ROWS, FF)

FIRST = 8
FIRST_COLS = 6144
SPLIT = FIRST_COLS // 2
PART = 1536
BLOCK = (ROWS // 8) * (WIDTH // PART)
N_EMBED = BLOCK
N_LAYER = N_EMBED + 6 * BLOCK
N = N_LAYER + (FF // PIECE) * (ROWS // 8) - FIRST_COLS // PIECE

LEAD = 4
FETCH = 7
RING = 9
LAG = 5
Y_RING = 2 * LAG + 2
M_RING = RING + LEAD


class Chunk:
    def __init__(self, kind, k):
        self.kind = kind
        if kind == "down":
            q = k - N_LAYER
            per = FF // PIECE
            self.width = PIECE
        else:
            q = k if kind == "embed" else (k - N_EMBED) % BLOCK
            per = WIDTH // PART
            self.width = PART
            self.j = 6 if kind == "embed" else (k - N_EMBED) // BLOCK
        self.row = pl.multiple_of((q // per) * 8, 8)
        self.rows = pl.ds(self.row, 8)
        self.cols = pl.ds(pl.multiple_of((q % per) * self.width, 512), self.width)

    def source(self, grads, q):
        g_layer, g_down, g_embed = grads
        rows = pl.ds(pl.multiple_of(q * ROWS + self.row, 8), 8)
        if self.kind == "embed":
            return g_embed.at[0, rows, self.cols]
        if self.kind == "layer":
            return g_layer.at[0, self.j, rows, self.cols]
        return g_down.at[0, rows, self.cols]

    def state(self, layer, down, embed):
        if self.kind == "embed":
            return embed.at[self.rows, self.cols]
        if self.kind == "layer":
            return layer.at[self.j, self.rows, self.cols]
        return down.at[self.rows, self.cols]

    def held(self, seven, down):
        if self.kind == "down":
            return down.at[self.rows, self.cols]
        return seven.at[self.j, self.rows, self.cols]

    def ring(self, ring, s):
        return ring.at[s, :, pl.ds(0, self.width)]


def on_chunk(k, use):
    if isinstance(k, int):
        use(Chunk("embed", k))
        return
    bounds = (0, N_EMBED, N_LAYER, N)
    for i, kind in enumerate(("embed", "layer", "down")):
        @pl.when(jnp.logical_and(k >= bounds[i], k < bounds[i + 1]))
        def _():
            use(Chunk(kind, k))


def start(copies):
    for copy in copies:
        copy.start()


def wait(copies):
    for copy in copies:
        copy.wait()


def squares(mean, width):
    parts = [mean[r:r + 8, i * 128:(i + 1) * 128] for r in range(0, mean.shape[0], 8) for i in range(width // 128)]
    sums = [p * p for p in parts[:4]]
    for i, p in enumerate(parts[4:]):
        sums[i % 4] = sums[i % 4] + p * p
    return (sums[0] + sums[1]) + (sums[2] + sums[3])


def reduce_kernel(g_layer, g_down, g_norm, g_embed, layer_w, layer_m, layer_v, down_w, down_m, down_v,
                  norm_w, norm_m, norm_v, embed_w, embed_m, embed_v,
                  sq_out, g7, gd, gn, w7, m7, v7, wd, md, vd, wn, mn, vn,
                  own_o, par_o, pm7, pmd, x7, xd, y7, yd, own_no, par_no, pmn, xn, yn, acc, sq_all, sq_first,
                  pre, fo_own, fo_par, f_held, f_y,
                  own_o_sem, own_m_sem, do_send, do_recv, dm_send, dm_recv, x_send, x_recv, y_send, y_recv,
                  st_sem, n_sem, n_send, n_recv, sq_send, sq_recv, sqf_send, sqf_recv, f_sem, f_send, f_recv, pre_sem, credit):
    dp = lax.axis_index("dp")
    f = lax.axis_index("fsdp")
    core = lax.rem(f, 2)
    f_core = f + 1 - 2 * core
    f_x = lax.rem(f + 2, 4)
    f_diag = lax.rem(f_core + 2, 4)
    peer_core = (dp, f_core)
    peer_x = (dp, f_x)
    peer_diag = (dp, f_diag)
    peer_y = (1 - dp, f)
    peers = (peer_core, peer_x, peer_diag, peer_y, (1 - dp, f_core), (1 - dp, f_x), (1 - dp, f_diag))

    def remote(src, dst, send, recv, peer):
        return pltpu.make_async_remote_copy(src_ref=src, dst_ref=dst, send_sem=send, recv_sem=recv,
                                            device_id=peer, device_id_type=MESH)

    grads = (g_layer, g_down, g_embed)

    def x_copy(k, chunk):
        s = lax.rem(k, RING)
        return remote(chunk.ring(own_o, s), chunk.held(x7, xd), x_send.at[s], x_recv.at[s], peer_x)

    def y_copy(k, chunk):
        s = lax.rem(k, RING)
        return remote(chunk.held(g7, gd), chunk.held(y7, yd), y_send.at[s], y_recv.at[lax.rem(k, Y_RING)], peer_y)

    def push_other(k, chunk, source):
        s = lax.rem(k, RING)
        return remote(source, chunk.ring(par_o, s), do_send.at[s], do_recv.at[s], peer_core)

    def push_mine(k, chunk, source):
        s = lax.rem(k, RING)
        return remote(source, chunk.held(pm7, pmd), dm_send.at[s], dm_recv.at[lax.rem(k, M_RING)], peer_core)

    def own_loads(k, chunk):
        s = lax.rem(k, RING)
        return [pltpu.make_async_copy(chunk.source(grads, f_x), chunk.ring(own_o, s), own_o_sem.at[s]),
                pltpu.make_async_copy(chunk.source(grads, f), chunk.held(g7, gd), own_m_sem.at[s])]

    def retire(k, chunk):
        s = lax.rem(k, RING)
        x_copy(k, chunk).wait_send()
        push_other(k, chunk, chunk.ring(par_o, s)).wait_send()
        push_mine(k, chunk, chunk.held(pm7, pmd)).wait_send()

    def fetch(k):
        @pl.when(jnp.logical_and(k >= RING, k < N))
        def _():
            on_chunk(k - RING, lambda chunk: retire(k - RING, chunk))
            pl.semaphore_wait(credit, 1)

        def begin(chunk):
            push_other(k, chunk, chunk.source(grads, f_diag)).start()
            for copy in own_loads(k, chunk):
                copy.start()
            push_mine(k, chunk, chunk.source(grads, f_core)).start()

        on_chunk(k, begin)

    def sum_x(k):
        s = lax.rem(k, RING)

        def use(chunk):
            mine = chunk.held(g7, gd)
            theirs = chunk.held(pm7, pmd)
            pltpu.make_async_copy(mine, mine, own_m_sem.at[s]).wait()
            push_mine(k, chunk, theirs).wait_recv()
            x_copy(k, chunk).wait_recv()
            mine[...] = (mine[...] + theirs[...]) + chunk.held(x7, xd)[...]

        on_chunk(k, use)

    def sum_chip(k):
        s = lax.rem(k, RING)

        def use(chunk):
            mine = chunk.ring(own_o, s)
            theirs = chunk.ring(par_o, s)
            pltpu.make_async_copy(mine, mine, own_o_sem.at[s]).wait()
            push_other(k, chunk, theirs).wait_recv()
            mine[...] = mine[...] + theirs[...]

        on_chunk(k, use)

    def start_x(k):
        on_chunk(k, lambda chunk: x_copy(k, chunk).start())

        @pl.when(jnp.logical_and(k >= 0, k < N - RING))
        def _():
            pl.semaphore_signal(credit, inc=1, device_id=peer_core, device_id_type=MESH)

    def start_y(k):
        def use(chunk):
            y_copy(k, chunk).start()
            seven = chunk.kind in ("embed", "layer")
            for i, (src, dst) in enumerate((((layer_w, down_w, embed_w), (w7, wd)), ((layer_m, down_m, embed_m), (m7, md)),
                                            ((layer_v, down_v, embed_v), (v7, vd)))):
                pltpu.make_async_copy(chunk.state(*src), chunk.held(*dst), st_sem.at[i if seven else 3 + i]).start()

        on_chunk(k, use)

    def sum_y(k):
        def use(chunk):
            y_copy(k, chunk).wait()
            mine = chunk.held(g7, gd)
            mean = (mine[...] + chunk.held(y7, yd)[...]) * 0.125
            mine[...] = mean
            acc[...] += squares(mean, chunk.width)

        on_chunk(k, use)

    last = pl.ds(ROWS - FIRST, FIRST)
    keep = pl.ds(pl.multiple_of(FF - FIRST_COLS + dp * SPLIT, PIECE // 2), SPLIT)
    give = pl.ds(pl.multiple_of(FF - FIRST_COLS + (1 - dp) * SPLIT, PIECE // 2), SPLIT)
    cols = pl.ds(FF - FIRST_COLS, FIRST_COLS)
    keep_o = pl.ds(pl.multiple_of(dp * SPLIT, PIECE // 2), SPLIT)
    give_o = pl.ds(pl.multiple_of((1 - dp) * SPLIT, PIECE // 2), SPLIT)

    def first_rows(q):
        return g_down.at[0, pl.ds(pl.multiple_of(q * ROWS + (ROWS - FIRST), 8), FIRST), cols]

    f_own = gd.at[last, cols]
    f_give = [pltpu.make_async_copy(first_rows(q), f_held.at[i], f_sem.at[i]) for i, q in enumerate((f_diag, f_core))]
    f_local = [pltpu.make_async_copy(first_rows(f_x), fo_own, f_sem.at[2]),
               pltpu.make_async_copy(first_rows(f), f_own, f_sem.at[3])]
    f_push = []
    for h, (half, half_o) in enumerate(((give, give_o), (keep, keep_o))):
        for i, ref in enumerate((fo_par.at[:, half_o], pmd.at[last, half])):
            f_push.append(remote(f_held.at[i, :, half_o], ref, f_send.at[4 + 2 * h + i], f_recv.at[4 + 2 * h + i],
                                 peer_core))
    f_state = [pltpu.make_async_copy(src.at[last, cols], dst.at[last, cols], st_sem.at[3 + i])
               for i, (src, dst) in enumerate(((down_w, wd), (down_m, md), (down_v, vd)))]
    f_scatter = [remote(fo_own.at[:, give_o], f_y, f_send.at[0], f_recv.at[0], peer_y),
                 remote(gd.at[last, give], yd.at[last, give], f_send.at[1], f_recv.at[1], peer_y)]
    f_cross = remote(fo_own.at[:, keep_o], xd.at[last, keep], f_send.at[2], f_recv.at[2], peer_x)
    f_gather = remote(gd.at[last, keep], yd.at[last, keep], f_send.at[3], f_recv.at[3], peer_y)
    me = dp * 4 + f
    sqf_copies = [remote(sq_first.at[me], sq_first.at[me], sqf_send.at[i], sqf_recv.at[i], peer)
                  for i, peer in enumerate(peers)]

    def norm_source(q):
        return g_norm.at[0, :, pl.ds(pl.multiple_of(q * NORM[1], 128), NORM[1])]

    n_push_other = remote(norm_source(f_diag), par_no, n_send.at[0], n_recv.at[0], peer_core)
    n_push_mine = remote(norm_source(f_core), pmn, n_send.at[1], n_recv.at[1], peer_core)
    n_x = remote(own_no, xn, n_send.at[2], n_recv.at[2], peer_x)
    n_y = remote(gn, yn, n_send.at[3], n_recv.at[3], peer_y)
    n_local = [pltpu.make_async_copy(src, dst, n_sem.at[i]) for i, (src, dst) in enumerate(
        ((norm_source(f_x), own_no), (norm_source(f), gn), (norm_w, wn), (norm_m, mn), (norm_v, vn)))]

    zero = Chunk("embed", 0)
    ahead = pltpu.make_async_copy(zero.source(grads, f_diag), pre, pre_sem)
    ahead.start()
    for copy in own_loads(0, zero):
        copy.start()
    for copy in f_give + f_local:
        copy.start()
    acc[...] = jnp.zeros_like(acc)

    barrier = pltpu.get_barrier_semaphore()
    near = (peer_core, peer_x, peer_y)
    for peer in near:
        pl.semaphore_signal(barrier, inc=1, device_id=peer, device_id_type=MESH)
    wait(f_give)
    pl.semaphore_wait(barrier, len(near))
    start(f_push[:2])
    ahead.wait()
    push_other(0, zero, pre).start()
    start(f_push[2:])
    push_mine(0, zero, zero.source(grads, f_core)).start()
    for k in range(1, FETCH - LEAD + 1):
        fetch(k)
    wait(f_local)
    wait(f_push[:1])
    fo_own[:, give_o] = fo_own[:, give_o] + fo_par[:, give_o]
    f_scatter[0].start()
    wait(f_push[1:2])
    gd[last, give] = gd[last, give] + pmd[last, give]
    f_scatter[1].start()
    sum_chip(0)
    start_x(0)
    wait(f_push[2:])
    fo_own[:, keep_o] = fo_own[:, keep_o] + fo_par[:, keep_o]
    gd[last, keep] = gd[last, keep] + pmd[last, keep]
    start(f_state)

    def step(t, _):
        i = t - FETCH
        fetch(i + FETCH)

        @pl.when(i == 0)
        def _():
            n_push_other.start()
            n_push_mine.start()
            for copy in n_local:
                copy.start()

        sum_x(i)
        sum_chip(i + LEAD)
        start_y(i)
        start_x(i + LEAD)

        @pl.when(i == 3)
        def _():
            for copy in n_local:
                copy.wait()
            n_push_other.wait()
            n_push_mine.wait()
            own_no[...] = own_no[...] + par_no[...]
            n_x.start()

        @pl.when(i == 10)
        def _():
            n_x.wait()
            gn[...] = (gn[...] + pmn[...]) + xn[...]
            n_y.start()
            for copy in f_scatter:
                copy.wait()
            fo_own[:, keep_o] = fo_own[:, keep_o] + f_y[...]
            gd[last, keep] = gd[last, keep] + yd[last, keep]

        @pl.when(i == 20)
        def _():
            n_y.wait()
            mean = (gn[...] + yn[...]) * 0.125
            gn[...] = mean
            square = mean * mean
            total = square[:, 0:128]
            for c in range(1, NORM[1] // 128):
                total = total + square[:, c * 128:(c + 1) * 128]
            acc[0:4, :] += total

        @pl.when(i == N - LEAD)
        def _():
            f_cross.start()

        @pl.when(i == N + LAG - 2)
        def _():
            f_cross.wait()
            mean = (gd[last, keep] + xd[last, keep]) * 0.125
            gd[last, keep] = mean
            sq_first[me] = squares(mean, SPLIT)
            start(sqf_copies)
            f_gather.start()

        sum_y(i - LAG)
        return 0

    lax.fori_loop(FETCH - LEAD + 1, FETCH + N + LAG, step, 0)

    sq_all[f] = acc[...]
    copies = [remote(sq_all.at[f], sq_all.at[f], sq_send.at[i], sq_recv.at[i], peer)
              for i, peer in enumerate((peer_core, peer_x, peer_diag))]
    for copy in copies:
        copy.start()

    def drain(k, _):
        on_chunk(k, lambda chunk: retire(k, chunk))
        return 0

    lax.fori_loop(N - RING, N, drain, 0)
    for i, ref in enumerate((w7, m7, v7, wd, md, vd)):
        pltpu.make_async_copy(ref, ref, st_sem.at[i]).wait()
    f_gather.wait()
    gd[last, give] = yd[last, give]
    for copy in sqf_copies:
        copy.wait()
    total = sq_first[0]
    for i in range(1, 8):
        total = total + sq_first[i]
    for copy in copies:
        copy.wait()
    sq_out[...] = ((sq_all[0] + sq_all[1]) + (sq_all[2] + sq_all[3])) + total


def update_math(avg_scale, sq_scale, g, w, m, v, decay):
    avg = ADAM_BETA1 * m + avg_scale * g
    root = sq_scale * g
    sq = ADAM_BETA2 * v + root * root
    dev = sq * lax.rsqrt(jnp.maximum(sq, SMALLEST))
    step_dir = avg / (dev + ADAM_EPS * ROOT_TWO)
    new = (1.0 - LEARN_RATE * decay) * w - (LEARN_RATE * ROOT_TWO / BIAS_ONE) * step_dir
    return new, avg, sq, new.astype(jnp.bfloat16)


def update_kernel(sq, g7, gd, gn, w7, m7, v7, wd, md, vd, wn, mn, vn,
                  lw, lm, lv, lb, dw, dm, dv, db, nw, nm, nv, nb, ew, em, ev, eb,
                  s7w, s7m, s7v, s7b, sdw, sdm, sdv, sdb, snw, snm, snv, snb, sem):
    total = jnp.sum(sq[...], keepdims=True)
    clip = jnp.minimum(1.0, 1.0 / (jnp.sqrt(total) + CLIP_EPS))
    scales = ((1.0 - ADAM_BETA1) * clip, math.sqrt(1.0 - ADAM_BETA2) * clip)

    outs = ((lw, lm, lv, lb), (dw, dm, dv, db), (nw, nm, nv, nb), (ew, em, ev, eb))
    seven_staged = (s7w, s7m, s7v, s7b)
    down_staged = (sdw, sdm, sdv, sdb)

    def layer_copies(j, row, rows):
        at = pl.ds(row, rows)
        return [pltpu.make_async_copy(src.at[j, at, :], dst.at[j, at, :], sem.at[0, a])
                for a, (src, dst) in enumerate(zip(seven_staged, outs[0]))]

    def embed_copies():
        return [pltpu.make_async_copy(src.at[6], dst, sem.at[1, a])
                for a, (src, dst) in enumerate(zip(seven_staged, outs[3]))]

    def down_copies(t):
        at = pl.ds(pl.multiple_of(t * 16, 16), 16)
        return [pltpu.make_async_copy(src.at[at, :], dst.at[at, :], sem.at[2, a])
                for a, (src, dst) in enumerate(zip(down_staged, outs[1]))]

    def seven(j, row, decay):
        for c in range(0, WIDTH, 512):
            ix = (j, pl.ds(row, 16), pl.ds(c, 512))
            out = update_math(*scales, g7[ix], w7[ix], m7[ix], v7[ix], decay)
            for ref, val in zip(seven_staged, out):
                ref[ix] = val

    def block(j, decay):
        def rows(t, _):
            seven(j, pl.multiple_of(t * 16, 16), decay)
            return 0

        lax.fori_loop(0, 4, rows, 0)

    def first_step(t, _):
        row = pl.multiple_of(t * 16, 16)
        seven(0, row, WEIGHT_DECAY)
        start(layer_copies(0, row, 16))
        return 0

    def half_step(t, _):
        seven(1, pl.multiple_of(t * 32, 32), WEIGHT_DECAY)
        seven(1, pl.multiple_of(t * 32 + 16, 16), WEIGHT_DECAY)
        start(layer_copies(1, pl.multiple_of(t * 32, 32), 32))
        return 0

    def layer_step(j, _):
        block(j, WEIGHT_DECAY)
        start(layer_copies(j, 0, ROWS))
        return 0

    def down_step(t, _):
        row = pl.multiple_of(t * 16, 16)

        def cols(u, _):
            ix = (pl.ds(row, 16), pl.ds(pl.multiple_of(u * 1024, 1024), 1024))
            out = update_math(*scales, gd[ix], wd[ix], md[ix], vd[ix], WEIGHT_DECAY)
            for ref, val in zip(down_staged, out):
                ref[ix] = val
            return 0

        lax.fori_loop(0, FF // 1024, cols, 0)
        start(down_copies(t))
        return 0

    lax.fori_loop(0, 4, first_step, 0)
    lax.fori_loop(0, 2, half_step, 0)
    lax.fori_loop(2, 6, layer_step, 0)
    out = update_math(*scales, gn[...], wn[...], mn[...], vn[...], WEIGHT_DECAY)
    for ref, val in zip((snw, snm, snv, snb), out):
        ref[...] = val
    norm_copies = [pltpu.make_async_copy(src, dst, sem.at[3, a])
                   for a, (src, dst) in enumerate(zip((snw, snm, snv, snb), outs[2]))]
    start(norm_copies)
    block(6, 0.0)
    start(embed_copies())
    lax.fori_loop(0, 4, down_step, 0)

    for a, staged in enumerate(seven_staged):
        pltpu.make_async_copy(staged.at[pl.ds(0, 6)], outs[0][a], sem.at[0, a]).wait()
    wait(embed_copies())
    wait(norm_copies)
    for a, staged in enumerate(down_staged):
        pltpu.make_async_copy(staged, outs[1][a], sem.at[2, a]).wait()


def local_update(g_layer, g_down, g_norm, g_embed, layer_w, layer_m, layer_v, down_w, down_m, down_v, norm_w, norm_m,
                 norm_v, embed_w, embed_m, embed_v):
    any_spec = pl.BlockSpec(memory_space=pl.ANY)
    vmem_spec = pl.BlockSpec(memory_space=pltpu.VMEM)
    dma = pltpu.SemaphoreType.DMA
    held = [(8, 128)] + [SEVEN, DOWN, NORM] + [SEVEN] * 3 + [DOWN] * 3 + [NORM] * 3
    reduced = pl.pallas_call(
        reduce_kernel,
        out_shape=[pltpu.VMEM(shape, F32) for shape in held],
        in_specs=[any_spec] * 16,
        out_specs=[vmem_spec] * len(held),
        scratch_shapes=[pltpu.VMEM((RING, 8, max(PART, PIECE)), F32)] * 2
        + [pltpu.VMEM(SEVEN, F32), pltpu.VMEM(DOWN, F32)] * 3
        + [pltpu.VMEM(NORM, F32)] * 5
        + [pltpu.VMEM((8, 128), F32), pltpu.VMEM((4, 8, 128), F32), pltpu.VMEM((8, 8, 128), F32)]
        + [pltpu.VMEM((8, PART), F32)] + [pltpu.VMEM((FIRST, FIRST_COLS), F32)] * 2
        + [pltpu.VMEM((2, FIRST, FIRST_COLS), F32), pltpu.VMEM((FIRST, SPLIT), F32)]
        + [dma((RING,)), dma((RING,)), dma((RING,)), dma((RING,)), dma((RING,)), dma((M_RING,)), dma((RING,)),
           dma((RING,)), dma((RING,)), dma((Y_RING,)), dma((6,)), dma((5,)), dma((4,)), dma((4,)), dma((3,)), dma((3,)),
           dma((7,)), dma((7,)), dma((4,)), dma((8,)), dma((8,)), dma,
           pltpu.SemaphoreType.REGULAR],
        compiler_params=pltpu.CompilerParams(collective_id=0, has_side_effects=True,
                                             vmem_limit_bytes=26 * 1024 * 1024),
    )(g_layer, g_down, g_norm, g_embed, layer_w, layer_m, layer_v, down_w, down_m, down_v, norm_w, norm_m, norm_v,
      embed_w, embed_m, embed_v)
    groups = ((6, ROWS, WIDTH), DOWN, NORM, (ROWS, WIDTH))
    out_shape = [jax.ShapeDtypeStruct(s, d) for s in groups for d in (F32, F32, F32, jnp.bfloat16)]
    staged = [pltpu.VMEM(s, d) for s in (SEVEN, DOWN, NORM) for d in (F32, F32, F32, jnp.bfloat16)]
    return pl.pallas_call(
        update_kernel,
        out_shape=out_shape,
        in_specs=[vmem_spec] * len(held),
        out_specs=[any_spec] * 16,
        scratch_shapes=staged + [dma((4, 4))],
        compiler_params=pltpu.CompilerParams(vmem_limit_bytes=26 * 1024 * 1024),
    )(*[pltpu.with_memory_space_constraint(a, pltpu.VMEM) for a in reduced])


def solution(mesh):
    grad_four = P(("dp", "fsdp"), None, None, None)
    grad_three = P(("dp", "fsdp"), None, None)
    layer_spec = P(None, "fsdp", None)
    down_spec = P("fsdp", None)
    norm_spec = P(None, "fsdp")
    embed_spec = P("fsdp", None)
    in_specs = (grad_four, grad_three, grad_three, grad_three,
                layer_spec, layer_spec, layer_spec, down_spec, down_spec, down_spec,
                norm_spec, norm_spec, norm_spec, embed_spec, embed_spec, embed_spec)
    out_specs = (layer_spec,) * 4 + (down_spec,) * 4 + (norm_spec,) * 4 + (embed_spec,) * 4
    return jax.shard_map(local_update, mesh=mesh, in_specs=in_specs, out_specs=out_specs, check_vma=False)
```

```python
import math

import jax
import jax.numpy as jnp
from jax import lax
from jax.experimental import pallas as pl
from jax.experimental.pallas import tpu as pltpu
from jax.sharding import PartitionSpec as P

ADAM_BETA1 = 0.9
ADAM_BETA2 = 0.95
ADAM_EPS = 1e-8
LEARN_RATE = 4e-4
WEIGHT_DECAY = 0.1
CLIP_EPS = 1e-6
OPT_STEP = 20
BIAS_ONE = 1.0 - ADAM_BETA1 ** OPT_STEP
BIAS_TWO = 1.0 - ADAM_BETA2 ** OPT_STEP
ROOT_TWO = math.sqrt(BIAS_TWO)
SMALLEST = 1.1754944e-38

MESH = pl.DeviceIdType.MESH
F32 = jnp.float32

ROWS = 64
WIDTH = 3072
FF = 8192
PIECE = 2048
NORM = (4, 768)
SEVEN = (7, ROWS, WIDTH)
DOWN = (ROWS, FF)

FIRST = 8
FIRST_COLS = 6144
SPLIT = FIRST_COLS // 2
PART = 1536
BLOCK = (ROWS // 8) * (WIDTH // PART)
N_EMBED = BLOCK
N_LAYER = N_EMBED + 6 * BLOCK
N = N_LAYER + (FF // PIECE) * (ROWS // 8) - FIRST_COLS // PIECE

LEAD = 4
FETCH = 7
RING = 9
LAG = 5
Y_RING = 2 * LAG + 2
M_RING = RING + LEAD


class Chunk:
    def __init__(self, kind, k):
        self.kind = kind
        if kind == "down":
            q = k - N_LAYER
            per = FF // PIECE
            self.width = PIECE
        else:
            q = k if kind == "embed" else (k - N_EMBED) % BLOCK
            per = WIDTH // PART
            self.width = PART
            self.j = 6 if kind == "embed" else (k - N_EMBED) // BLOCK
        self.row = pl.multiple_of((q // per) * 8, 8)
        self.rows = pl.ds(self.row, 8)
        self.cols = pl.ds(pl.multiple_of((q % per) * self.width, 512), self.width)

    def source(self, grads, q):
        g_layer, g_down, g_embed = grads
        rows = pl.ds(pl.multiple_of(q * ROWS + self.row, 8), 8)
        if self.kind == "embed":
            return g_embed.at[0, rows, self.cols]
        if self.kind == "layer":
            return g_layer.at[0, self.j, rows, self.cols]
        return g_down.at[0, rows, self.cols]

    def state(self, layer, down, embed):
        if self.kind == "embed":
            return embed.at[self.rows, self.cols]
        if self.kind == "layer":
            return layer.at[self.j, self.rows, self.cols]
        return down.at[self.rows, self.cols]

    def held(self, seven, down):
        if self.kind == "down":
            return down.at[self.rows, self.cols]
        return seven.at[self.j, self.rows, self.cols]

    def ring(self, ring, s):
        return ring.at[s, :, pl.ds(0, self.width)]


def on_chunk(k, use):
    if isinstance(k, int):
        use(Chunk("embed", k))
        return
    bounds = (0, N_EMBED, N_LAYER, N)
    for i, kind in enumerate(("embed", "layer", "down")):
        @pl.when(jnp.logical_and(k >= bounds[i], k < bounds[i + 1]))
        def _():
            use(Chunk(kind, k))


def start(copies):
    for copy in copies:
        copy.start()


def wait(copies):
    for copy in copies:
        copy.wait()


def take(ref, sem):
    pltpu.make_async_copy(ref, ref, sem).wait()


def squares(mean, width):
    parts = [mean[r:r + 8, i * 128:(i + 1) * 128] for r in range(0, mean.shape[0], 8) for i in range(width // 128)]
    sums = [p * p for p in parts[:4]]
    for i, p in enumerate(parts[4:]):
        sums[i % 4] = sums[i % 4] + p * p
    return (sums[0] + sums[1]) + (sums[2] + sums[3])


def reduce_kernel(g_layer, g_down, g_norm, g_embed, layer_w, layer_m, layer_v, down_w, down_m, down_v,
                  norm_w, norm_m, norm_v, embed_w, embed_m, embed_v,
                  sq_out, g7, gd, gn, w7, m7, v7, wd, md, vd, wn, mn, vn,
                  own_o, par_o, pm7, pmd, x7, xd, y7, yd, own_no, par_no, pmn, xn, yn, acc, sq_all, sq_first,
                  pre, fo_own, fo_par, f_held, f_y,
                  out_sem, other_sem, mine_sem, y_sem, st_sem, n_sem, sq_sem, f_sem, pre_sem, credit):
    dp = lax.axis_index("dp")
    f = lax.axis_index("fsdp")
    core = lax.rem(f, 2)
    f_core = f + 1 - 2 * core
    f_x = lax.rem(f + 2, 4)
    f_diag = lax.rem(f_core + 2, 4)
    peer_core = (dp, f_core)
    peer_x = (dp, f_x)
    peer_diag = (dp, f_diag)
    peer_y = (1 - dp, f)
    peers = (peer_core, peer_x, peer_diag, peer_y, (1 - dp, f_core), (1 - dp, f_x), (1 - dp, f_diag))

    def remote(src, dst, send, recv, peer):
        return pltpu.make_async_remote_copy(src_ref=src, dst_ref=dst, send_sem=send, recv_sem=recv,
                                            device_id=peer, device_id_type=MESH)

    grads = (g_layer, g_down, g_embed)

    def x_copy(k, chunk):
        s = lax.rem(k, RING)
        return remote(chunk.ring(own_o, s), chunk.held(x7, xd), out_sem.at[s], mine_sem.at[lax.rem(k, M_RING)], peer_x)

    def y_copy(k, chunk):
        sem = y_sem.at[lax.rem(k, Y_RING)]
        return remote(chunk.held(g7, gd), chunk.held(y7, yd), sem, sem, peer_y)

    def push_other(k, chunk, source):
        s = lax.rem(k, RING)
        return remote(source, chunk.ring(par_o, s), out_sem.at[s], other_sem.at[s], peer_core)

    def push_mine(k, chunk, source):
        s = lax.rem(k, RING)
        return remote(source, chunk.held(pm7, pmd), out_sem.at[s], mine_sem.at[lax.rem(k, M_RING)], peer_core)

    def own_loads(k, chunk):
        s = lax.rem(k, RING)
        return [pltpu.make_async_copy(chunk.source(grads, f_x), chunk.ring(own_o, s), other_sem.at[s]),
                pltpu.make_async_copy(chunk.source(grads, f), chunk.held(g7, gd), mine_sem.at[lax.rem(k, M_RING)])]

    def times(count, chunk):
        return own_o.at[pl.ds(0, count), :, pl.ds(0, chunk.width)]

    def retire(k, chunk):
        take(times(3, chunk), out_sem.at[lax.rem(k, RING)])

    def fetch(k):
        @pl.when(jnp.logical_and(k >= RING, k < N))
        def _():
            on_chunk(k - RING, lambda chunk: retire(k - RING, chunk))
            pl.semaphore_wait(credit, 1)

        def begin(chunk):
            push_other(k, chunk, chunk.source(grads, f_diag)).start()
            for copy in own_loads(k, chunk):
                copy.start()
            push_mine(k, chunk, chunk.source(grads, f_core)).start()

        on_chunk(k, begin)

    def sum_x(k):
        def use(chunk):
            take(times(3, chunk), mine_sem.at[lax.rem(k, M_RING)])
            mine = chunk.held(g7, gd)
            theirs = chunk.held(pm7, pmd)
            mine[...] = (mine[...] + theirs[...]) + chunk.held(x7, xd)[...]

        on_chunk(k, use)

    def sum_chip(k):
        s = lax.rem(k, RING)

        def use(chunk):
            mine = chunk.ring(own_o, s)
            theirs = chunk.ring(par_o, s)
            take(times(2, chunk), other_sem.at[s])
            mine[...] = mine[...] + theirs[...]

        on_chunk(k, use)

    def start_x(k):
        on_chunk(k, lambda chunk: x_copy(k, chunk).start())

        @pl.when(jnp.logical_and(k >= 0, k < N - RING))
        def _():
            pl.semaphore_signal(credit, inc=1, device_id=peer_core, device_id_type=MESH)

    def start_y(k):
        def use(chunk):
            y_copy(k, chunk).start()
            seven = chunk.kind in ("embed", "layer")
            for i, (src, dst) in enumerate((((layer_w, down_w, embed_w), (w7, wd)), ((layer_m, down_m, embed_m), (m7, md)),
                                            ((layer_v, down_v, embed_v), (v7, vd)))):
                pltpu.make_async_copy(chunk.state(*src), chunk.held(*dst), st_sem.at[i if seven else 3 + i]).start()

        on_chunk(k, use)

    def sum_y(k):
        def use(chunk):
            take(times(2, chunk), y_sem.at[lax.rem(k, Y_RING)])
            mine = chunk.held(g7, gd)
            mean = (mine[...] + chunk.held(y7, yd)[...]) * 0.125
            mine[...] = mean
            acc[...] += squares(mean, chunk.width)

        on_chunk(k, use)

    last = pl.ds(ROWS - FIRST, FIRST)
    keep = pl.ds(pl.multiple_of(FF - FIRST_COLS + dp * SPLIT, PIECE // 2), SPLIT)
    give = pl.ds(pl.multiple_of(FF - FIRST_COLS + (1 - dp) * SPLIT, PIECE // 2), SPLIT)
    cols = pl.ds(FF - FIRST_COLS, FIRST_COLS)
    keep_o = pl.ds(pl.multiple_of(dp * SPLIT, PIECE // 2), SPLIT)
    give_o = pl.ds(pl.multiple_of((1 - dp) * SPLIT, PIECE // 2), SPLIT)

    def first_rows(q):
        return g_down.at[0, pl.ds(pl.multiple_of(q * ROWS + (ROWS - FIRST), 8), FIRST), cols]

    f_own = gd.at[last, cols]
    f_give = [pltpu.make_async_copy(first_rows(q), f_held.at[i], f_sem.at[0]) for i, q in enumerate((f_diag, f_core))]
    f_local = [pltpu.make_async_copy(first_rows(f_x), fo_own, f_sem.at[1]),
               pltpu.make_async_copy(first_rows(f), f_own, f_sem.at[1])]
    f_push = []
    for h, (half, half_o) in enumerate(((give, give_o), (keep, keep_o))):
        for i, ref in enumerate((fo_par.at[:, half_o], pmd.at[last, half])):
            f_push.append(remote(f_held.at[i, :, half_o], ref, f_sem.at[2],
                                 f_sem.at[3 + i] if h == 0 else f_sem.at[5], peer_core))
    f_state = [pltpu.make_async_copy(src.at[last, cols], dst.at[last, cols], st_sem.at[3 + i])
               for i, (src, dst) in enumerate(((down_w, wd), (down_m, md), (down_v, vd)))]
    f_scatter = [remote(fo_own.at[:, give_o], f_y, f_sem.at[6], f_sem.at[6], peer_y),
                 remote(gd.at[last, give], yd.at[last, give], f_sem.at[6], f_sem.at[6], peer_y)]
    f_cross = remote(fo_own.at[:, keep_o], xd.at[last, keep], f_sem.at[7], f_sem.at[7], peer_x)
    f_gather = remote(gd.at[last, keep], yd.at[last, keep], f_sem.at[8], f_sem.at[8], peer_y)
    me = dp * 4 + f
    sqf_copies = [remote(sq_first.at[me], sq_first.at[me], sq_sem.at[0], sq_sem.at[1], peer)
                  for peer in peers]

    def norm_source(q):
        return g_norm.at[0, :, pl.ds(pl.multiple_of(q * NORM[1], 128), NORM[1])]

    n_push_other = remote(norm_source(f_diag), par_no, n_sem.at[1], n_sem.at[0], peer_core)
    n_push_mine = remote(norm_source(f_core), pmn, n_sem.at[1], n_sem.at[0], peer_core)
    n_x = remote(own_no, xn, n_sem.at[2], n_sem.at[2], peer_x)
    n_y = remote(gn, yn, n_sem.at[3], n_sem.at[3], peer_y)
    n_local = [pltpu.make_async_copy(src, dst, n_sem.at[0]) for src, dst in
               ((norm_source(f_x), own_no), (norm_source(f), gn), (norm_w, wn), (norm_m, mn), (norm_v, vn))]

    def n_times(count):
        return fo_par.at[:, pl.ds(0, count * NORM[0] * NORM[1] // 8)]


    zero = Chunk("embed", 0)
    ahead = pltpu.make_async_copy(zero.source(grads, f_diag), pre, pre_sem)
    ahead.start()
    for copy in own_loads(0, zero):
        copy.start()
    for copy in f_give + f_local:
        copy.start()
    acc[...] = jnp.zeros_like(acc)

    barrier = pltpu.get_barrier_semaphore()
    near = (peer_core, peer_x, peer_y)
    for peer in near:
        pl.semaphore_signal(barrier, inc=1, device_id=peer, device_id_type=MESH)
    take(f_held, f_sem.at[0])
    pl.semaphore_wait(barrier, len(near))
    start(f_push[:2])
    ahead.wait()
    push_other(0, zero, pre).start()
    start(f_push[2:])
    push_mine(0, zero, zero.source(grads, f_core)).start()
    for k in range(1, FETCH - LEAD + 1):
        fetch(k)
    take(f_held, f_sem.at[1])
    take(fo_par.at[:, give_o], f_sem.at[3])
    fo_own[:, give_o] = fo_own[:, give_o] + fo_par[:, give_o]
    f_scatter[0].start()
    take(fo_par.at[:, give_o], f_sem.at[4])
    gd[last, give] = gd[last, give] + pmd[last, give]
    f_scatter[1].start()
    sum_chip(0)
    start_x(0)
    take(fo_par, f_sem.at[5])
    take(f_held, f_sem.at[2])
    fo_own[:, keep_o] = fo_own[:, keep_o] + fo_par[:, keep_o]
    gd[last, keep] = gd[last, keep] + pmd[last, keep]
    start(f_state)

    def step(t, _):
        i = t - FETCH
        fetch(i + FETCH)

        @pl.when(i == 0)
        def _():
            n_push_other.start()
            n_push_mine.start()
            for copy in n_local:
                copy.start()

        sum_x(i)
        sum_chip(i + LEAD)
        start_y(i)
        start_x(i + LEAD)

        @pl.when(i == 3)
        def _():
            take(n_times(7), n_sem.at[0])
            take(n_times(2), n_sem.at[1])
            own_no[...] = own_no[...] + par_no[...]
            n_x.start()

        @pl.when(i == 10)
        def _():
            take(n_times(2), n_sem.at[2])
            gn[...] = (gn[...] + pmn[...]) + xn[...]
            n_y.start()
            take(f_held, f_sem.at[6])
            fo_own[:, keep_o] = fo_own[:, keep_o] + f_y[...]
            gd[last, keep] = gd[last, keep] + yd[last, keep]

        @pl.when(i == 20)
        def _():
            take(n_times(2), n_sem.at[3])
            mean = (gn[...] + yn[...]) * 0.125
            gn[...] = mean
            square = mean * mean
            total = square[:, 0:128]
            for c in range(1, NORM[1] // 128):
                total = total + square[:, c * 128:(c + 1) * 128]
            acc[0:4, :] += total

        @pl.when(i == N - LEAD)
        def _():
            f_cross.start()

        @pl.when(i == N + LAG - 3)
        def _():
            take(fo_par, f_sem.at[7])
            mean = (gd[last, keep] + xd[last, keep]) * 0.125
            gd[last, keep] = mean
            sq_first[me] = squares(mean, SPLIT)
            start(sqf_copies)
            f_gather.start()

        sum_y(i - LAG)
        return 0

    lax.fori_loop(FETCH - LEAD + 1, FETCH + N + LAG, step, 0)

    sq_all[f] = acc[...]
    copies = [remote(sq_all.at[f], sq_all.at[f], sq_sem.at[2], sq_sem.at[3], peer)
              for peer in (peer_core, peer_x, peer_diag)]
    for copy in copies:
        copy.start()

    def drain(k, _):
        on_chunk(k, lambda chunk: retire(k, chunk))
        return 0

    lax.fori_loop(N - RING, N, drain, 0)
    for i, ref in enumerate((w7, m7, v7, wd, md, vd)):
        pltpu.make_async_copy(ref, ref, st_sem.at[i]).wait()
    take(fo_par, f_sem.at[8])
    gd[last, give] = yd[last, give]
    take(sq_first.at[pl.ds(0, 7)], sq_sem.at[0])
    take(sq_first.at[pl.ds(0, 7)], sq_sem.at[1])
    total = sq_first[0]
    for i in range(1, 8):
        total = total + sq_first[i]
    take(sq_all.at[pl.ds(0, 3)], sq_sem.at[2])
    take(sq_all.at[pl.ds(0, 3)], sq_sem.at[3])
    sq_out[...] = ((sq_all[0] + sq_all[1]) + (sq_all[2] + sq_all[3])) + total


def update_math(avg_scale, sq_scale, g, w, m, v, decay):
    avg = ADAM_BETA1 * m + avg_scale * g
    root = sq_scale * g
    sq = ADAM_BETA2 * v + root * root
    dev = sq * lax.rsqrt(jnp.maximum(sq, SMALLEST))
    step_dir = avg / (dev + ADAM_EPS * ROOT_TWO)
    new = (1.0 - LEARN_RATE * decay) * w - (LEARN_RATE * ROOT_TWO / BIAS_ONE) * step_dir
    return new, avg, sq, new.astype(jnp.bfloat16)


def update_kernel(sq, g7, gd, gn, w7, m7, v7, wd, md, vd, wn, mn, vn,
                  lw, lm, lv, lb, dw, dm, dv, db, nw, nm, nv, nb, ew, em, ev, eb,
                  s7w, s7m, s7v, s7b, sdw, sdm, sdv, sdb, snw, snm, snv, snb, sem):
    total = jnp.sum(sq[...], keepdims=True)
    clip = jnp.minimum(1.0, 1.0 / (jnp.sqrt(total) + CLIP_EPS))
    scales = ((1.0 - ADAM_BETA1) * clip, math.sqrt(1.0 - ADAM_BETA2) * clip)

    outs = ((lw, lm, lv, lb), (dw, dm, dv, db), (nw, nm, nv, nb), (ew, em, ev, eb))
    seven_staged = (s7w, s7m, s7v, s7b)
    down_staged = (sdw, sdm, sdv, sdb)

    def layer_copies(j, row, rows):
        at = pl.ds(row, rows)
        return [pltpu.make_async_copy(src.at[j, at, :], dst.at[j, at, :], sem.at[0, a])
                for a, (src, dst) in enumerate(zip(seven_staged, outs[0]))]

    def embed_copies():
        return [pltpu.make_async_copy(src.at[6], dst, sem.at[1, a])
                for a, (src, dst) in enumerate(zip(seven_staged, outs[3]))]

    def down_copies(t):
        at = pl.ds(pl.multiple_of(t * 16, 16), 16)
        return [pltpu.make_async_copy(src.at[at, :], dst.at[at, :], sem.at[2, a])
                for a, (src, dst) in enumerate(zip(down_staged, outs[1]))]

    def seven(j, row, decay):
        for c in range(0, WIDTH, 512):
            ix = (j, pl.ds(row, 16), pl.ds(c, 512))
            out = update_math(*scales, g7[ix], w7[ix], m7[ix], v7[ix], decay)
            for ref, val in zip(seven_staged, out):
                ref[ix] = val

    def block(j, decay):
        def rows(t, _):
            seven(j, pl.multiple_of(t * 16, 16), decay)
            return 0

        lax.fori_loop(0, 4, rows, 0)

    def first_step(t, _):
        row = pl.multiple_of(t * 16, 16)
        seven(0, row, WEIGHT_DECAY)
        start(layer_copies(0, row, 16))
        return 0

    def half_step(t, _):
        seven(1, pl.multiple_of(t * 32, 32), WEIGHT_DECAY)
        seven(1, pl.multiple_of(t * 32 + 16, 16), WEIGHT_DECAY)
        start(layer_copies(1, pl.multiple_of(t * 32, 32), 32))
        return 0

    def layer_step(j, _):
        block(j, WEIGHT_DECAY)
        start(layer_copies(j, 0, ROWS))
        return 0

    def down_step(t, _):
        row = pl.multiple_of(t * 16, 16)

        def cols(u, _):
            ix = (pl.ds(row, 16), pl.ds(pl.multiple_of(u * 1024, 1024), 1024))
            out = update_math(*scales, gd[ix], wd[ix], md[ix], vd[ix], WEIGHT_DECAY)
            for ref, val in zip(down_staged, out):
                ref[ix] = val
            return 0

        lax.fori_loop(0, FF // 1024, cols, 0)
        start(down_copies(t))
        return 0

    lax.fori_loop(0, 4, first_step, 0)
    lax.fori_loop(0, 2, half_step, 0)
    lax.fori_loop(2, 6, layer_step, 0)
    out = update_math(*scales, gn[...], wn[...], mn[...], vn[...], WEIGHT_DECAY)
    for ref, val in zip((snw, snm, snv, snb), out):
        ref[...] = val
    norm_copies = [pltpu.make_async_copy(src, dst, sem.at[3, a])
                   for a, (src, dst) in enumerate(zip((snw, snm, snv, snb), outs[2]))]
    start(norm_copies)
    block(6, 0.0)
    start(embed_copies())
    lax.fori_loop(0, 4, down_step, 0)

    for a, staged in enumerate(seven_staged):
        pltpu.make_async_copy(staged.at[pl.ds(0, 6)], outs[0][a], sem.at[0, a]).wait()
    wait(embed_copies())
    wait(norm_copies)
    for a, staged in enumerate(down_staged):
        pltpu.make_async_copy(staged, outs[1][a], sem.at[2, a]).wait()


def local_update(g_layer, g_down, g_norm, g_embed, layer_w, layer_m, layer_v, down_w, down_m, down_v, norm_w, norm_m,
                 norm_v, embed_w, embed_m, embed_v):
    any_spec = pl.BlockSpec(memory_space=pl.ANY)
    vmem_spec = pl.BlockSpec(memory_space=pltpu.VMEM)
    dma = pltpu.SemaphoreType.DMA
    held = [(8, 128)] + [SEVEN, DOWN, NORM] + [SEVEN] * 3 + [DOWN] * 3 + [NORM] * 3
    reduced = pl.pallas_call(
        reduce_kernel,
        out_shape=[pltpu.VMEM(shape, F32) for shape in held],
        in_specs=[any_spec] * 16,
        out_specs=[vmem_spec] * len(held),
        scratch_shapes=[pltpu.VMEM((RING, 8, max(PART, PIECE)), F32)] * 2
        + [pltpu.VMEM(SEVEN, F32), pltpu.VMEM(DOWN, F32)] * 3
        + [pltpu.VMEM(NORM, F32)] * 5
        + [pltpu.VMEM((8, 128), F32), pltpu.VMEM((4, 8, 128), F32), pltpu.VMEM((8, 8, 128), F32)]
        + [pltpu.VMEM((8, PART), F32)] + [pltpu.VMEM((FIRST, FIRST_COLS), F32)] * 2
        + [pltpu.VMEM((2, FIRST, FIRST_COLS), F32), pltpu.VMEM((FIRST, SPLIT), F32)]
        + [dma((RING,)), dma((RING,)), dma((M_RING,)), dma((Y_RING,)), dma((6,)), dma((4,)), dma((4,)), dma((9,)), dma,
           pltpu.SemaphoreType.REGULAR],
        compiler_params=pltpu.CompilerParams(collective_id=0, has_side_effects=True,
                                             vmem_limit_bytes=26 * 1024 * 1024),
    )(g_layer, g_down, g_norm, g_embed, layer_w, layer_m, layer_v, down_w, down_m, down_v, norm_w, norm_m, norm_v,
      embed_w, embed_m, embed_v)
    groups = ((6, ROWS, WIDTH), DOWN, NORM, (ROWS, WIDTH))
    out_shape = [jax.ShapeDtypeStruct(s, d) for s in groups for d in (F32, F32, F32, jnp.bfloat16)]
    staged = [pltpu.VMEM(s, d) for s in (SEVEN, DOWN, NORM) for d in (F32, F32, F32, jnp.bfloat16)]
    return pl.pallas_call(
        update_kernel,
        out_shape=out_shape,
        in_specs=[vmem_spec] * len(held),
        out_specs=[any_spec] * 16,
        scratch_shapes=staged + [dma((4, 4))],
        compiler_params=pltpu.CompilerParams(vmem_limit_bytes=26 * 1024 * 1024),
    )(*[pltpu.with_memory_space_constraint(a, pltpu.VMEM) for a in reduced])


def solution(mesh):
    grad_four = P(("dp", "fsdp"), None, None, None)
    grad_three = P(("dp", "fsdp"), None, None)
    layer_spec = P(None, "fsdp", None)
    down_spec = P("fsdp", None)
    norm_spec = P(None, "fsdp")
    embed_spec = P("fsdp", None)
    in_specs = (grad_four, grad_three, grad_three, grad_three,
                layer_spec, layer_spec, layer_spec, down_spec, down_spec, down_spec,
                norm_spec, norm_spec, norm_spec, embed_spec, embed_spec, embed_spec)
    out_specs = (layer_spec,) * 4 + (down_spec,) * 4 + (norm_spec,) * 4 + (embed_spec,) * 4
    return jax.shard_map(local_update, mesh=mesh, in_specs=in_specs, out_specs=out_specs, check_vma=False)
```

```python
import math

import jax
import jax.numpy as jnp
from jax import lax
from jax.experimental import pallas as pl
from jax.experimental.pallas import tpu as pltpu
from jax.sharding import PartitionSpec as P

ADAM_BETA1 = 0.9
ADAM_BETA2 = 0.95
ADAM_EPS = 1e-8
LEARN_RATE = 4e-4
WEIGHT_DECAY = 0.1
CLIP_EPS = 1e-6
OPT_STEP = 20
BIAS_ONE = 1.0 - ADAM_BETA1 ** OPT_STEP
BIAS_TWO = 1.0 - ADAM_BETA2 ** OPT_STEP
ROOT_TWO = math.sqrt(BIAS_TWO)
SMALLEST = 1.1754944e-38

MESH = pl.DeviceIdType.MESH
F32 = jnp.float32

ROWS = 64
WIDTH = 3072
FF = 8192
PIECE = 1024
NORM = (4, 768)
SEVEN = (7, ROWS, WIDTH)
DOWN = (ROWS, FF)

FIRST = 8
FIRST_COLS = 5120
SPLIT = FIRST_COLS // 2
PART = 1536
BLOCK = (ROWS // 8) * (WIDTH // PART)
N_EMBED = BLOCK
N_LAYER = N_EMBED + 6 * BLOCK
N_HALF = 3
N = N_LAYER + (FF // PIECE) * (ROWS // 8) - FIRST_COLS // PIECE

LEAD = 5
FETCH = 7
RING = 9
LAG = 5
Y_RING = 2 * LAG + 2
M_RING = RING + LEAD


class Chunk:
    def __init__(self, kind, k):
        self.kind = kind
        if kind in ("half", "down"):
            q = k - N_LAYER
            per = FF // PIECE
            self.width = PIECE
        else:
            q = k if kind == "embed" else (k - N_EMBED) % BLOCK
            per = WIDTH // PART
            self.width = PART
            self.j = 6 if kind == "embed" else (k - N_EMBED) // BLOCK
        self.row = pl.multiple_of((q // per) * 8, 8)
        self.rows = pl.ds(self.row, 8)
        self.col = (q % per) * self.width
        self.cols = pl.ds(pl.multiple_of(self.col, 512), self.width)

    def half(self, dp):
        half = self.width // 2
        return pl.ds(pl.multiple_of(self.col + dp * half, 512), half)

    def source(self, grads, q):
        g_layer, g_down, g_embed = grads
        rows = pl.ds(pl.multiple_of(q * ROWS + self.row, 8), 8)
        if self.kind == "embed":
            return g_embed.at[0, rows, self.cols]
        if self.kind == "layer":
            return g_layer.at[0, self.j, rows, self.cols]
        return g_down.at[0, rows, self.cols]

    def state(self, layer, down, embed):
        if self.kind == "embed":
            return embed.at[self.rows, self.cols]
        if self.kind == "layer":
            return layer.at[self.j, self.rows, self.cols]
        return down.at[self.rows, self.cols]

    def held(self, seven, down):
        if self.kind in ("half", "down"):
            return down.at[self.rows, self.cols]
        return seven.at[self.j, self.rows, self.cols]

    def ring(self, ring, s):
        return ring.at[s, :, pl.ds(0, self.width)]


def on_chunk(k, use):
    if isinstance(k, int):
        use(Chunk("embed", k))
        return
    bounds = (0, N_EMBED, N_LAYER, N_LAYER + N_HALF, N)
    for i, kind in enumerate(("embed", "layer", "half", "down")):
        @pl.when(jnp.logical_and(k >= bounds[i], k < bounds[i + 1]))
        def _():
            use(Chunk(kind, k))


def start(copies):
    for copy in copies:
        copy.start()


def wait(copies):
    for copy in copies:
        copy.wait()


def take(ref, sem):
    pltpu.make_async_copy(ref, ref, sem).wait()


def squares(mean, width):
    parts = [mean[r:r + 8, i * 128:(i + 1) * 128] for r in range(0, mean.shape[0], 8) for i in range(width // 128)]
    sums = [p * p for p in parts[:4]]
    for i, p in enumerate(parts[4:]):
        sums[i % 4] = sums[i % 4] + p * p
    return (sums[0] + sums[1]) + (sums[2] + sums[3])


def reduce_kernel(g_layer, g_down, g_norm, g_embed, layer_w, layer_m, layer_v, down_w, down_m, down_v,
                  norm_w, norm_m, norm_v, embed_w, embed_m, embed_v,
                  sq_out, g7, gd, gn, w7, m7, v7, wd, md, vd, wn, mn, vn,
                  own_o, par_o, pm7, pmd, x7, xd, y7, yd, own_no, par_no, pmn, xn, yn, acc, acc_first, sq_all, sq_first,
                  pre, fo_own, fo_par, f_held, f_y,
                  out_sem, other_sem, mine_sem, y_sem, st_sem, n_sem, sq_sem, f_sem, pre_sem, credit):
    dp = lax.axis_index("dp")
    f = lax.axis_index("fsdp")
    core = lax.rem(f, 2)
    f_core = f + 1 - 2 * core
    f_x = lax.rem(f + 2, 4)
    f_diag = lax.rem(f_core + 2, 4)
    peer_core = (dp, f_core)
    peer_x = (dp, f_x)
    peer_diag = (dp, f_diag)
    peer_y = (1 - dp, f)
    peers = (peer_core, peer_x, peer_diag, peer_y, (1 - dp, f_core), (1 - dp, f_x), (1 - dp, f_diag))

    def remote(src, dst, send, recv, peer):
        return pltpu.make_async_remote_copy(src_ref=src, dst_ref=dst, send_sem=send, recv_sem=recv,
                                            device_id=peer, device_id_type=MESH)

    grads = (g_layer, g_down, g_embed)

    def x_copy(k, chunk):
        s = lax.rem(k, RING)
        return remote(chunk.ring(own_o, s), chunk.held(x7, xd), out_sem.at[s], mine_sem.at[lax.rem(k, M_RING)], peer_x)

    def y_copy(k, chunk):
        sem = y_sem.at[lax.rem(k, Y_RING)]
        return remote(chunk.held(g7, gd), chunk.held(y7, yd), sem, sem, peer_y)

    def half_copy(k, chunk):
        sem = y_sem.at[lax.rem(k, Y_RING)]
        give = chunk.half(1 - dp)
        return remote(gd.at[chunk.rows, give], yd.at[chunk.rows, give], sem, sem, peer_y)

    def by_core(chunk, on_whole, on_half):
        if chunk.kind == "half":
            pl.when(core == 0)(on_half)
            pl.when(core == 1)(on_whole)
        else:
            on_whole()

    def push_other(k, chunk, source):
        s = lax.rem(k, RING)
        return remote(source, chunk.ring(par_o, s), out_sem.at[s], other_sem.at[s], peer_core)

    def push_mine(k, chunk, source):
        s = lax.rem(k, RING)
        return remote(source, chunk.held(pm7, pmd), out_sem.at[s], mine_sem.at[lax.rem(k, M_RING)], peer_core)

    def own_loads(k, chunk):
        s = lax.rem(k, RING)
        return [pltpu.make_async_copy(chunk.source(grads, f_x), chunk.ring(own_o, s), other_sem.at[s]),
                pltpu.make_async_copy(chunk.source(grads, f), chunk.held(g7, gd), mine_sem.at[lax.rem(k, M_RING)])]

    def times(count, chunk):
        return own_o.at[pl.ds(0, count), :, pl.ds(0, chunk.width)]

    def retire(k, chunk):
        take(times(3, chunk), out_sem.at[lax.rem(k, RING)])

    def fetch(k):
        @pl.when(jnp.logical_and(k >= RING, k < N))
        def _():
            on_chunk(k - RING, lambda chunk: retire(k - RING, chunk))
            pl.semaphore_wait(credit, 1)

        def begin(chunk):
            push_other(k, chunk, chunk.source(grads, f_diag)).start()
            for copy in own_loads(k, chunk):
                copy.start()
            push_mine(k, chunk, chunk.source(grads, f_core)).start()

        on_chunk(k, begin)

    def sum_x(k):
        def use(chunk):
            take(times(3, chunk), mine_sem.at[lax.rem(k, M_RING)])
            mine = chunk.held(g7, gd)
            theirs = chunk.held(pm7, pmd)
            mine[...] = (mine[...] + theirs[...]) + chunk.held(x7, xd)[...]

        on_chunk(k, use)

    def sum_chip(k):
        s = lax.rem(k, RING)

        def use(chunk):
            mine = chunk.ring(own_o, s)
            theirs = chunk.ring(par_o, s)
            take(times(2, chunk), other_sem.at[s])
            mine[...] = mine[...] + theirs[...]

        on_chunk(k, use)

    def start_x(k):
        on_chunk(k, lambda chunk: x_copy(k, chunk).start())

        @pl.when(jnp.logical_and(k >= 0, k < N - RING))
        def _():
            pl.semaphore_signal(credit, inc=1, device_id=peer_core, device_id_type=MESH)

    def start_y(k):
        def use(chunk):
            by_core(chunk, lambda: y_copy(k, chunk).start(), lambda: half_copy(k, chunk).start())
            seven = chunk.kind in ("embed", "layer")
            for i, (src, dst) in enumerate((((layer_w, down_w, embed_w), (w7, wd)), ((layer_m, down_m, embed_m), (m7, md)),
                                            ((layer_v, down_v, embed_v), (v7, vd)))):
                pltpu.make_async_copy(chunk.state(*src), chunk.held(*dst), st_sem.at[i if seven else 3 + i]).start()

        on_chunk(k, use)

    def sum_y(k):
        def use(chunk):
            sem = y_sem.at[lax.rem(k, Y_RING)]

            def whole():
                take(times(2, chunk), sem)
                mine = chunk.held(g7, gd)
                mean = (mine[...] + chunk.held(y7, yd)[...]) * 0.125
                mine[...] = mean
                acc[...] += squares(mean, chunk.width)

            def half():
                take(times(1, chunk), sem)
                keep = chunk.half(dp)
                mean = (gd[chunk.rows, keep] + yd[chunk.rows, keep]) * 0.125
                gd[chunk.rows, keep] = mean
                acc_first[...] += squares(mean, chunk.width // 2)

            by_core(chunk, whole, half)

        on_chunk(k, use)

    last = pl.ds(ROWS - FIRST, FIRST)
    keep = pl.ds(pl.multiple_of(FF - FIRST_COLS + dp * SPLIT, PIECE // 2), SPLIT)
    give = pl.ds(pl.multiple_of(FF - FIRST_COLS + (1 - dp) * SPLIT, PIECE // 2), SPLIT)
    cols = pl.ds(FF - FIRST_COLS, FIRST_COLS)
    keep_o = pl.ds(pl.multiple_of(dp * SPLIT, PIECE // 2), SPLIT)
    give_o = pl.ds(pl.multiple_of((1 - dp) * SPLIT, PIECE // 2), SPLIT)

    def first_rows(q):
        return g_down.at[0, pl.ds(pl.multiple_of(q * ROWS + (ROWS - FIRST), 8), FIRST), cols]

    f_own = gd.at[last, cols]
    f_give = [pltpu.make_async_copy(first_rows(q), f_held.at[i], f_sem.at[0]) for i, q in enumerate((f_diag, f_core))]
    f_local = [pltpu.make_async_copy(first_rows(f_x), fo_own, f_sem.at[1]),
               pltpu.make_async_copy(first_rows(f), f_own, f_sem.at[1])]
    f_push = []
    for h, (half, half_o) in enumerate(((give, give_o), (keep, keep_o))):
        for i, ref in enumerate((fo_par.at[:, half_o], pmd.at[last, half])):
            f_push.append(remote(f_held.at[i, :, half_o], ref, f_sem.at[2],
                                 f_sem.at[3 + i] if h == 0 else f_sem.at[5], peer_core))
    f_state = [pltpu.make_async_copy(src.at[last, cols], dst.at[last, cols], st_sem.at[3 + i])
               for i, (src, dst) in enumerate(((down_w, wd), (down_m, md), (down_v, vd)))]
    f_scatter = [remote(fo_own.at[:, give_o], f_y, f_sem.at[6], f_sem.at[6], peer_y),
                 remote(gd.at[last, give], yd.at[last, give], f_sem.at[6], f_sem.at[6], peer_y)]
    f_cross = remote(fo_own.at[:, keep_o], xd.at[last, keep], f_sem.at[7], f_sem.at[7], peer_x)
    f_gather = remote(gd.at[last, keep], yd.at[last, keep], f_sem.at[8], f_sem.at[8], peer_y)
    halves = [Chunk("half", N_LAYER + i) for i in range(N_HALF)]
    h_gather = [remote(gd.at[chunk.rows, chunk.half(dp)], yd.at[chunk.rows, chunk.half(dp)], f_sem.at[9], f_sem.at[9],
                       peer_y) for chunk in halves]
    me = dp * 4 + f
    sqf_copies = [remote(sq_first.at[me], sq_first.at[me], sq_sem.at[0], sq_sem.at[1], peer)
                  for peer in peers]

    def norm_source(q):
        return g_norm.at[0, :, pl.ds(pl.multiple_of(q * NORM[1], 128), NORM[1])]

    n_push_other = remote(norm_source(f_diag), par_no, n_sem.at[1], n_sem.at[0], peer_core)
    n_push_mine = remote(norm_source(f_core), pmn, n_sem.at[1], n_sem.at[0], peer_core)
    n_x = remote(own_no, xn, n_sem.at[2], n_sem.at[2], peer_x)
    n_y = remote(gn, yn, n_sem.at[3], n_sem.at[3], peer_y)
    n_local = [pltpu.make_async_copy(src, dst, n_sem.at[0]) for src, dst in
               ((norm_source(f_x), own_no), (norm_source(f), gn), (norm_w, wn), (norm_m, mn), (norm_v, vn))]

    def n_times(count):
        return fo_par.at[:, pl.ds(0, count * NORM[0] * NORM[1] // 8)]


    zero = Chunk("embed", 0)
    ahead = pltpu.make_async_copy(zero.source(grads, f_diag), pre, pre_sem)
    ahead.start()
    for copy in own_loads(0, zero):
        copy.start()
    for copy in f_give + f_local:
        copy.start()
    acc[...] = jnp.zeros_like(acc)
    acc_first[...] = jnp.zeros_like(acc_first)

    barrier = pltpu.get_barrier_semaphore()
    near = (peer_core, peer_x, peer_y)
    for peer in near:
        pl.semaphore_signal(barrier, inc=1, device_id=peer, device_id_type=MESH)
    take(f_held, f_sem.at[0])
    pl.semaphore_wait(barrier, len(near))
    f_push[0].start()
    ahead.wait()
    push_other(0, zero, pre).start()
    f_push[1].start()
    start(f_push[2:])
    push_mine(0, zero, zero.source(grads, f_core)).start()
    for k in range(1, FETCH - LEAD + 1):
        fetch(k)
    take(f_held, f_sem.at[1])
    take(fo_par.at[:, give_o], f_sem.at[3])
    fo_own[:, give_o] = fo_own[:, give_o] + fo_par[:, give_o]
    f_scatter[0].start()
    sum_chip(0)
    start_x(0)
    take(fo_par.at[:, give_o], f_sem.at[4])
    gd[last, give] = gd[last, give] + pmd[last, give]
    f_scatter[1].start()
    take(fo_par, f_sem.at[5])
    take(f_held, f_sem.at[2])
    fo_own[:, keep_o] = fo_own[:, keep_o] + fo_par[:, keep_o]
    gd[last, keep] = gd[last, keep] + pmd[last, keep]
    start(f_state)

    def step(t, _):
        i = t - FETCH
        fetch(i + FETCH)

        @pl.when(i == 0)
        def _():
            n_push_other.start()
            n_push_mine.start()
            for copy in n_local:
                copy.start()

        sum_x(i)
        sum_chip(i + LEAD)
        start_y(i)
        start_x(i + LEAD)

        @pl.when(i == 3)
        def _():
            take(n_times(7), n_sem.at[0])
            take(n_times(2), n_sem.at[1])
            own_no[...] = own_no[...] + par_no[...]
            n_x.start()

        @pl.when(i == 10)
        def _():
            take(n_times(2), n_sem.at[2])
            gn[...] = (gn[...] + pmn[...]) + xn[...]
            n_y.start()
            take(f_held, f_sem.at[6])
            fo_own[:, keep_o] = fo_own[:, keep_o] + f_y[...]
            gd[last, keep] = gd[last, keep] + yd[last, keep]

        @pl.when(i == 20)
        def _():
            take(n_times(2), n_sem.at[3])
            mean = (gn[...] + yn[...]) * 0.125
            gn[...] = mean
            square = mean * mean
            total = square[:, 0:128]
            for c in range(1, NORM[1] // 128):
                total = total + square[:, c * 128:(c + 1) * 128]
            acc[0:4, :] += total

        @pl.when(i == N - LEAD)
        def _():
            f_cross.start()

        @pl.when(jnp.logical_and(i == N, core == 0))
        def _():
            start(h_gather)

        @pl.when(i == N + LAG - 3)
        def _():
            take(fo_par, f_sem.at[7])
            mean = (gd[last, keep] + xd[last, keep]) * 0.125
            gd[last, keep] = mean
            sq_first[me] = acc_first[...] + squares(mean, SPLIT)
            start(sqf_copies)
            f_gather.start()

        sum_y(i - LAG)
        return 0

    lax.fori_loop(FETCH - LEAD + 1, FETCH + N + LAG, step, 0)

    sq_all[f] = acc[...]
    copies = [remote(sq_all.at[f], sq_all.at[f], sq_sem.at[2], sq_sem.at[3], peer)
              for peer in (peer_core, peer_x, peer_diag)]
    for copy in copies:
        copy.start()

    def drain(k, _):
        on_chunk(k, lambda chunk: retire(k, chunk))
        return 0

    lax.fori_loop(N - RING, N, drain, 0)
    for i, ref in enumerate((w7, m7, v7, wd, md, vd)):
        pltpu.make_async_copy(ref, ref, st_sem.at[i]).wait()

    @pl.when(core == 0)
    def _():
        take(gd.at[pl.ds(0, 8), pl.ds(0, N_HALF * PIECE)], f_sem.at[9])
        for chunk in halves:
            gd[chunk.rows, chunk.half(1 - dp)] = yd[chunk.rows, chunk.half(1 - dp)]

    take(fo_par, f_sem.at[8])
    gd[last, give] = yd[last, give]
    take(sq_first.at[pl.ds(0, 7)], sq_sem.at[0])
    take(sq_first.at[pl.ds(0, 7)], sq_sem.at[1])
    total = sq_first[0]
    for i in range(1, 8):
        total = total + sq_first[i]
    take(sq_all.at[pl.ds(0, 3)], sq_sem.at[2])
    take(sq_all.at[pl.ds(0, 3)], sq_sem.at[3])
    sq_out[...] = ((sq_all[0] + sq_all[1]) + (sq_all[2] + sq_all[3])) + total


def update_math(avg_scale, sq_scale, g, w, m, v, decay):
    avg = ADAM_BETA1 * m + avg_scale * g
    root = sq_scale * g
    sq = ADAM_BETA2 * v + root * root
    dev = sq * lax.rsqrt(jnp.maximum(sq, SMALLEST))
    step_dir = avg / (dev + ADAM_EPS * ROOT_TWO)
    new = (1.0 - LEARN_RATE * decay) * w - (LEARN_RATE * ROOT_TWO / BIAS_ONE) * step_dir
    return new, avg, sq, new.astype(jnp.bfloat16)


def update_kernel(sq, g7, gd, gn, w7, m7, v7, wd, md, vd, wn, mn, vn,
                  lw, lm, lv, lb, dw, dm, dv, db, nw, nm, nv, nb, ew, em, ev, eb,
                  s7w, s7m, s7v, s7b, sdw, sdm, sdv, sdb, snw, snm, snv, snb, sem):
    total = jnp.sum(sq[...], keepdims=True)
    clip = jnp.minimum(1.0, 1.0 / (jnp.sqrt(total) + CLIP_EPS))
    scales = ((1.0 - ADAM_BETA1) * clip, math.sqrt(1.0 - ADAM_BETA2) * clip)

    outs = ((lw, lm, lv, lb), (dw, dm, dv, db), (nw, nm, nv, nb), (ew, em, ev, eb))
    seven_staged = (s7w, s7m, s7v, s7b)
    down_staged = (sdw, sdm, sdv, sdb)

    def layer_copies(j, row, rows):
        at = pl.ds(row, rows)
        return [pltpu.make_async_copy(src.at[j, at, :], dst.at[j, at, :], sem.at[0, a])
                for a, (src, dst) in enumerate(zip(seven_staged, outs[0]))]

    def embed_copies():
        return [pltpu.make_async_copy(src.at[6], dst, sem.at[1, a])
                for a, (src, dst) in enumerate(zip(seven_staged, outs[3]))]

    def down_copies(t):
        at = pl.ds(pl.multiple_of(t * 16, 16), 16)
        return [pltpu.make_async_copy(src.at[at, :], dst.at[at, :], sem.at[2, a])
                for a, (src, dst) in enumerate(zip(down_staged, outs[1]))]

    def seven(j, row, decay):
        for c in range(0, WIDTH, 512):
            ix = (j, pl.ds(row, 16), pl.ds(c, 512))
            out = update_math(*scales, g7[ix], w7[ix], m7[ix], v7[ix], decay)
            for ref, val in zip(seven_staged, out):
                ref[ix] = val

    def block(j, decay):
        def rows(t, _):
            seven(j, pl.multiple_of(t * 16, 16), decay)
            return 0

        lax.fori_loop(0, 4, rows, 0)

    def first_step(t, _):
        row = pl.multiple_of(t * 16, 16)
        seven(0, row, WEIGHT_DECAY)
        start(layer_copies(0, row, 16))
        return 0

    def half_step(t, _):
        seven(1, pl.multiple_of(t * 32, 32), WEIGHT_DECAY)
        seven(1, pl.multiple_of(t * 32 + 16, 16), WEIGHT_DECAY)
        start(layer_copies(1, pl.multiple_of(t * 32, 32), 32))
        return 0

    def layer_step(j, _):
        block(j, WEIGHT_DECAY)
        start(layer_copies(j, 0, ROWS))
        return 0

    def down_step(t, _):
        row = pl.multiple_of(t * 16, 16)

        def cols(u, _):
            ix = (pl.ds(row, 16), pl.ds(pl.multiple_of(u * 1024, 1024), 1024))
            out = update_math(*scales, gd[ix], wd[ix], md[ix], vd[ix], WEIGHT_DECAY)
            for ref, val in zip(down_staged, out):
                ref[ix] = val
            return 0

        lax.fori_loop(0, FF // 1024, cols, 0)
        start(down_copies(t))
        return 0

    lax.fori_loop(0, 4, first_step, 0)
    lax.fori_loop(0, 2, half_step, 0)
    lax.fori_loop(2, 6, layer_step, 0)
    out = update_math(*scales, gn[...], wn[...], mn[...], vn[...], WEIGHT_DECAY)
    for ref, val in zip((snw, snm, snv, snb), out):
        ref[...] = val
    norm_copies = [pltpu.make_async_copy(src, dst, sem.at[3, a])
                   for a, (src, dst) in enumerate(zip((snw, snm, snv, snb), outs[2]))]
    start(norm_copies)
    block(6, 0.0)
    start(embed_copies())
    lax.fori_loop(0, 4, down_step, 0)

    for a, staged in enumerate(seven_staged):
        pltpu.make_async_copy(staged.at[pl.ds(0, 6)], outs[0][a], sem.at[0, a]).wait()
    wait(embed_copies())
    wait(norm_copies)
    for a, staged in enumerate(down_staged):
        pltpu.make_async_copy(staged, outs[1][a], sem.at[2, a]).wait()


def local_update(g_layer, g_down, g_norm, g_embed, layer_w, layer_m, layer_v, down_w, down_m, down_v, norm_w, norm_m,
                 norm_v, embed_w, embed_m, embed_v):
    any_spec = pl.BlockSpec(memory_space=pl.ANY)
    vmem_spec = pl.BlockSpec(memory_space=pltpu.VMEM)
    dma = pltpu.SemaphoreType.DMA
    held = [(8, 128)] + [SEVEN, DOWN, NORM] + [SEVEN] * 3 + [DOWN] * 3 + [NORM] * 3
    reduced = pl.pallas_call(
        reduce_kernel,
        out_shape=[pltpu.VMEM(shape, F32) for shape in held],
        in_specs=[any_spec] * 16,
        out_specs=[vmem_spec] * len(held),
        scratch_shapes=[pltpu.VMEM((RING, 8, max(PART, PIECE)), F32)] * 2
        + [pltpu.VMEM(SEVEN, F32), pltpu.VMEM(DOWN, F32)] * 3
        + [pltpu.VMEM(NORM, F32)] * 5
        + [pltpu.VMEM((8, 128), F32)] * 2 + [pltpu.VMEM((4, 8, 128), F32), pltpu.VMEM((8, 8, 128), F32)]
        + [pltpu.VMEM((8, PART), F32)] + [pltpu.VMEM((FIRST, FIRST_COLS), F32)] * 2
        + [pltpu.VMEM((2, FIRST, FIRST_COLS), F32), pltpu.VMEM((FIRST, SPLIT), F32)]
        + [dma((RING,)), dma((RING,)), dma((M_RING,)), dma((Y_RING,)), dma((6,)), dma((4,)), dma((4,)), dma((10,)), dma,
           pltpu.SemaphoreType.REGULAR],
        compiler_params=pltpu.CompilerParams(collective_id=0, has_side_effects=True,
                                             vmem_limit_bytes=26 * 1024 * 1024),
    )(g_layer, g_down, g_norm, g_embed, layer_w, layer_m, layer_v, down_w, down_m, down_v, norm_w, norm_m, norm_v,
      embed_w, embed_m, embed_v)
    groups = ((6, ROWS, WIDTH), DOWN, NORM, (ROWS, WIDTH))
    out_shape = [jax.ShapeDtypeStruct(s, d) for s in groups for d in (F32, F32, F32, jnp.bfloat16)]
    staged = [pltpu.VMEM(s, d) for s in (SEVEN, DOWN, NORM) for d in (F32, F32, F32, jnp.bfloat16)]
    return pl.pallas_call(
        update_kernel,
        out_shape=out_shape,
        in_specs=[vmem_spec] * len(held),
        out_specs=[any_spec] * 16,
        scratch_shapes=staged + [dma((4, 4))],
        compiler_params=pltpu.CompilerParams(vmem_limit_bytes=26 * 1024 * 1024),
    )(*[pltpu.with_memory_space_constraint(a, pltpu.VMEM) for a in reduced])


def solution(mesh):
    grad_four = P(("dp", "fsdp"), None, None, None)
    grad_three = P(("dp", "fsdp"), None, None)
    layer_spec = P(None, "fsdp", None)
    down_spec = P("fsdp", None)
    norm_spec = P(None, "fsdp")
    embed_spec = P("fsdp", None)
    in_specs = (grad_four, grad_three, grad_three, grad_three,
                layer_spec, layer_spec, layer_spec, down_spec, down_spec, down_spec,
                norm_spec, norm_spec, norm_spec, embed_spec, embed_spec, embed_spec)
    out_specs = (layer_spec,) * 4 + (down_spec,) * 4 + (norm_spec,) * 4 + (embed_spec,) * 4
    return jax.shard_map(local_update, mesh=mesh, in_specs=in_specs, out_specs=out_specs, check_vma=False)
```

```python
import math

import jax
import jax.numpy as jnp
from jax import lax
from jax.experimental import pallas as pl
from jax.experimental.pallas import tpu as pltpu
from jax.sharding import PartitionSpec as P

ADAM_BETA1 = 0.9
ADAM_BETA2 = 0.95
ADAM_EPS = 1e-8
LEARN_RATE = 4e-4
WEIGHT_DECAY = 0.1
CLIP_EPS = 1e-6
OPT_STEP = 20
BIAS_ONE = 1.0 - ADAM_BETA1 ** OPT_STEP
BIAS_TWO = 1.0 - ADAM_BETA2 ** OPT_STEP
ROOT_TWO = math.sqrt(BIAS_TWO)
SMALLEST = 1.1754944e-38

MESH = pl.DeviceIdType.MESH
F32 = jnp.float32

ROWS = 64
WIDTH = 3072
FF = 8192
PIECE = 1024
NORM = (4, 768)
SEVEN = (7, ROWS, WIDTH)
DOWN = (ROWS, FF)

FIRST = 8
FIRST_COLS = 5120
SPLIT = FIRST_COLS // 2
PART = 1536
BLOCK = (ROWS // 8) * (WIDTH // PART)
N_EMBED = BLOCK
N_LAYER = N_EMBED + 6 * BLOCK
N_HALF = 3
N = N_LAYER + (FF // PIECE) * (ROWS // 8) - FIRST_COLS // PIECE

LEAD = 5
FETCH = 7
RING = 9
LAG = 5
Y_RING = 2 * LAG + 2
M_RING = RING + LEAD


class Chunk:
    def __init__(self, kind, k):
        self.kind = kind
        if kind in ("half", "down"):
            q = k - N_LAYER
            per = FF // PIECE
            self.width = PIECE
        else:
            q = k if kind == "embed" else (k - N_EMBED) % BLOCK
            per = WIDTH // PART
            self.width = PART
            self.j = 6 if kind == "embed" else (k - N_EMBED) // BLOCK
        self.row = pl.multiple_of((q // per) * 8, 8)
        self.rows = pl.ds(self.row, 8)
        self.col = (q % per) * self.width
        self.cols = pl.ds(pl.multiple_of(self.col, 512), self.width)

    def half(self, dp):
        half = self.width // 2
        return pl.ds(pl.multiple_of(self.col + dp * half, 512), half)

    def source(self, grads, q):
        g_layer, g_down, g_embed = grads
        rows = pl.ds(pl.multiple_of(q * ROWS + self.row, 8), 8)
        if self.kind == "embed":
            return g_embed.at[0, rows, self.cols]
        if self.kind == "layer":
            return g_layer.at[0, self.j, rows, self.cols]
        return g_down.at[0, rows, self.cols]

    def state(self, layer, down, embed):
        if self.kind == "embed":
            return embed.at[self.rows, self.cols]
        if self.kind == "layer":
            return layer.at[self.j, self.rows, self.cols]
        return down.at[self.rows, self.cols]

    def held(self, seven, down):
        if self.kind in ("half", "down"):
            return down.at[self.rows, self.cols]
        return seven.at[self.j, self.rows, self.cols]

    def ring(self, ring, s):
        return ring.at[s, :, pl.ds(0, self.width)]


def on_chunk(k, use):
    if isinstance(k, int):
        use(Chunk("embed", k))
        return
    bounds = (0, N_EMBED, N_LAYER, N_LAYER + N_HALF, N)
    for i, kind in enumerate(("embed", "layer", "half", "down")):
        @pl.when(jnp.logical_and(k >= bounds[i], k < bounds[i + 1]))
        def _():
            use(Chunk(kind, k))


def start(copies):
    for copy in copies:
        copy.start()


def wait(copies):
    for copy in copies:
        copy.wait()


def take(ref, sem):
    pltpu.make_async_copy(ref, ref, sem).wait()


def squares(mean, width):
    parts = [mean[r:r + 8, i * 128:(i + 1) * 128] for r in range(0, mean.shape[0], 8) for i in range(width // 128)]
    sums = [p * p for p in parts[:4]]
    for i, p in enumerate(parts[4:]):
        sums[i % 4] = sums[i % 4] + p * p
    return (sums[0] + sums[1]) + (sums[2] + sums[3])


def reduce_kernel(g_layer, g_down, g_norm, g_embed, layer_w, layer_m, layer_v, down_w, down_m, down_v,
                  norm_w, norm_m, norm_v, embed_w, embed_m, embed_v,
                  sq_out, g7, gd, gn, w7, m7, v7, wd, md, vd, wn, mn, vn,
                  own_o, par_o, pm7, pmd, x7, xd, y7, yd, own_no, par_no, pmn, xn, yn, acc, acc_first, sq_all, sq_first,
                  pre, fo_own, fo_par, f_held, f_y,
                  out_sem, other_sem, mine_sem, y_sem, st_sem, n_sem, sq_sem, f_sem, pre_sem, credit):
    dp = lax.axis_index("dp")
    f = lax.axis_index("fsdp")
    core = lax.rem(f, 2)
    f_core = f + 1 - 2 * core
    f_x = lax.rem(f + 2, 4)
    f_diag = lax.rem(f_core + 2, 4)
    peer_core = (dp, f_core)
    peer_x = (dp, f_x)
    peer_diag = (dp, f_diag)
    peer_y = (1 - dp, f)
    peers = (peer_core, peer_x, peer_diag, peer_y, (1 - dp, f_core), (1 - dp, f_x), (1 - dp, f_diag))

    def remote(src, dst, send, recv, peer):
        return pltpu.make_async_remote_copy(src_ref=src, dst_ref=dst, send_sem=send, recv_sem=recv,
                                            device_id=peer, device_id_type=MESH)

    grads = (g_layer, g_down, g_embed)

    def x_copy(k, chunk):
        s = lax.rem(k, RING)
        return remote(chunk.ring(own_o, s), chunk.held(x7, xd), out_sem.at[s], mine_sem.at[lax.rem(k, M_RING)], peer_x)

    def y_copy(k, chunk):
        sem = y_sem.at[lax.rem(k, Y_RING)]
        return remote(chunk.held(g7, gd), chunk.held(y7, yd), sem, sem, peer_y)

    def half_copy(k, chunk):
        sem = y_sem.at[lax.rem(k, Y_RING)]
        give = chunk.half(1 - dp)
        return remote(gd.at[chunk.rows, give], yd.at[chunk.rows, give], sem, sem, peer_y)

    def by_core(chunk, on_whole, on_half):
        if chunk.kind == "half":
            pl.when(core == 0)(on_half)
            pl.when(core == 1)(on_whole)
        else:
            on_whole()

    def push_other(k, chunk, source):
        s = lax.rem(k, RING)
        return remote(source, chunk.ring(par_o, s), out_sem.at[s], other_sem.at[s], peer_core)

    def push_mine(k, chunk, source):
        s = lax.rem(k, RING)
        return remote(source, chunk.held(pm7, pmd), out_sem.at[s], mine_sem.at[lax.rem(k, M_RING)], peer_core)

    def own_loads(k, chunk):
        s = lax.rem(k, RING)
        return [pltpu.make_async_copy(chunk.source(grads, f_x), chunk.ring(own_o, s), other_sem.at[s]),
                pltpu.make_async_copy(chunk.source(grads, f), chunk.held(g7, gd), mine_sem.at[lax.rem(k, M_RING)])]

    def times(count, chunk):
        return own_o.at[pl.ds(0, count), :, pl.ds(0, chunk.width)]

    def retire(k, chunk):
        take(times(3, chunk), out_sem.at[lax.rem(k, RING)])

    def fetch(k):
        @pl.when(jnp.logical_and(k >= RING, k < N))
        def _():
            on_chunk(k - RING, lambda chunk: retire(k - RING, chunk))
            pl.semaphore_wait(credit, 1)

        def begin(chunk):
            push_other(k, chunk, chunk.source(grads, f_diag)).start()
            for copy in own_loads(k, chunk):
                copy.start()
            push_mine(k, chunk, chunk.source(grads, f_core)).start()

        on_chunk(k, begin)

    def sum_x(k):
        def use(chunk):
            take(times(3, chunk), mine_sem.at[lax.rem(k, M_RING)])
            mine = chunk.held(g7, gd)
            theirs = chunk.held(pm7, pmd)
            mine[...] = (mine[...] + theirs[...]) + chunk.held(x7, xd)[...]

        on_chunk(k, use)

    def sum_chip(k):
        s = lax.rem(k, RING)

        def use(chunk):
            mine = chunk.ring(own_o, s)
            theirs = chunk.ring(par_o, s)
            take(times(2, chunk), other_sem.at[s])
            mine[...] = mine[...] + theirs[...]

        on_chunk(k, use)

    def start_x(k):
        on_chunk(k, lambda chunk: x_copy(k, chunk).start())

        @pl.when(jnp.logical_and(k >= 0, k < N - RING))
        def _():
            pl.semaphore_signal(credit, inc=1, device_id=peer_core, device_id_type=MESH)

    def start_y(k):
        def use(chunk):
            by_core(chunk, lambda: y_copy(k, chunk).start(), lambda: half_copy(k, chunk).start())
            seven = chunk.kind in ("embed", "layer")
            for i, (src, dst) in enumerate((((layer_w, down_w, embed_w), (w7, wd)), ((layer_m, down_m, embed_m), (m7, md)),
                                            ((layer_v, down_v, embed_v), (v7, vd)))):
                pltpu.make_async_copy(chunk.state(*src), chunk.held(*dst), st_sem.at[i if seven else 3 + i]).start()

        on_chunk(k, use)

    def sum_y(k):
        def use(chunk):
            sem = y_sem.at[lax.rem(k, Y_RING)]

            def whole():
                take(times(2, chunk), sem)
                mine = chunk.held(g7, gd)
                mean = (mine[...] + chunk.held(y7, yd)[...]) * 0.125
                mine[...] = mean
                acc[...] += squares(mean, chunk.width)

            def half():
                take(times(1, chunk), sem)
                keep = chunk.half(dp)
                mean = (gd[chunk.rows, keep] + yd[chunk.rows, keep]) * 0.125
                gd[chunk.rows, keep] = mean
                acc_first[...] += squares(mean, chunk.width // 2)

            by_core(chunk, whole, half)

        on_chunk(k, use)

    last = pl.ds(ROWS - FIRST, FIRST)
    keep = pl.ds(pl.multiple_of(FF - FIRST_COLS + dp * SPLIT, PIECE // 2), SPLIT)
    give = pl.ds(pl.multiple_of(FF - FIRST_COLS + (1 - dp) * SPLIT, PIECE // 2), SPLIT)
    cols = pl.ds(FF - FIRST_COLS, FIRST_COLS)
    keep_o = pl.ds(pl.multiple_of(dp * SPLIT, PIECE // 2), SPLIT)
    give_o = pl.ds(pl.multiple_of((1 - dp) * SPLIT, PIECE // 2), SPLIT)

    def first_rows(q):
        return g_down.at[0, pl.ds(pl.multiple_of(q * ROWS + (ROWS - FIRST), 8), FIRST), cols]

    f_own = gd.at[last, cols]
    f_give = [pltpu.make_async_copy(first_rows(q), f_held.at[i], f_sem.at[0]) for i, q in enumerate((f_diag, f_core))]
    f_local = [pltpu.make_async_copy(first_rows(f_x), fo_own, f_sem.at[1]),
               pltpu.make_async_copy(first_rows(f), f_own, f_sem.at[1])]
    f_push = []
    for h, (half, half_o) in enumerate(((give, give_o), (keep, keep_o))):
        for i, ref in enumerate((fo_par.at[:, half_o], pmd.at[last, half])):
            f_push.append(remote(f_held.at[i, :, half_o], ref, f_sem.at[2],
                                 f_sem.at[3 + i] if h == 0 else f_sem.at[5], peer_core))
    f_state = [pltpu.make_async_copy(src.at[last, cols], dst.at[last, cols], st_sem.at[3 + i])
               for i, (src, dst) in enumerate(((down_w, wd), (down_m, md), (down_v, vd)))]
    f_scatter = [remote(fo_own.at[:, give_o], f_y, f_sem.at[6], f_sem.at[6], peer_y),
                 remote(gd.at[last, give], yd.at[last, give], f_sem.at[6], f_sem.at[6], peer_y)]
    f_cross = remote(fo_own.at[:, keep_o], xd.at[last, keep], f_sem.at[7], f_sem.at[7], peer_x)
    f_gather = remote(gd.at[last, keep], yd.at[last, keep], f_sem.at[8], f_sem.at[8], peer_y)
    halves = [Chunk("half", N_LAYER + i) for i in range(N_HALF)]
    h_gather = [remote(gd.at[chunk.rows, chunk.half(dp)], yd.at[chunk.rows, chunk.half(dp)], f_sem.at[9], f_sem.at[9],
                       peer_y) for chunk in halves]
    me = dp * 4 + f
    sqf_copies = [remote(sq_first.at[me], sq_first.at[me], sq_sem.at[0], sq_sem.at[1], peer)
                  for peer in peers]

    def norm_source(q):
        return g_norm.at[0, :, pl.ds(pl.multiple_of(q * NORM[1], 128), NORM[1])]

    n_push_other = remote(norm_source(f_diag), par_no, n_sem.at[1], n_sem.at[0], peer_core)
    n_push_mine = remote(norm_source(f_core), pmn, n_sem.at[1], n_sem.at[0], peer_core)
    n_x = remote(own_no, xn, n_sem.at[2], n_sem.at[2], peer_x)
    n_y = remote(gn, yn, n_sem.at[3], n_sem.at[3], peer_y)
    n_local = [pltpu.make_async_copy(src, dst, n_sem.at[0]) for src, dst in
               ((norm_source(f_x), own_no), (norm_source(f), gn), (norm_w, wn), (norm_m, mn), (norm_v, vn))]

    def n_times(count):
        return fo_par.at[:, pl.ds(0, count * NORM[0] * NORM[1] // 8)]


    zero = Chunk("embed", 0)
    ahead = pltpu.make_async_copy(zero.source(grads, f_diag), pre, pre_sem)
    ahead.start()
    for copy in own_loads(0, zero):
        copy.start()
    for copy in f_give + f_local:
        copy.start()
    acc[...] = jnp.zeros_like(acc)
    acc_first[...] = jnp.zeros_like(acc_first)

    barrier = pltpu.get_barrier_semaphore()
    near = (peer_core, peer_x, peer_y)
    for peer in near:
        pl.semaphore_signal(barrier, inc=1, device_id=peer, device_id_type=MESH)
    take(f_held, f_sem.at[0])
    pl.semaphore_wait(barrier, len(near))
    f_push[0].start()
    ahead.wait()
    push_other(0, zero, pre).start()
    f_push[1].start()
    start(f_push[2:])
    push_mine(0, zero, zero.source(grads, f_core)).start()
    for k in range(1, FETCH - LEAD + 1):
        fetch(k)
    take(f_held, f_sem.at[1])
    take(fo_par.at[:, give_o], f_sem.at[3])
    fo_own[:, give_o] = fo_own[:, give_o] + fo_par[:, give_o]
    f_scatter[0].start()
    sum_chip(0)
    start_x(0)
    take(fo_par.at[:, give_o], f_sem.at[4])
    gd[last, give] = gd[last, give] + pmd[last, give]
    f_scatter[1].start()
    take(fo_par, f_sem.at[5])
    take(f_held, f_sem.at[2])
    fo_own[:, keep_o] = fo_own[:, keep_o] + fo_par[:, keep_o]
    gd[last, keep] = gd[last, keep] + pmd[last, keep]
    start(f_state)

    def step(t, _):
        i = t - FETCH
        fetch(i + FETCH)

        @pl.when(i == 0)
        def _():
            n_push_other.start()
            n_push_mine.start()
            for copy in n_local:
                copy.start()

        sum_x(i)
        sum_chip(i + LEAD)
        start_y(i)
        start_x(i + LEAD)

        @pl.when(i == 3)
        def _():
            take(n_times(7), n_sem.at[0])
            take(n_times(2), n_sem.at[1])
            own_no[...] = own_no[...] + par_no[...]
            n_x.start()

        @pl.when(i == 10)
        def _():
            take(n_times(2), n_sem.at[2])
            gn[...] = (gn[...] + pmn[...]) + xn[...]
            n_y.start()
            take(f_held, f_sem.at[6])
            fo_own[:, keep_o] = fo_own[:, keep_o] + f_y[...]
            gd[last, keep] = gd[last, keep] + yd[last, keep]

        @pl.when(i == 20)
        def _():
            take(n_times(2), n_sem.at[3])
            mean = (gn[...] + yn[...]) * 0.125
            gn[...] = mean
            square = mean * mean
            total = square[:, 0:128]
            for c in range(1, NORM[1] // 128):
                total = total + square[:, c * 128:(c + 1) * 128]
            acc[0:4, :] += total

        @pl.when(i == N - LEAD)
        def _():
            f_cross.start()

        @pl.when(jnp.logical_and(i == N, core == 0))
        def _():
            start(h_gather)

        @pl.when(i == N + LAG - 3)
        def _():
            take(fo_par, f_sem.at[7])
            mean = (gd[last, keep] + xd[last, keep]) * 0.125
            gd[last, keep] = mean
            sq_first[me] = jnp.sum(acc_first[...] + squares(mean, SPLIT), axis=0, keepdims=True)
            start(sqf_copies)
            f_gather.start()

        sum_y(i - LAG)
        return 0

    lax.fori_loop(FETCH - LEAD + 1, FETCH + N + LAG, step, 0)

    sq_all[f] = jnp.sum(acc[...], axis=0, keepdims=True)
    copies = [remote(sq_all.at[f], sq_all.at[f], sq_sem.at[2], sq_sem.at[3], peer)
              for peer in (peer_core, peer_x, peer_diag)]
    for copy in copies:
        copy.start()

    def drain(k, _):
        on_chunk(k, lambda chunk: retire(k, chunk))
        return 0

    lax.fori_loop(N - RING, N, drain, 0)
    for i, ref in enumerate((w7, m7, v7, wd, md, vd)):
        pltpu.make_async_copy(ref, ref, st_sem.at[i]).wait()

    @pl.when(core == 0)
    def _():
        take(gd.at[pl.ds(0, 8), pl.ds(0, N_HALF * PIECE)], f_sem.at[9])
        for chunk in halves:
            gd[chunk.rows, chunk.half(1 - dp)] = yd[chunk.rows, chunk.half(1 - dp)]

    take(fo_par, f_sem.at[8])
    gd[last, give] = yd[last, give]
    take(sq_first.at[pl.ds(0, 7)], sq_sem.at[0])
    take(sq_first.at[pl.ds(0, 7)], sq_sem.at[1])
    total = sq_first[0]
    for i in range(1, 8):
        total = total + sq_first[i]
    take(sq_all.at[pl.ds(0, 3)], sq_sem.at[2])
    take(sq_all.at[pl.ds(0, 3)], sq_sem.at[3])
    sq_out[...] = ((sq_all[0] + sq_all[1]) + (sq_all[2] + sq_all[3])) + total


def update_math(avg_scale, sq_scale, g, w, m, v, decay):
    avg = ADAM_BETA1 * m + avg_scale * g
    root = sq_scale * g
    sq = ADAM_BETA2 * v + root * root
    dev = sq * lax.rsqrt(jnp.maximum(sq, SMALLEST))
    step_dir = avg / (dev + ADAM_EPS * ROOT_TWO)
    new = (1.0 - LEARN_RATE * decay) * w - (LEARN_RATE * ROOT_TWO / BIAS_ONE) * step_dir
    return new, avg, sq, new.astype(jnp.bfloat16)


def update_kernel(sq, g7, gd, gn, w7, m7, v7, wd, md, vd, wn, mn, vn,
                  lw, lm, lv, lb, dw, dm, dv, db, nw, nm, nv, nb, ew, em, ev, eb,
                  s7w, s7m, s7v, s7b, sdw, sdm, sdv, sdb, snw, snm, snv, snb, sem):
    total = jnp.sum(sq[...], keepdims=True)
    clip = jnp.minimum(1.0, 1.0 / (jnp.sqrt(total) + CLIP_EPS))
    scales = ((1.0 - ADAM_BETA1) * clip, math.sqrt(1.0 - ADAM_BETA2) * clip)

    outs = ((lw, lm, lv, lb), (dw, dm, dv, db), (nw, nm, nv, nb), (ew, em, ev, eb))
    seven_staged = (s7w, s7m, s7v, s7b)
    down_staged = (sdw, sdm, sdv, sdb)

    def layer_copies(j, row, rows):
        at = pl.ds(row, rows)
        return [pltpu.make_async_copy(src.at[j, at, :], dst.at[j, at, :], sem.at[0, a])
                for a, (src, dst) in enumerate(zip(seven_staged, outs[0]))]

    def embed_copies():
        return [pltpu.make_async_copy(src.at[6], dst, sem.at[1, a])
                for a, (src, dst) in enumerate(zip(seven_staged, outs[3]))]

    def down_copies(t):
        at = pl.ds(pl.multiple_of(t * 16, 16), 16)
        return [pltpu.make_async_copy(src.at[at, :], dst.at[at, :], sem.at[2, a])
                for a, (src, dst) in enumerate(zip(down_staged, outs[1]))]

    def seven(j, row, decay):
        for c in range(0, WIDTH, 512):
            ix = (j, pl.ds(row, 16), pl.ds(c, 512))
            out = update_math(*scales, g7[ix], w7[ix], m7[ix], v7[ix], decay)
            for ref, val in zip(seven_staged, out):
                ref[ix] = val

    def block(j, decay):
        def rows(t, _):
            seven(j, pl.multiple_of(t * 16, 16), decay)
            return 0

        lax.fori_loop(0, 4, rows, 0)

    def first_step(t, _):
        row = pl.multiple_of(t * 16, 16)
        seven(0, row, WEIGHT_DECAY)
        start(layer_copies(0, row, 16))
        return 0

    def half_step(t, _):
        seven(1, pl.multiple_of(t * 32, 32), WEIGHT_DECAY)
        seven(1, pl.multiple_of(t * 32 + 16, 16), WEIGHT_DECAY)
        start(layer_copies(1, pl.multiple_of(t * 32, 32), 32))
        return 0

    def layer_step(j, _):
        block(j, WEIGHT_DECAY)
        start(layer_copies(j, 0, ROWS))
        return 0

    def down_step(t, _):
        row = pl.multiple_of(t * 16, 16)

        def cols(u, _):
            ix = (pl.ds(row, 16), pl.ds(pl.multiple_of(u * 1024, 1024), 1024))
            out = update_math(*scales, gd[ix], wd[ix], md[ix], vd[ix], WEIGHT_DECAY)
            for ref, val in zip(down_staged, out):
                ref[ix] = val
            return 0

        lax.fori_loop(0, FF // 1024, cols, 0)
        start(down_copies(t))
        return 0

    lax.fori_loop(0, 4, first_step, 0)
    lax.fori_loop(0, 2, half_step, 0)
    lax.fori_loop(2, 6, layer_step, 0)
    out = update_math(*scales, gn[...], wn[...], mn[...], vn[...], WEIGHT_DECAY)
    for ref, val in zip((snw, snm, snv, snb), out):
        ref[...] = val
    norm_copies = [pltpu.make_async_copy(src, dst, sem.at[3, a])
                   for a, (src, dst) in enumerate(zip((snw, snm, snv, snb), outs[2]))]
    start(norm_copies)
    block(6, 0.0)
    start(embed_copies())
    lax.fori_loop(0, 4, down_step, 0)

    for a, staged in enumerate(seven_staged):
        pltpu.make_async_copy(staged.at[pl.ds(0, 6)], outs[0][a], sem.at[0, a]).wait()
    wait(embed_copies())
    wait(norm_copies)
    for a, staged in enumerate(down_staged):
        pltpu.make_async_copy(staged, outs[1][a], sem.at[2, a]).wait()


def local_update(g_layer, g_down, g_norm, g_embed, layer_w, layer_m, layer_v, down_w, down_m, down_v, norm_w, norm_m,
                 norm_v, embed_w, embed_m, embed_v):
    any_spec = pl.BlockSpec(memory_space=pl.ANY)
    vmem_spec = pl.BlockSpec(memory_space=pltpu.VMEM)
    dma = pltpu.SemaphoreType.DMA
    held = [(1, 128)] + [SEVEN, DOWN, NORM] + [SEVEN] * 3 + [DOWN] * 3 + [NORM] * 3
    reduced = pl.pallas_call(
        reduce_kernel,
        out_shape=[pltpu.VMEM(shape, F32) for shape in held],
        in_specs=[any_spec] * 16,
        out_specs=[vmem_spec] * len(held),
        scratch_shapes=[pltpu.VMEM((RING, 8, max(PART, PIECE)), F32)] * 2
        + [pltpu.VMEM(SEVEN, F32), pltpu.VMEM(DOWN, F32)] * 3
        + [pltpu.VMEM(NORM, F32)] * 5
        + [pltpu.VMEM((8, 128), F32)] * 2 + [pltpu.VMEM((4, 1, 128), F32), pltpu.VMEM((8, 1, 128), F32)]
        + [pltpu.VMEM((8, PART), F32)] + [pltpu.VMEM((FIRST, FIRST_COLS), F32)] * 2
        + [pltpu.VMEM((2, FIRST, FIRST_COLS), F32), pltpu.VMEM((FIRST, SPLIT), F32)]
        + [dma((RING,)), dma((RING,)), dma((M_RING,)), dma((Y_RING,)), dma((6,)), dma((4,)), dma((4,)), dma((10,)), dma,
           pltpu.SemaphoreType.REGULAR],
        compiler_params=pltpu.CompilerParams(collective_id=0, has_side_effects=True,
                                             vmem_limit_bytes=26 * 1024 * 1024),
    )(g_layer, g_down, g_norm, g_embed, layer_w, layer_m, layer_v, down_w, down_m, down_v, norm_w, norm_m, norm_v,
      embed_w, embed_m, embed_v)
    groups = ((6, ROWS, WIDTH), DOWN, NORM, (ROWS, WIDTH))
    out_shape = [jax.ShapeDtypeStruct(s, d) for s in groups for d in (F32, F32, F32, jnp.bfloat16)]
    staged = [pltpu.VMEM(s, d) for s in (SEVEN, DOWN, NORM) for d in (F32, F32, F32, jnp.bfloat16)]
    return pl.pallas_call(
        update_kernel,
        out_shape=out_shape,
        in_specs=[vmem_spec] * len(held),
        out_specs=[any_spec] * 16,
        scratch_shapes=staged + [dma((4, 4))],
        compiler_params=pltpu.CompilerParams(vmem_limit_bytes=26 * 1024 * 1024),
    )(*[pltpu.with_memory_space_constraint(a, pltpu.VMEM) for a in reduced])


def solution(mesh):
    grad_four = P(("dp", "fsdp"), None, None, None)
    grad_three = P(("dp", "fsdp"), None, None)
    layer_spec = P(None, "fsdp", None)
    down_spec = P("fsdp", None)
    norm_spec = P(None, "fsdp")
    embed_spec = P("fsdp", None)
    in_specs = (grad_four, grad_three, grad_three, grad_three,
                layer_spec, layer_spec, layer_spec, down_spec, down_spec, down_spec,
                norm_spec, norm_spec, norm_spec, embed_spec, embed_spec, embed_spec)
    out_specs = (layer_spec,) * 4 + (down_spec,) * 4 + (norm_spec,) * 4 + (embed_spec,) * 4
    return jax.shard_map(local_update, mesh=mesh, in_specs=in_specs, out_specs=out_specs, check_vma=False)
```

```python
import math

import jax
import jax.numpy as jnp
from jax import lax
from jax.experimental import pallas as pl
from jax.experimental.pallas import tpu as pltpu
from jax.sharding import PartitionSpec as P

ADAM_BETA1 = 0.9
ADAM_BETA2 = 0.95
ADAM_EPS = 1e-8
LEARN_RATE = 4e-4
WEIGHT_DECAY = 0.1
CLIP_EPS = 1e-6
OPT_STEP = 20
BIAS_ONE = 1.0 - ADAM_BETA1 ** OPT_STEP
BIAS_TWO = 1.0 - ADAM_BETA2 ** OPT_STEP
ROOT_TWO = math.sqrt(BIAS_TWO)
SMALLEST = 1.1754944e-38

MESH = pl.DeviceIdType.MESH
F32 = jnp.float32

ROWS = 64
WIDTH = 3072
FF = 8192
PIECE = 1024
NORM = (4, 768)
SEVEN = (7, ROWS, WIDTH)
DOWN = (ROWS, FF)

FIRST = 8
FIRST_COLS = 5120
SPLIT = FIRST_COLS // 2
PART = 1536
BLOCK = (ROWS // 8) * (WIDTH // PART)
N_EMBED = BLOCK
N_LAYER = N_EMBED + 6 * BLOCK
N_HALF = 3
N = N_LAYER + (FF // PIECE) * (ROWS // 8) - FIRST_COLS // PIECE

LEAD = 5
FETCH = 7
RING = 8
LAG = 5
Y_RING = 2 * LAG + 2
M_RING = RING + LEAD


class Chunk:
    def __init__(self, kind, k):
        self.kind = kind
        if kind in ("half", "down"):
            q = k - N_LAYER
            per = FF // PIECE
            self.width = PIECE
        else:
            q = k if kind == "embed" else (k - N_EMBED) % BLOCK
            per = WIDTH // PART
            self.width = PART
            self.j = 6 if kind == "embed" else (k - N_EMBED) // BLOCK
        self.row = pl.multiple_of((q // per) * 8, 8)
        self.rows = pl.ds(self.row, 8)
        self.col = (q % per) * self.width
        self.cols = pl.ds(pl.multiple_of(self.col, 512), self.width)

    def half(self, dp):
        half = self.width // 2
        return pl.ds(pl.multiple_of(self.col + dp * half, 512), half)

    def source(self, grads, q):
        g_layer, g_down, g_embed = grads
        rows = pl.ds(pl.multiple_of(q * ROWS + self.row, 8), 8)
        if self.kind == "embed":
            return g_embed.at[0, rows, self.cols]
        if self.kind == "layer":
            return g_layer.at[0, self.j, rows, self.cols]
        return g_down.at[0, rows, self.cols]

    def state(self, layer, down, embed):
        if self.kind == "embed":
            return embed.at[self.rows, self.cols]
        if self.kind == "layer":
            return layer.at[self.j, self.rows, self.cols]
        return down.at[self.rows, self.cols]

    def held(self, seven, down):
        if self.kind in ("half", "down"):
            return down.at[self.rows, self.cols]
        return seven.at[self.j, self.rows, self.cols]

    def ring(self, ring, s):
        return ring.at[s, :, pl.ds(0, self.width)]


def on_chunk(k, use):
    if isinstance(k, int):
        use(Chunk("embed", k))
        return
    bounds = (0, N_EMBED, N_LAYER, N_LAYER + N_HALF, N)
    for i, kind in enumerate(("embed", "layer", "half", "down")):
        @pl.when(jnp.logical_and(k >= bounds[i], k < bounds[i + 1]))
        def _():
            use(Chunk(kind, k))


def start(copies):
    for copy in copies:
        copy.start()


def wait(copies):
    for copy in copies:
        copy.wait()


def take(ref, sem):
    pltpu.make_async_copy(ref, ref, sem).wait()


def squares(mean, width):
    parts = [mean[r:r + 8, i * 128:(i + 1) * 128] for r in range(0, mean.shape[0], 8) for i in range(width // 128)]
    sums = [p * p for p in parts[:4]]
    for i, p in enumerate(parts[4:]):
        sums[i % 4] = sums[i % 4] + p * p
    return (sums[0] + sums[1]) + (sums[2] + sums[3])


def reduce_kernel(g_layer, g_down, g_norm, g_embed, layer_w, layer_m, layer_v, down_w, down_m, down_v,
                  norm_w, norm_m, norm_v, embed_w, embed_m, embed_v,
                  sq_out, g7, gd, gn, w7, m7, v7, wd, md, vd, wn, mn, vn,
                  own_o, par_o, pm7, pmd, x7, xd, y7, yd, own_no, par_no, pmn, xn, yn, acc, acc_first, sq_all, sq_first,
                  pre, fo_own, fo_par, f_held, f_y,
                  out_sem, other_sem, mine_sem, y_sem, st_sem, n_sem, sq_sem, f_sem, pre_sem, credit):
    dp = lax.axis_index("dp")
    f = lax.axis_index("fsdp")
    core = lax.rem(f, 2)
    f_core = f + 1 - 2 * core
    f_x = lax.rem(f + 2, 4)
    f_diag = lax.rem(f_core + 2, 4)
    peer_core = (dp, f_core)
    peer_x = (dp, f_x)
    peer_diag = (dp, f_diag)
    peer_y = (1 - dp, f)
    peers = (peer_core, peer_x, peer_diag, peer_y, (1 - dp, f_core), (1 - dp, f_x), (1 - dp, f_diag))

    def remote(src, dst, send, recv, peer):
        return pltpu.make_async_remote_copy(src_ref=src, dst_ref=dst, send_sem=send, recv_sem=recv,
                                            device_id=peer, device_id_type=MESH)

    grads = (g_layer, g_down, g_embed)

    def x_copy(k, chunk):
        s = lax.rem(k, RING)
        return remote(chunk.ring(own_o, s), chunk.held(x7, xd), out_sem.at[s], mine_sem.at[lax.rem(k, M_RING)], peer_x)

    def y_copy(k, chunk):
        sem = y_sem.at[lax.rem(k, Y_RING)]
        return remote(chunk.held(g7, gd), chunk.held(y7, yd), sem, sem, peer_y)

    def half_copy(k, chunk):
        sem = y_sem.at[lax.rem(k, Y_RING)]
        give = chunk.half(1 - dp)
        return remote(gd.at[chunk.rows, give], yd.at[chunk.rows, give], sem, sem, peer_y)

    def by_core(chunk, on_whole, on_half):
        if chunk.kind == "half":
            pl.when(core == 0)(on_half)
            pl.when(core == 1)(on_whole)
        else:
            on_whole()

    def push_other(k, chunk, source):
        s = lax.rem(k, RING)
        return remote(source, chunk.ring(par_o, s), out_sem.at[s], other_sem.at[s], peer_core)

    def push_mine(k, chunk, source):
        s = lax.rem(k, RING)
        return remote(source, chunk.held(pm7, pmd), out_sem.at[s], mine_sem.at[lax.rem(k, M_RING)], peer_core)

    def own_loads(k, chunk):
        s = lax.rem(k, RING)
        return [pltpu.make_async_copy(chunk.source(grads, f_x), chunk.ring(own_o, s), other_sem.at[s]),
                pltpu.make_async_copy(chunk.source(grads, f), chunk.held(g7, gd), mine_sem.at[lax.rem(k, M_RING)])]

    def times(count, chunk):
        return own_o.at[pl.ds(0, count), :, pl.ds(0, chunk.width)]

    def retire(k, chunk):
        take(times(3, chunk), out_sem.at[lax.rem(k, RING)])

    def fetch(k):
        @pl.when(jnp.logical_and(k >= RING, k < N))
        def _():
            on_chunk(k - RING, lambda chunk: retire(k - RING, chunk))
            pl.semaphore_wait(credit, 1)

        def begin(chunk):
            push_other(k, chunk, chunk.source(grads, f_diag)).start()
            for copy in own_loads(k, chunk):
                copy.start()
            push_mine(k, chunk, chunk.source(grads, f_core)).start()

        on_chunk(k, begin)

    def sum_x(k):
        def use(chunk):
            take(times(3, chunk), mine_sem.at[lax.rem(k, M_RING)])
            mine = chunk.held(g7, gd)
            theirs = chunk.held(pm7, pmd)
            mine[...] = (mine[...] + theirs[...]) + chunk.held(x7, xd)[...]

        on_chunk(k, use)

    def sum_chip(k):
        s = lax.rem(k, RING)

        def use(chunk):
            mine = chunk.ring(own_o, s)
            theirs = chunk.ring(par_o, s)
            take(times(2, chunk), other_sem.at[s])
            mine[...] = mine[...] + theirs[...]

        on_chunk(k, use)

    def start_x(k):
        on_chunk(k, lambda chunk: x_copy(k, chunk).start())

        @pl.when(jnp.logical_and(k >= 0, k < N - RING))
        def _():
            pl.semaphore_signal(credit, inc=1, device_id=peer_core, device_id_type=MESH)

    def start_y(k):
        def use(chunk):
            by_core(chunk, lambda: y_copy(k, chunk).start(), lambda: half_copy(k, chunk).start())
            seven = chunk.kind in ("embed", "layer")
            for i, (src, dst) in enumerate((((layer_w, down_w, embed_w), (w7, wd)), ((layer_m, down_m, embed_m), (m7, md)),
                                            ((layer_v, down_v, embed_v), (v7, vd)))):
                pltpu.make_async_copy(chunk.state(*src), chunk.held(*dst), st_sem.at[i if seven else 3 + i]).start()

        on_chunk(k, use)

    def sum_y(k):
        def use(chunk):
            sem = y_sem.at[lax.rem(k, Y_RING)]

            def whole():
                take(times(2, chunk), sem)
                mine = chunk.held(g7, gd)
                mean = (mine[...] + chunk.held(y7, yd)[...]) * 0.125
                mine[...] = mean
                acc[...] += squares(mean, chunk.width)

            def half():
                take(times(1, chunk), sem)
                keep = chunk.half(dp)
                mean = (gd[chunk.rows, keep] + yd[chunk.rows, keep]) * 0.125
                gd[chunk.rows, keep] = mean
                acc_first[...] += squares(mean, chunk.width // 2)

            by_core(chunk, whole, half)

        on_chunk(k, use)

    last = pl.ds(ROWS - FIRST, FIRST)
    keep = pl.ds(pl.multiple_of(FF - FIRST_COLS + dp * SPLIT, PIECE // 2), SPLIT)
    give = pl.ds(pl.multiple_of(FF - FIRST_COLS + (1 - dp) * SPLIT, PIECE // 2), SPLIT)
    cols = pl.ds(FF - FIRST_COLS, FIRST_COLS)
    keep_o = pl.ds(pl.multiple_of(dp * SPLIT, PIECE // 2), SPLIT)
    give_o = pl.ds(pl.multiple_of((1 - dp) * SPLIT, PIECE // 2), SPLIT)

    def first_rows(q):
        return g_down.at[0, pl.ds(pl.multiple_of(q * ROWS + (ROWS - FIRST), 8), FIRST), cols]

    f_own = gd.at[last, cols]
    f_give = [pltpu.make_async_copy(first_rows(q), f_held.at[i], f_sem.at[0]) for i, q in enumerate((f_diag, f_core))]
    f_local = [pltpu.make_async_copy(first_rows(f_x), fo_own, f_sem.at[1]),
               pltpu.make_async_copy(first_rows(f), f_own, f_sem.at[1])]
    f_push = []
    for h, (half, half_o) in enumerate(((give, give_o), (keep, keep_o))):
        for i, ref in enumerate((fo_par.at[:, half_o], pmd.at[last, half])):
            f_push.append(remote(f_held.at[i, :, half_o], ref, f_sem.at[2],
                                 f_sem.at[3 + i] if h == 0 else f_sem.at[5], peer_core))
    f_state = [pltpu.make_async_copy(src.at[last, cols], dst.at[last, cols], st_sem.at[3 + i])
               for i, (src, dst) in enumerate(((down_w, wd), (down_m, md), (down_v, vd)))]
    f_scatter = [remote(fo_own.at[:, give_o], f_y, f_sem.at[6], f_sem.at[6], peer_y),
                 remote(gd.at[last, give], yd.at[last, give], f_sem.at[6], f_sem.at[6], peer_y)]
    f_cross = remote(fo_own.at[:, keep_o], xd.at[last, keep], f_sem.at[7], f_sem.at[7], peer_x)
    f_gather = remote(gd.at[last, keep], yd.at[last, keep], f_sem.at[8], f_sem.at[8], peer_y)
    halves = [Chunk("half", N_LAYER + i) for i in range(N_HALF)]
    h_gather = [remote(gd.at[chunk.rows, chunk.half(dp)], yd.at[chunk.rows, chunk.half(dp)], f_sem.at[9], f_sem.at[9],
                       peer_y) for chunk in halves]
    me = dp * 4 + f
    sqf_copies = [remote(sq_first.at[me], sq_first.at[me], sq_sem.at[0], sq_sem.at[1], peer)
                  for peer in peers]

    def norm_source(q):
        return g_norm.at[0, :, pl.ds(pl.multiple_of(q * NORM[1], 128), NORM[1])]

    n_push_other = remote(norm_source(f_diag), par_no, n_sem.at[1], n_sem.at[0], peer_core)
    n_push_mine = remote(norm_source(f_core), pmn, n_sem.at[1], n_sem.at[0], peer_core)
    n_x = remote(own_no, xn, n_sem.at[2], n_sem.at[2], peer_x)
    n_y = remote(gn, yn, n_sem.at[3], n_sem.at[3], peer_y)
    n_local = [pltpu.make_async_copy(src, dst, n_sem.at[0]) for src, dst in
               ((norm_source(f_x), own_no), (norm_source(f), gn), (norm_w, wn), (norm_m, mn), (norm_v, vn))]

    def n_times(count):
        return fo_par.at[:, pl.ds(0, count * NORM[0] * NORM[1] // 8)]


    barrier = pltpu.get_barrier_semaphore()
    near = (peer_core, peer_x, peer_y)
    for peer in near:
        pl.semaphore_signal(barrier, inc=1, device_id=peer, device_id_type=MESH)
    zero = Chunk("embed", 0)
    ahead = pltpu.make_async_copy(zero.source(grads, f_diag), pre, pre_sem)
    ahead.start()
    for copy in own_loads(0, zero):
        copy.start()
    for copy in f_give + f_local:
        copy.start()
    acc[...] = jnp.zeros_like(acc)
    acc_first[...] = jnp.zeros_like(acc_first)

    take(f_held, f_sem.at[0])
    pl.semaphore_wait(barrier, len(near))
    f_push[0].start()
    ahead.wait()
    push_other(0, zero, pre).start()
    f_push[1].start()
    start(f_push[2:])
    push_mine(0, zero, zero.source(grads, f_core)).start()
    for k in range(1, FETCH - LEAD + 1):
        fetch(k)
    take(f_held, f_sem.at[1])
    take(fo_par.at[:, give_o], f_sem.at[3])
    fo_own[:, give_o] = fo_own[:, give_o] + fo_par[:, give_o]
    f_scatter[0].start()
    sum_chip(0)
    start_x(0)
    take(fo_par.at[:, give_o], f_sem.at[4])
    gd[last, give] = gd[last, give] + pmd[last, give]
    f_scatter[1].start()
    take(fo_par, f_sem.at[5])
    take(f_held, f_sem.at[2])
    fo_own[:, keep_o] = fo_own[:, keep_o] + fo_par[:, keep_o]
    gd[last, keep] = gd[last, keep] + pmd[last, keep]
    start(f_state)

    def step(t, _):
        i = t - FETCH
        fetch(i + FETCH)

        @pl.when(i == 0)
        def _():
            n_push_other.start()
            n_push_mine.start()
            for copy in n_local:
                copy.start()

        sum_x(i)
        sum_chip(i + LEAD)
        start_y(i)
        start_x(i + LEAD)

        @pl.when(i == 3)
        def _():
            take(n_times(7), n_sem.at[0])
            take(n_times(2), n_sem.at[1])
            own_no[...] = own_no[...] + par_no[...]
            n_x.start()

        @pl.when(i == 10)
        def _():
            take(n_times(2), n_sem.at[2])
            gn[...] = (gn[...] + pmn[...]) + xn[...]
            n_y.start()
            take(f_held, f_sem.at[6])
            fo_own[:, keep_o] = fo_own[:, keep_o] + f_y[...]
            gd[last, keep] = gd[last, keep] + yd[last, keep]

        @pl.when(i == 20)
        def _():
            take(n_times(2), n_sem.at[3])
            mean = (gn[...] + yn[...]) * 0.125
            gn[...] = mean
            square = mean * mean
            total = square[:, 0:128]
            for c in range(1, NORM[1] // 128):
                total = total + square[:, c * 128:(c + 1) * 128]
            acc[0:4, :] += total

        @pl.when(i == N - LEAD)
        def _():
            f_cross.start()

        @pl.when(jnp.logical_and(i == N, core == 0))
        def _():
            start(h_gather)

        @pl.when(i == N + LAG - 3)
        def _():
            take(fo_par, f_sem.at[7])
            mean = (gd[last, keep] + xd[last, keep]) * 0.125
            gd[last, keep] = mean
            sq_first[me] = jnp.sum(acc_first[...] + squares(mean, SPLIT), axis=0, keepdims=True)
            f_gather.start()
            start(sqf_copies)

        sum_y(i - LAG)
        return 0

    lax.fori_loop(FETCH - LEAD + 1, FETCH + N + LAG, step, 0)

    sq_all[f] = jnp.sum(acc[...], axis=0, keepdims=True)
    copies = [remote(sq_all.at[f], sq_all.at[f], sq_sem.at[2], sq_sem.at[3], peer)
              for peer in (peer_core, peer_x, peer_diag)]
    for copy in copies:
        copy.start()

    def drain(k, _):
        on_chunk(k, lambda chunk: retire(k, chunk))
        return 0

    lax.fori_loop(N - RING, N, drain, 0)
    for i, ref in enumerate((w7, m7, v7, wd, md, vd)):
        pltpu.make_async_copy(ref, ref, st_sem.at[i]).wait()

    @pl.when(core == 0)
    def _():
        take(gd.at[pl.ds(0, 8), pl.ds(0, N_HALF * PIECE)], f_sem.at[9])
        for chunk in halves:
            gd[chunk.rows, chunk.half(1 - dp)] = yd[chunk.rows, chunk.half(1 - dp)]

    take(fo_par, f_sem.at[8])
    gd[last, give] = yd[last, give]
    take(sq_first.at[pl.ds(0, 7)], sq_sem.at[0])
    take(sq_first.at[pl.ds(0, 7)], sq_sem.at[1])
    total = sq_first[0]
    for i in range(1, 8):
        total = total + sq_first[i]
    take(sq_all.at[pl.ds(0, 3)], sq_sem.at[2])
    take(sq_all.at[pl.ds(0, 3)], sq_sem.at[3])
    sq_out[...] = ((sq_all[0] + sq_all[1]) + (sq_all[2] + sq_all[3])) + total


def update_math(avg_scale, sq_scale, g, w, m, v, decay):
    avg = ADAM_BETA1 * m + avg_scale * g
    root = sq_scale * g
    sq = ADAM_BETA2 * v + root * root
    dev = sq * lax.rsqrt(jnp.maximum(sq, SMALLEST))
    step_dir = avg / (dev + ADAM_EPS * ROOT_TWO)
    new = (1.0 - LEARN_RATE * decay) * w - (LEARN_RATE * ROOT_TWO / BIAS_ONE) * step_dir
    return new, avg, sq, new.astype(jnp.bfloat16)


def update_kernel(sq, g7, gd, gn, w7, m7, v7, wd, md, vd, wn, mn, vn,
                  lw, lm, lv, lb, dw, dm, dv, db, nw, nm, nv, nb, ew, em, ev, eb,
                  s7w, s7m, s7v, s7b, sdw, sdm, sdv, sdb, snw, snm, snv, snb, sem):
    total = jnp.sum(sq[...], keepdims=True)
    clip = jnp.minimum(1.0, 1.0 / (jnp.sqrt(total) + CLIP_EPS))
    scales = ((1.0 - ADAM_BETA1) * clip, math.sqrt(1.0 - ADAM_BETA2) * clip)

    outs = ((lw, lm, lv, lb), (dw, dm, dv, db), (nw, nm, nv, nb), (ew, em, ev, eb))
    seven_staged = (s7w, s7m, s7v, s7b)
    down_staged = (sdw, sdm, sdv, sdb)

    def layer_copies(j, row, rows):
        at = pl.ds(row, rows)
        return [pltpu.make_async_copy(src.at[j, at, :], dst.at[j, at, :], sem.at[0, a])
                for a, (src, dst) in enumerate(zip(seven_staged, outs[0]))]

    def embed_copies():
        return [pltpu.make_async_copy(src.at[6], dst, sem.at[1, a])
                for a, (src, dst) in enumerate(zip(seven_staged, outs[3]))]

    def down_copies(t):
        at = pl.ds(pl.multiple_of(t * 16, 16), 16)
        return [pltpu.make_async_copy(src.at[at, :], dst.at[at, :], sem.at[2, a])
                for a, (src, dst) in enumerate(zip(down_staged, outs[1]))]

    def seven(j, row, decay):
        for c in range(0, WIDTH, 512):
            ix = (j, pl.ds(row, 16), pl.ds(c, 512))
            out = update_math(*scales, g7[ix], w7[ix], m7[ix], v7[ix], decay)
            for ref, val in zip(seven_staged, out):
                ref[ix] = val

    def block(j, decay):
        def rows(t, _):
            seven(j, pl.multiple_of(t * 16, 16), decay)
            return 0

        lax.fori_loop(0, 4, rows, 0)

    def first_step(t, _):
        row = pl.multiple_of(t * 16, 16)
        seven(0, row, WEIGHT_DECAY)
        start(layer_copies(0, row, 16))
        return 0

    def half_step(t, _):
        seven(1, pl.multiple_of(t * 32, 32), WEIGHT_DECAY)
        seven(1, pl.multiple_of(t * 32 + 16, 16), WEIGHT_DECAY)
        start(layer_copies(1, pl.multiple_of(t * 32, 32), 32))
        return 0

    def layer_step(j, _):
        block(j, WEIGHT_DECAY)
        start(layer_copies(j, 0, ROWS))
        return 0

    def down_step(t, _):
        row = pl.multiple_of(t * 16, 16)

        def cols(u, _):
            ix = (pl.ds(row, 16), pl.ds(pl.multiple_of(u * 1024, 1024), 1024))
            out = update_math(*scales, gd[ix], wd[ix], md[ix], vd[ix], WEIGHT_DECAY)
            for ref, val in zip(down_staged, out):
                ref[ix] = val
            return 0

        lax.fori_loop(0, FF // 1024, cols, 0)
        start(down_copies(t))
        return 0

    lax.fori_loop(0, 4, first_step, 0)
    lax.fori_loop(1, 6, layer_step, 0)
    out = update_math(*scales, gn[...], wn[...], mn[...], vn[...], WEIGHT_DECAY)
    for ref, val in zip((snw, snm, snv, snb), out):
        ref[...] = val
    norm_copies = [pltpu.make_async_copy(src, dst, sem.at[3, a])
                   for a, (src, dst) in enumerate(zip((snw, snm, snv, snb), outs[2]))]
    start(norm_copies)
    block(6, 0.0)
    start(embed_copies())
    lax.fori_loop(0, 4, down_step, 0)

    for a, staged in enumerate(seven_staged):
        pltpu.make_async_copy(staged.at[pl.ds(0, 6)], outs[0][a], sem.at[0, a]).wait()
    wait(embed_copies())
    wait(norm_copies)
    for a, staged in enumerate(down_staged):
        pltpu.make_async_copy(staged, outs[1][a], sem.at[2, a]).wait()


def local_update(g_layer, g_down, g_norm, g_embed, layer_w, layer_m, layer_v, down_w, down_m, down_v, norm_w, norm_m,
                 norm_v, embed_w, embed_m, embed_v):
    any_spec = pl.BlockSpec(memory_space=pl.ANY)
    vmem_spec = pl.BlockSpec(memory_space=pltpu.VMEM)
    dma = pltpu.SemaphoreType.DMA
    held = [(1, 128)] + [SEVEN, DOWN, NORM] + [SEVEN] * 3 + [DOWN] * 3 + [NORM] * 3
    reduced = pl.pallas_call(
        reduce_kernel,
        out_shape=[pltpu.VMEM(shape, F32) for shape in held],
        in_specs=[any_spec] * 16,
        out_specs=[vmem_spec] * len(held),
        scratch_shapes=[pltpu.VMEM((RING, 8, max(PART, PIECE)), F32)] * 2
        + [pltpu.VMEM(SEVEN, F32), pltpu.VMEM(DOWN, F32)] * 3
        + [pltpu.VMEM(NORM, F32)] * 5
        + [pltpu.VMEM((8, 128), F32)] * 2 + [pltpu.VMEM((4, 1, 128), F32), pltpu.VMEM((8, 1, 128), F32)]
        + [pltpu.VMEM((8, PART), F32)] + [pltpu.VMEM((FIRST, FIRST_COLS), F32)] * 2
        + [pltpu.VMEM((2, FIRST, FIRST_COLS), F32), pltpu.VMEM((FIRST, SPLIT), F32)]
        + [dma((RING,)), dma((RING,)), dma((M_RING,)), dma((Y_RING,)), dma((6,)), dma((4,)), dma((4,)), dma((10,)), dma,
           pltpu.SemaphoreType.REGULAR],
        compiler_params=pltpu.CompilerParams(collective_id=0, has_side_effects=True,
                                             vmem_limit_bytes=26 * 1024 * 1024),
    )(g_layer, g_down, g_norm, g_embed, layer_w, layer_m, layer_v, down_w, down_m, down_v, norm_w, norm_m, norm_v,
      embed_w, embed_m, embed_v)
    groups = ((6, ROWS, WIDTH), DOWN, NORM, (ROWS, WIDTH))
    out_shape = [jax.ShapeDtypeStruct(s, d) for s in groups for d in (F32, F32, F32, jnp.bfloat16)]
    staged = [pltpu.VMEM(s, d) for s in (SEVEN, DOWN, NORM) for d in (F32, F32, F32, jnp.bfloat16)]
    return pl.pallas_call(
        update_kernel,
        out_shape=out_shape,
        in_specs=[vmem_spec] * len(held),
        out_specs=[any_spec] * 16,
        scratch_shapes=staged + [dma((4, 4))],
        compiler_params=pltpu.CompilerParams(vmem_limit_bytes=26 * 1024 * 1024),
    )(*[pltpu.with_memory_space_constraint(a, pltpu.VMEM) for a in reduced])


def solution(mesh):
    grad_four = P(("dp", "fsdp"), None, None, None)
    grad_three = P(("dp", "fsdp"), None, None)
    layer_spec = P(None, "fsdp", None)
    down_spec = P("fsdp", None)
    norm_spec = P(None, "fsdp")
    embed_spec = P("fsdp", None)
    in_specs = (grad_four, grad_three, grad_three, grad_three,
                layer_spec, layer_spec, layer_spec, down_spec, down_spec, down_spec,
                norm_spec, norm_spec, norm_spec, embed_spec, embed_spec, embed_spec)
    out_specs = (layer_spec,) * 4 + (down_spec,) * 4 + (norm_spec,) * 4 + (embed_spec,) * 4
    return jax.shard_map(local_update, mesh=mesh, in_specs=in_specs, out_specs=out_specs, check_vma=False)
```

```python
import math

import jax
import jax.numpy as jnp
from jax import lax
from jax.experimental import pallas as pl
from jax.experimental.pallas import tpu as pltpu
from jax.sharding import PartitionSpec as P

ADAM_BETA1 = 0.9
ADAM_BETA2 = 0.95
ADAM_EPS = 1e-8
LEARN_RATE = 4e-4
WEIGHT_DECAY = 0.1
CLIP_EPS = 1e-6
OPT_STEP = 20
BIAS_ONE = 1.0 - ADAM_BETA1 ** OPT_STEP
BIAS_TWO = 1.0 - ADAM_BETA2 ** OPT_STEP
ROOT_TWO = math.sqrt(BIAS_TWO)
SMALLEST = 1.1754944e-38

MESH = pl.DeviceIdType.MESH
F32 = jnp.float32

ROWS = 64
WIDTH = 3072
FF = 8192
PIECE = 1024
NORM = (4, 768)
SEVEN = (7, ROWS, WIDTH)
DOWN = (ROWS, FF)

FIRST = 8
FIRST_COLS = 5120
SPLIT = FIRST_COLS // 2
PART = 1536
BLOCK = (ROWS // 8) * (WIDTH // PART)
N_EMBED = BLOCK
N_LAYER = N_EMBED + 6 * BLOCK
N_HALF = 3
N = N_LAYER + (FF // PIECE) * (ROWS // 8) - FIRST_COLS // PIECE

LEAD = 5
FETCH = 7
RING = 8
LAG = 5
Y_RING = 2 * LAG + 2
M_RING = RING + LEAD


class Chunk:
    def __init__(self, kind, k):
        self.kind = kind
        if kind in ("half", "down"):
            q = k - N_LAYER
            per = FF // PIECE
            self.width = PIECE
        else:
            q = k if kind == "embed" else (k - N_EMBED) % BLOCK
            per = WIDTH // PART
            self.width = PART
            self.j = 6 if kind == "embed" else (k - N_EMBED) // BLOCK
        self.row = pl.multiple_of((q // per) * 8, 8)
        self.rows = pl.ds(self.row, 8)
        self.col = (q % per) * self.width
        self.cols = pl.ds(pl.multiple_of(self.col, 512), self.width)

    def half(self, dp):
        half = self.width // 2
        return pl.ds(pl.multiple_of(self.col + dp * half, 512), half)

    def source(self, grads, q):
        g_layer, g_down, g_embed = grads
        rows = pl.ds(pl.multiple_of(q * ROWS + self.row, 8), 8)
        if self.kind == "embed":
            return g_embed.at[0, rows, self.cols]
        if self.kind == "layer":
            return g_layer.at[0, self.j, rows, self.cols]
        return g_down.at[0, rows, self.cols]

    def state(self, layer, down, embed):
        if self.kind == "embed":
            return embed.at[self.rows, self.cols]
        if self.kind == "layer":
            return layer.at[self.j, self.rows, self.cols]
        return down.at[self.rows, self.cols]

    def held(self, seven, down):
        if self.kind in ("half", "down"):
            return down.at[self.rows, self.cols]
        return seven.at[self.j, self.rows, self.cols]

    def ring(self, ring, s):
        return ring.at[s, :, pl.ds(0, self.width)]


def on_chunk(k, use):
    if isinstance(k, int):
        use(Chunk("embed", k))
        return
    bounds = (0, N_EMBED, N_LAYER, N_LAYER + N_HALF, N)
    for i, kind in enumerate(("embed", "layer", "half", "down")):
        @pl.when(jnp.logical_and(k >= bounds[i], k < bounds[i + 1]))
        def _():
            use(Chunk(kind, k))


def start(copies):
    for copy in copies:
        copy.start()


def wait(copies):
    for copy in copies:
        copy.wait()


def take(ref, sem):
    pltpu.make_async_copy(ref, ref, sem).wait()


def squares(mean, width):
    parts = [mean[r:r + 8, i * 128:(i + 1) * 128] for r in range(0, mean.shape[0], 8) for i in range(width // 128)]
    sums = [p * p for p in parts[:4]]
    for i, p in enumerate(parts[4:]):
        sums[i % 4] = sums[i % 4] + p * p
    return (sums[0] + sums[1]) + (sums[2] + sums[3])


def reduce_kernel(g_layer, g_down, g_norm, g_embed, layer_w, layer_m, layer_v, down_w, down_m, down_v,
                  norm_w, norm_m, norm_v, embed_w, embed_m, embed_v,
                  sq_out, g7, gd, gn, w7, m7, v7, wd, md, vd, wn, mn, vn,
                  own_o, par_o, pm7, pmd, x7, xd, y7, yd, own_no, par_no, pmn, xn, yn, acc, acc_first, sq_all, sq_first,
                  pre, fo_own, fo_par, f_held, f_y,
                  out_sem, other_sem, mine_sem, y_sem, st_sem, n_sem, sq_sem, f_sem, pre_sem, credit):
    dp = lax.axis_index("dp")
    f = lax.axis_index("fsdp")
    core = lax.rem(f, 2)
    f_core = f + 1 - 2 * core
    f_x = lax.rem(f + 2, 4)
    f_diag = lax.rem(f_core + 2, 4)
    peer_core = (dp, f_core)
    peer_x = (dp, f_x)
    peer_diag = (dp, f_diag)
    peer_y = (1 - dp, f)
    peers = (peer_core, peer_x, peer_diag, peer_y, (1 - dp, f_core), (1 - dp, f_x), (1 - dp, f_diag))

    def remote(src, dst, send, recv, peer):
        return pltpu.make_async_remote_copy(src_ref=src, dst_ref=dst, send_sem=send, recv_sem=recv,
                                            device_id=peer, device_id_type=MESH)

    grads = (g_layer, g_down, g_embed)

    def x_copy(k, chunk):
        s = lax.rem(k, RING)
        return remote(chunk.ring(own_o, s), chunk.held(x7, xd), out_sem.at[s], mine_sem.at[lax.rem(k, M_RING)], peer_x)

    def y_copy(k, chunk):
        sem = y_sem.at[lax.rem(k, Y_RING)]
        return remote(chunk.held(g7, gd), chunk.held(y7, yd), sem, sem, peer_y)

    def half_copy(k, chunk):
        sem = y_sem.at[lax.rem(k, Y_RING)]
        give = chunk.half(1 - dp)
        return remote(gd.at[chunk.rows, give], yd.at[chunk.rows, give], sem, sem, peer_y)

    def by_core(chunk, on_whole, on_half):
        if chunk.kind == "half":
            pl.when(core == 0)(on_half)
            pl.when(core == 1)(on_whole)
        else:
            on_whole()

    def push_other(k, chunk, source):
        s = lax.rem(k, RING)
        return remote(source, chunk.ring(par_o, s), out_sem.at[s], other_sem.at[s], peer_core)

    def push_mine(k, chunk, source):
        s = lax.rem(k, RING)
        return remote(source, chunk.held(pm7, pmd), out_sem.at[s], mine_sem.at[lax.rem(k, M_RING)], peer_core)

    def own_loads(k, chunk):
        s = lax.rem(k, RING)
        return [pltpu.make_async_copy(chunk.source(grads, f_x), chunk.ring(own_o, s), other_sem.at[s]),
                pltpu.make_async_copy(chunk.source(grads, f), chunk.held(g7, gd), mine_sem.at[lax.rem(k, M_RING)])]

    def times(count, chunk):
        return own_o.at[pl.ds(0, count), :, pl.ds(0, chunk.width)]

    def retire(k, chunk):
        take(times(3, chunk), out_sem.at[lax.rem(k, RING)])

    def fetch(k):
        @pl.when(jnp.logical_and(k >= RING, k < N))
        def _():
            on_chunk(k - RING, lambda chunk: retire(k - RING, chunk))
            pl.semaphore_wait(credit, 1)

        def begin(chunk):
            push_other(k, chunk, chunk.source(grads, f_diag)).start()
            for copy in own_loads(k, chunk):
                copy.start()
            push_mine(k, chunk, chunk.source(grads, f_core)).start()

        on_chunk(k, begin)

    def sum_x(k):
        def use(chunk):
            take(times(3, chunk), mine_sem.at[lax.rem(k, M_RING)])
            mine = chunk.held(g7, gd)
            theirs = chunk.held(pm7, pmd)
            mine[...] = (mine[...] + theirs[...]) + chunk.held(x7, xd)[...]

        on_chunk(k, use)

    def sum_chip(k):
        s = lax.rem(k, RING)

        def use(chunk):
            mine = chunk.ring(own_o, s)
            theirs = chunk.ring(par_o, s)
            take(times(2, chunk), other_sem.at[s])
            mine[...] = mine[...] + theirs[...]

        on_chunk(k, use)

    def start_x(k):
        on_chunk(k, lambda chunk: x_copy(k, chunk).start())

        @pl.when(jnp.logical_and(k >= 0, k < N - RING))
        def _():
            pl.semaphore_signal(credit, inc=1, device_id=peer_core, device_id_type=MESH)

    def start_y(k):
        def use(chunk):
            by_core(chunk, lambda: y_copy(k, chunk).start(), lambda: half_copy(k, chunk).start())
            seven = chunk.kind in ("embed", "layer")
            for i, (src, dst) in enumerate((((layer_w, down_w, embed_w), (w7, wd)), ((layer_m, down_m, embed_m), (m7, md)),
                                            ((layer_v, down_v, embed_v), (v7, vd)))):
                pltpu.make_async_copy(chunk.state(*src), chunk.held(*dst), st_sem.at[0 if seven else 1]).start()

        on_chunk(k, use)

    def sum_y(k):
        def use(chunk):
            sem = y_sem.at[lax.rem(k, Y_RING)]

            def whole():
                take(times(2, chunk), sem)
                mine = chunk.held(g7, gd)
                mean = (mine[...] + chunk.held(y7, yd)[...]) * 0.125
                mine[...] = mean
                acc[...] += squares(mean, chunk.width)

            def half():
                take(times(1, chunk), sem)
                keep = chunk.half(dp)
                mean = (gd[chunk.rows, keep] + yd[chunk.rows, keep]) * 0.125
                gd[chunk.rows, keep] = mean
                acc_first[...] += squares(mean, chunk.width // 2)

            by_core(chunk, whole, half)

        on_chunk(k, use)

    last = pl.ds(ROWS - FIRST, FIRST)
    keep = pl.ds(pl.multiple_of(FF - FIRST_COLS + dp * SPLIT, PIECE // 2), SPLIT)
    give = pl.ds(pl.multiple_of(FF - FIRST_COLS + (1 - dp) * SPLIT, PIECE // 2), SPLIT)
    cols = pl.ds(FF - FIRST_COLS, FIRST_COLS)
    keep_o = pl.ds(pl.multiple_of(dp * SPLIT, PIECE // 2), SPLIT)
    give_o = pl.ds(pl.multiple_of((1 - dp) * SPLIT, PIECE // 2), SPLIT)

    def first_rows(q):
        return g_down.at[0, pl.ds(pl.multiple_of(q * ROWS + (ROWS - FIRST), 8), FIRST), cols]

    f_own = gd.at[last, cols]
    f_give = [pltpu.make_async_copy(first_rows(q), f_held.at[i], f_sem.at[0]) for i, q in enumerate((f_diag, f_core))]
    f_local = [pltpu.make_async_copy(first_rows(f_x), fo_own, f_sem.at[1]),
               pltpu.make_async_copy(first_rows(f), f_own, f_sem.at[1])]
    f_push = []
    for h, (half, half_o) in enumerate(((give, give_o), (keep, keep_o))):
        for i, ref in enumerate((fo_par.at[:, half_o], pmd.at[last, half])):
            f_push.append(remote(f_held.at[i, :, half_o], ref, f_sem.at[2],
                                 f_sem.at[3 + i] if h == 0 else f_sem.at[5], peer_core))
    f_state = [pltpu.make_async_copy(src.at[last, cols], dst.at[last, cols], st_sem.at[1])
               for i, (src, dst) in enumerate(((down_w, wd), (down_m, md), (down_v, vd)))]
    f_scatter = [remote(fo_own.at[:, give_o], f_y, f_sem.at[6], f_sem.at[6], peer_y),
                 remote(gd.at[last, give], yd.at[last, give], f_sem.at[6], f_sem.at[6], peer_y)]
    f_cross = remote(fo_own.at[:, keep_o], xd.at[last, keep], f_sem.at[7], f_sem.at[7], peer_x)
    f_gather = remote(gd.at[last, keep], yd.at[last, keep], f_sem.at[8], f_sem.at[8], peer_y)
    halves = [Chunk("half", N_LAYER + i) for i in range(N_HALF)]
    h_gather = [remote(gd.at[chunk.rows, chunk.half(dp)], yd.at[chunk.rows, chunk.half(dp)], f_sem.at[9], f_sem.at[9],
                       peer_y) for chunk in halves]
    me = dp * 4 + f
    sqf_copies = [remote(sq_first.at[me], sq_first.at[me], sq_sem.at[0], sq_sem.at[1], peer)
                  for peer in peers]

    def norm_source(q):
        return g_norm.at[0, :, pl.ds(pl.multiple_of(q * NORM[1], 128), NORM[1])]

    n_push_other = remote(norm_source(f_diag), par_no, n_sem.at[1], n_sem.at[0], peer_core)
    n_push_mine = remote(norm_source(f_core), pmn, n_sem.at[1], n_sem.at[0], peer_core)
    n_x = remote(own_no, xn, n_sem.at[2], n_sem.at[2], peer_x)
    n_y = remote(gn, yn, n_sem.at[3], n_sem.at[3], peer_y)
    n_local = [pltpu.make_async_copy(src, dst, n_sem.at[0]) for src, dst in
               ((norm_source(f_x), own_no), (norm_source(f), gn), (norm_w, wn), (norm_m, mn), (norm_v, vn))]

    def n_times(count):
        return fo_par.at[:, pl.ds(0, count * NORM[0] * NORM[1] // 8)]


    barrier = pltpu.get_barrier_semaphore()
    near = (peer_core, peer_x, peer_y)
    for peer in near:
        pl.semaphore_signal(barrier, inc=1, device_id=peer, device_id_type=MESH)
    zero = Chunk("embed", 0)
    ahead = pltpu.make_async_copy(zero.source(grads, f_diag), pre, pre_sem)
    ahead.start()
    for copy in own_loads(0, zero):
        copy.start()
    for copy in f_give + f_local:
        copy.start()
    acc[...] = jnp.zeros_like(acc)
    acc_first[...] = jnp.zeros_like(acc_first)

    take(f_held, f_sem.at[0])
    pl.semaphore_wait(barrier, len(near))
    f_push[0].start()
    ahead.wait()
    push_other(0, zero, pre).start()
    f_push[1].start()
    start(f_push[2:])
    push_mine(0, zero, zero.source(grads, f_core)).start()
    for k in range(1, FETCH - LEAD + 1):
        fetch(k)
    take(f_held, f_sem.at[1])
    take(fo_par.at[:, give_o], f_sem.at[3])
    fo_own[:, give_o] = fo_own[:, give_o] + fo_par[:, give_o]
    f_scatter[0].start()
    sum_chip(0)
    start_x(0)
    take(fo_par.at[:, give_o], f_sem.at[4])
    gd[last, give] = gd[last, give] + pmd[last, give]
    f_scatter[1].start()
    take(fo_par, f_sem.at[5])
    take(f_held, f_sem.at[2])
    fo_own[:, keep_o] = fo_own[:, keep_o] + fo_par[:, keep_o]
    gd[last, keep] = gd[last, keep] + pmd[last, keep]
    start(f_state)

    def step(t, _):
        i = t - FETCH
        fetch(i + FETCH)

        @pl.when(i == 0)
        def _():
            n_push_other.start()
            n_push_mine.start()
            for copy in n_local:
                copy.start()

        sum_x(i)
        sum_chip(i + LEAD)
        start_y(i)
        start_x(i + LEAD)

        @pl.when(i == 3)
        def _():
            take(n_times(7), n_sem.at[0])
            take(n_times(2), n_sem.at[1])
            own_no[...] = own_no[...] + par_no[...]
            n_x.start()

        @pl.when(i == 10)
        def _():
            take(n_times(2), n_sem.at[2])
            gn[...] = (gn[...] + pmn[...]) + xn[...]
            n_y.start()
            take(f_held, f_sem.at[6])
            fo_own[:, keep_o] = fo_own[:, keep_o] + f_y[...]
            gd[last, keep] = gd[last, keep] + yd[last, keep]

        @pl.when(i == 20)
        def _():
            take(n_times(2), n_sem.at[3])
            mean = (gn[...] + yn[...]) * 0.125
            gn[...] = mean
            square = mean * mean
            total = square[:, 0:128]
            for c in range(1, NORM[1] // 128):
                total = total + square[:, c * 128:(c + 1) * 128]
            acc[0:4, :] += total

        @pl.when(i == N - LEAD)
        def _():
            f_cross.start()

        @pl.when(jnp.logical_and(i == N, core == 0))
        def _():
            start(h_gather)

        @pl.when(i == N + LAG - 3)
        def _():
            take(fo_par, f_sem.at[7])
            mean = (gd[last, keep] + xd[last, keep]) * 0.125
            gd[last, keep] = mean
            sq_first[me] = jnp.sum(acc_first[...] + squares(mean, SPLIT), axis=0, keepdims=True)
            f_gather.start()
            start(sqf_copies)

        sum_y(i - LAG)
        return 0

    lax.fori_loop(FETCH - LEAD + 1, FETCH + N + LAG, step, 0)

    sq_all[f] = jnp.sum(acc[...], axis=0, keepdims=True)
    copies = [remote(sq_all.at[f], sq_all.at[f], sq_sem.at[2], sq_sem.at[3], peer)
              for peer in (peer_core, peer_x, peer_diag)]
    for copy in copies:
        copy.start()

    def drain(k, _):
        on_chunk(k, lambda chunk: retire(k, chunk))
        return 0

    lax.fori_loop(N - RING, N, drain, 0)
    for i, ref in enumerate((w7, m7, v7, wd, md, vd)):
        pltpu.make_async_copy(ref, ref, st_sem.at[i // 3]).wait()

    @pl.when(core == 0)
    def _():
        take(gd.at[pl.ds(0, 8), pl.ds(0, N_HALF * PIECE)], f_sem.at[9])
        for chunk in halves:
            gd[chunk.rows, chunk.half(1 - dp)] = yd[chunk.rows, chunk.half(1 - dp)]

    take(fo_par, f_sem.at[8])
    gd[last, give] = yd[last, give]
    take(sq_first.at[pl.ds(0, 7)], sq_sem.at[0])
    take(sq_first.at[pl.ds(0, 7)], sq_sem.at[1])
    total = sq_first[0]
    for i in range(1, 8):
        total = total + sq_first[i]
    take(sq_all.at[pl.ds(0, 3)], sq_sem.at[2])
    take(sq_all.at[pl.ds(0, 3)], sq_sem.at[3])
    sq_out[...] = ((sq_all[0] + sq_all[1]) + (sq_all[2] + sq_all[3])) + total


def update_math(avg_scale, sq_scale, g, w, m, v, decay):
    avg = ADAM_BETA1 * m + avg_scale * g
    root = sq_scale * g
    sq = ADAM_BETA2 * v + root * root
    dev = sq * lax.rsqrt(jnp.maximum(sq, SMALLEST))
    step_dir = avg / (dev + ADAM_EPS * ROOT_TWO)
    new = (1.0 - LEARN_RATE * decay) * w - (LEARN_RATE * ROOT_TWO / BIAS_ONE) * step_dir
    return new, avg, sq, new.astype(jnp.bfloat16)


def update_kernel(sq, g7, gd, gn, w7, m7, v7, wd, md, vd, wn, mn, vn,
                  lw, lm, lv, lb, dw, dm, dv, db, nw, nm, nv, nb, ew, em, ev, eb,
                  s7w, s7m, s7v, s7b, sdw, sdm, sdv, sdb, snw, snm, snv, snb, sem):
    total = jnp.sum(sq[...], keepdims=True)
    clip = jnp.minimum(1.0, 1.0 / (jnp.sqrt(total) + CLIP_EPS))
    scales = ((1.0 - ADAM_BETA1) * clip, math.sqrt(1.0 - ADAM_BETA2) * clip)

    outs = ((lw, lm, lv, lb), (dw, dm, dv, db), (nw, nm, nv, nb), (ew, em, ev, eb))
    seven_staged = (s7w, s7m, s7v, s7b)
    down_staged = (sdw, sdm, sdv, sdb)

    def layer_copies(j, row, rows):
        at = pl.ds(row, rows)
        return [pltpu.make_async_copy(src.at[j, at, :], dst.at[j, at, :], sem.at[0, a // 3])
                for a, (src, dst) in enumerate(zip(seven_staged, outs[0]))]

    def embed_copies():
        return [pltpu.make_async_copy(src.at[6], dst, sem.at[1, a // 3])
                for a, (src, dst) in enumerate(zip(seven_staged, outs[3]))]

    def down_copies(t):
        at = pl.ds(pl.multiple_of(t * 16, 16), 16)
        return [pltpu.make_async_copy(src.at[at, :], dst.at[at, :], sem.at[2, a // 3])
                for a, (src, dst) in enumerate(zip(down_staged, outs[1]))]

    def seven(j, row, decay):
        for c in range(0, WIDTH, 512):
            ix = (j, pl.ds(row, 16), pl.ds(c, 512))
            out = update_math(*scales, g7[ix], w7[ix], m7[ix], v7[ix], decay)
            for ref, val in zip(seven_staged, out):
                ref[ix] = val

    def block(j, decay):
        def rows(t, _):
            seven(j, pl.multiple_of(t * 16, 16), decay)
            return 0

        lax.fori_loop(0, 4, rows, 0)

    def first_step(t, _):
        row = pl.multiple_of(t * 16, 16)
        seven(0, row, WEIGHT_DECAY)
        start(layer_copies(0, row, 16))
        return 0

    def half_step(t, _):
        seven(1, pl.multiple_of(t * 32, 32), WEIGHT_DECAY)
        seven(1, pl.multiple_of(t * 32 + 16, 16), WEIGHT_DECAY)
        start(layer_copies(1, pl.multiple_of(t * 32, 32), 32))
        return 0

    def layer_step(j, _):
        block(j, WEIGHT_DECAY)
        start(layer_copies(j, 0, ROWS))
        return 0

    def down_step(t, _):
        row = pl.multiple_of(t * 16, 16)

        def cols(u, _):
            ix = (pl.ds(row, 16), pl.ds(pl.multiple_of(u * 1024, 1024), 1024))
            out = update_math(*scales, gd[ix], wd[ix], md[ix], vd[ix], WEIGHT_DECAY)
            for ref, val in zip(down_staged, out):
                ref[ix] = val
            return 0

        lax.fori_loop(0, FF // 1024, cols, 0)
        start(down_copies(t))
        return 0

    lax.fori_loop(0, 4, first_step, 0)
    lax.fori_loop(1, 6, layer_step, 0)
    out = update_math(*scales, gn[...], wn[...], mn[...], vn[...], WEIGHT_DECAY)
    for ref, val in zip((snw, snm, snv, snb), out):
        ref[...] = val
    norm_copies = [pltpu.make_async_copy(src, dst, sem.at[3, a // 3])
                   for a, (src, dst) in enumerate(zip((snw, snm, snv, snb), outs[2]))]
    start(norm_copies)
    block(6, 0.0)
    start(embed_copies())
    lax.fori_loop(0, 4, down_step, 0)

    for a, staged in enumerate(seven_staged):
        pltpu.make_async_copy(staged.at[pl.ds(0, 6)], outs[0][a], sem.at[0, a // 3]).wait()
    wait(embed_copies())
    wait(norm_copies)
    for a, staged in enumerate(down_staged):
        pltpu.make_async_copy(staged, outs[1][a], sem.at[2, a // 3]).wait()


def local_update(g_layer, g_down, g_norm, g_embed, layer_w, layer_m, layer_v, down_w, down_m, down_v, norm_w, norm_m,
                 norm_v, embed_w, embed_m, embed_v):
    any_spec = pl.BlockSpec(memory_space=pl.ANY)
    vmem_spec = pl.BlockSpec(memory_space=pltpu.VMEM)
    dma = pltpu.SemaphoreType.DMA
    held = [(1, 128)] + [SEVEN, DOWN, NORM] + [SEVEN] * 3 + [DOWN] * 3 + [NORM] * 3
    reduced = pl.pallas_call(
        reduce_kernel,
        out_shape=[pltpu.VMEM(shape, F32) for shape in held],
        in_specs=[any_spec] * 16,
        out_specs=[vmem_spec] * len(held),
        scratch_shapes=[pltpu.VMEM((RING, 8, max(PART, PIECE)), F32)] * 2
        + [pltpu.VMEM(SEVEN, F32), pltpu.VMEM(DOWN, F32)] * 3
        + [pltpu.VMEM(NORM, F32)] * 5
        + [pltpu.VMEM((8, 128), F32)] * 2 + [pltpu.VMEM((4, 1, 128), F32), pltpu.VMEM((8, 1, 128), F32)]
        + [pltpu.VMEM((8, PART), F32)] + [pltpu.VMEM((FIRST, FIRST_COLS), F32)] * 2
        + [pltpu.VMEM((2, FIRST, FIRST_COLS), F32), pltpu.VMEM((FIRST, SPLIT), F32)]
        + [dma((RING,)), dma((RING,)), dma((M_RING,)), dma((Y_RING,)), dma((2,)), dma((4,)), dma((4,)), dma((10,)), dma,
           pltpu.SemaphoreType.REGULAR],
        compiler_params=pltpu.CompilerParams(collective_id=0, has_side_effects=True,
                                             vmem_limit_bytes=26 * 1024 * 1024),
    )(g_layer, g_down, g_norm, g_embed, layer_w, layer_m, layer_v, down_w, down_m, down_v, norm_w, norm_m, norm_v,
      embed_w, embed_m, embed_v)
    groups = ((6, ROWS, WIDTH), DOWN, NORM, (ROWS, WIDTH))
    out_shape = [jax.ShapeDtypeStruct(s, d) for s in groups for d in (F32, F32, F32, jnp.bfloat16)]
    staged = [pltpu.VMEM(s, d) for s in (SEVEN, DOWN, NORM) for d in (F32, F32, F32, jnp.bfloat16)]
    return pl.pallas_call(
        update_kernel,
        out_shape=out_shape,
        in_specs=[vmem_spec] * len(held),
        out_specs=[any_spec] * 16,
        scratch_shapes=staged + [dma((4, 2))],
        compiler_params=pltpu.CompilerParams(vmem_limit_bytes=26 * 1024 * 1024),
    )(*[pltpu.with_memory_space_constraint(a, pltpu.VMEM) for a in reduced])


def solution(mesh):
    grad_four = P(("dp", "fsdp"), None, None, None)
    grad_three = P(("dp", "fsdp"), None, None)
    layer_spec = P(None, "fsdp", None)
    down_spec = P("fsdp", None)
    norm_spec = P(None, "fsdp")
    embed_spec = P("fsdp", None)
    in_specs = (grad_four, grad_three, grad_three, grad_three,
                layer_spec, layer_spec, layer_spec, down_spec, down_spec, down_spec,
                norm_spec, norm_spec, norm_spec, embed_spec, embed_spec, embed_spec)
    out_specs = (layer_spec,) * 4 + (down_spec,) * 4 + (norm_spec,) * 4 + (embed_spec,) * 4
    return jax.shard_map(local_update, mesh=mesh, in_specs=in_specs, out_specs=out_specs, check_vma=False)
```

```python
import math

import jax
import jax.numpy as jnp
from jax import lax
from jax.experimental import pallas as pl
from jax.experimental.pallas import tpu as pltpu
from jax.sharding import PartitionSpec as P

ADAM_BETA1 = 0.9
ADAM_BETA2 = 0.95
ADAM_EPS = 1e-8
LEARN_RATE = 4e-4
WEIGHT_DECAY = 0.1
CLIP_EPS = 1e-6
OPT_STEP = 20
BIAS_ONE = 1.0 - ADAM_BETA1 ** OPT_STEP
BIAS_TWO = 1.0 - ADAM_BETA2 ** OPT_STEP
ROOT_TWO = math.sqrt(BIAS_TWO)
SMALLEST = 1.1754944e-38

MESH = pl.DeviceIdType.MESH
F32 = jnp.float32

ROWS = 64
WIDTH = 3072
FF = 8192
PIECE = 1024
NORM = (4, 768)
SEVEN = (7, ROWS, WIDTH)
DOWN = (ROWS, FF)

FIRST = 8
FIRST_COLS = 5120
SPLIT = FIRST_COLS // 2
PART = 1536
BLOCK = (ROWS // 8) * (WIDTH // PART)
N_EMBED = BLOCK
N_LAYER = N_EMBED + 6 * BLOCK
N_HALF = 3
N = N_LAYER + (FF // PIECE) * (ROWS // 8) - FIRST_COLS // PIECE

LEAD = 5
FETCH = 7
RING = 8
LAG = 5
Y_RING = 2 * LAG + 2
M_RING = RING + LEAD


class Chunk:
    def __init__(self, kind, k):
        self.kind = kind
        if kind in ("half", "down"):
            q = k - N_LAYER
            per = FF // PIECE
            self.width = PIECE
        else:
            q = k if kind == "embed" else (k - N_EMBED) % BLOCK
            per = WIDTH // PART
            self.width = PART
            self.j = 6 if kind == "embed" else (k - N_EMBED) // BLOCK
        self.row = pl.multiple_of((q // per) * 8, 8)
        self.rows = pl.ds(self.row, 8)
        self.col = (q % per) * self.width
        self.cols = pl.ds(pl.multiple_of(self.col, 512), self.width)

    def half(self, dp):
        half = self.width // 2
        return pl.ds(pl.multiple_of(self.col + dp * half, 512), half)

    def source(self, grads, q):
        g_layer, g_down, g_embed = grads
        rows = pl.ds(pl.multiple_of(q * ROWS + self.row, 8), 8)
        if self.kind == "embed":
            return g_embed.at[0, rows, self.cols]
        if self.kind == "layer":
            return g_layer.at[0, self.j, rows, self.cols]
        return g_down.at[0, rows, self.cols]

    def state(self, layer, down, embed):
        if self.kind == "embed":
            return embed.at[self.rows, self.cols]
        if self.kind == "layer":
            return layer.at[self.j, self.rows, self.cols]
        return down.at[self.rows, self.cols]

    def held(self, seven, down):
        if self.kind in ("half", "down"):
            return down.at[self.rows, self.cols]
        return seven.at[self.j, self.rows, self.cols]

    def ring(self, ring, s):
        return ring.at[s, :, pl.ds(0, self.width)]


def on_chunk(k, use):
    if isinstance(k, int):
        use(Chunk("embed", k))
        return
    bounds = (0, N_EMBED, N_LAYER, N_LAYER + N_HALF, N)
    for i, kind in enumerate(("embed", "layer", "half", "down")):
        @pl.when(jnp.logical_and(k >= bounds[i], k < bounds[i + 1]))
        def _():
            use(Chunk(kind, k))


def start(copies):
    for copy in copies:
        copy.start()


def wait(copies):
    for copy in copies:
        copy.wait()


def take(ref, sem):
    pltpu.make_async_copy(ref, ref, sem).wait()


def squares(mean, width):
    parts = [mean[r:r + 8, i * 128:(i + 1) * 128] for r in range(0, mean.shape[0], 8) for i in range(width // 128)]
    sums = [p * p for p in parts[:4]]
    for i, p in enumerate(parts[4:]):
        sums[i % 4] = sums[i % 4] + p * p
    return (sums[0] + sums[1]) + (sums[2] + sums[3])


def reduce_kernel(g_layer, g_down, g_norm, g_embed, layer_w, layer_m, layer_v, down_w, down_m, down_v,
                  norm_w, norm_m, norm_v, embed_w, embed_m, embed_v,
                  sq_out, g7, gd, gn, w7, m7, v7, wd, md, vd, wn, mn, vn,
                  own_o, par_o, pm7, pmd, x7, xd, y7, yd, own_no, par_no, pmn, xn, yn, acc, acc_first, sq_all, sq_first,
                  pre, fo_own, fo_par, f_held, f_y,
                  out_sem, other_sem, mine_sem, y_sem, st_sem, n_sem, sq_sem, f_sem, pre_sem, credit):
    dp = lax.axis_index("dp")
    f = lax.axis_index("fsdp")
    core = lax.rem(f, 2)
    f_core = f + 1 - 2 * core
    f_x = lax.rem(f + 2, 4)
    f_diag = lax.rem(f_core + 2, 4)
    peer_core = (dp, f_core)
    peer_x = (dp, f_x)
    peer_diag = (dp, f_diag)
    peer_y = (1 - dp, f)
    peers = (peer_core, peer_x, peer_diag, peer_y, (1 - dp, f_core), (1 - dp, f_x), (1 - dp, f_diag))

    def remote(src, dst, send, recv, peer):
        return pltpu.make_async_remote_copy(src_ref=src, dst_ref=dst, send_sem=send, recv_sem=recv,
                                            device_id=peer, device_id_type=MESH)

    grads = (g_layer, g_down, g_embed)

    def x_copy(k, chunk):
        s = lax.rem(k, RING)
        return remote(chunk.ring(own_o, s), chunk.held(x7, xd), out_sem.at[s], mine_sem.at[lax.rem(k, M_RING)], peer_x)

    def y_copy(k, chunk):
        sem = y_sem.at[lax.rem(k, Y_RING)]
        return remote(chunk.held(g7, gd), chunk.held(y7, yd), sem, sem, peer_y)

    def half_copy(k, chunk):
        sem = y_sem.at[lax.rem(k, Y_RING)]
        give = chunk.half(1 - dp)
        return remote(gd.at[chunk.rows, give], yd.at[chunk.rows, give], sem, sem, peer_y)

    def by_core(chunk, on_whole, on_half):
        if chunk.kind == "half":
            pl.when(core == 0)(on_half)
            pl.when(core == 1)(on_whole)
        else:
            on_whole()

    def push_other(k, chunk, source):
        s = lax.rem(k, RING)
        return remote(source, chunk.ring(par_o, s), out_sem.at[s], other_sem.at[s], peer_core)

    def push_mine(k, chunk, source):
        s = lax.rem(k, RING)
        return remote(source, chunk.held(pm7, pmd), out_sem.at[s], mine_sem.at[lax.rem(k, M_RING)], peer_core)

    def own_loads(k, chunk):
        s = lax.rem(k, RING)
        return [pltpu.make_async_copy(chunk.source(grads, f_x), chunk.ring(own_o, s), other_sem.at[s]),
                pltpu.make_async_copy(chunk.source(grads, f), chunk.held(g7, gd), mine_sem.at[lax.rem(k, M_RING)])]

    def times(count, chunk):
        return own_o.at[pl.ds(0, count), :, pl.ds(0, chunk.width)]

    def retire(k, chunk):
        take(times(3, chunk), out_sem.at[lax.rem(k, RING)])

    def fetch(k):
        @pl.when(jnp.logical_and(k >= RING, k < N))
        def _():
            on_chunk(k - RING, lambda chunk: retire(k - RING, chunk))
            pl.semaphore_wait(credit, 1)

        def begin(chunk):
            push_other(k, chunk, chunk.source(grads, f_diag)).start()
            for copy in own_loads(k, chunk):
                copy.start()
            push_mine(k, chunk, chunk.source(grads, f_core)).start()

        on_chunk(k, begin)

    def sum_x(k):
        def use(chunk):
            take(times(3, chunk), mine_sem.at[lax.rem(k, M_RING)])
            mine = chunk.held(g7, gd)
            theirs = chunk.held(pm7, pmd)
            mine[...] = (mine[...] + theirs[...]) + chunk.held(x7, xd)[...]

        on_chunk(k, use)

    def sum_chip(k):
        s = lax.rem(k, RING)

        def use(chunk):
            mine = chunk.ring(own_o, s)
            theirs = chunk.ring(par_o, s)
            take(times(2, chunk), other_sem.at[s])
            mine[...] = mine[...] + theirs[...]

        on_chunk(k, use)

    def start_x(k):
        on_chunk(k, lambda chunk: x_copy(k, chunk).start())

        @pl.when(jnp.logical_and(k >= 0, k < N - RING))
        def _():
            pl.semaphore_signal(credit, inc=1, device_id=peer_core, device_id_type=MESH)

    def start_y(k):
        def use(chunk):
            by_core(chunk, lambda: y_copy(k, chunk).start(), lambda: half_copy(k, chunk).start())
            seven = chunk.kind in ("embed", "layer")
            for i, (src, dst) in enumerate((((layer_w, down_w, embed_w), (w7, wd)), ((layer_m, down_m, embed_m), (m7, md)),
                                            ((layer_v, down_v, embed_v), (v7, vd)))):
                pltpu.make_async_copy(chunk.state(*src), chunk.held(*dst), st_sem.at[0 if seven else 1]).start()

        on_chunk(k, use)

    def sum_y(k):
        def use(chunk):
            sem = y_sem.at[lax.rem(k, Y_RING)]

            def whole():
                take(times(2, chunk), sem)
                mine = chunk.held(g7, gd)
                mean = (mine[...] + chunk.held(y7, yd)[...]) * 0.125
                mine[...] = mean
                acc[...] += squares(mean, chunk.width)

            def half():
                take(times(1, chunk), sem)
                keep = chunk.half(dp)
                mean = (gd[chunk.rows, keep] + yd[chunk.rows, keep]) * 0.125
                gd[chunk.rows, keep] = mean
                acc_first[...] += squares(mean, chunk.width // 2)

            by_core(chunk, whole, half)

        on_chunk(k, use)

    last = pl.ds(ROWS - FIRST, FIRST)
    keep = pl.ds(pl.multiple_of(FF - FIRST_COLS + dp * SPLIT, PIECE // 2), SPLIT)
    give = pl.ds(pl.multiple_of(FF - FIRST_COLS + (1 - dp) * SPLIT, PIECE // 2), SPLIT)
    cols = pl.ds(FF - FIRST_COLS, FIRST_COLS)
    keep_o = pl.ds(pl.multiple_of(dp * SPLIT, PIECE // 2), SPLIT)
    give_o = pl.ds(pl.multiple_of((1 - dp) * SPLIT, PIECE // 2), SPLIT)

    def first_rows(q):
        return g_down.at[0, pl.ds(pl.multiple_of(q * ROWS + (ROWS - FIRST), 8), FIRST), cols]

    f_own = gd.at[last, cols]
    f_give = [pltpu.make_async_copy(first_rows(q), f_held.at[i], f_sem.at[0]) for i, q in enumerate((f_diag, f_core))]
    f_local = [pltpu.make_async_copy(first_rows(f_x), fo_own, f_sem.at[1]),
               pltpu.make_async_copy(first_rows(f), f_own, f_sem.at[1])]
    f_push = []
    for h, (half, half_o) in enumerate(((give, give_o), (keep, keep_o))):
        for i, ref in enumerate((fo_par.at[:, half_o], pmd.at[last, half])):
            f_push.append(remote(f_held.at[i, :, half_o], ref, f_sem.at[2],
                                 f_sem.at[3 + i] if h == 0 else f_sem.at[5], peer_core))
    f_state = [pltpu.make_async_copy(src.at[last, cols], dst.at[last, cols], st_sem.at[1])
               for i, (src, dst) in enumerate(((down_w, wd), (down_m, md), (down_v, vd)))]
    f_scatter = [remote(fo_own.at[:, give_o], f_y, f_sem.at[6], f_sem.at[6], peer_y),
                 remote(gd.at[last, give], yd.at[last, give], f_sem.at[6], f_sem.at[6], peer_y)]
    f_cross = remote(fo_own.at[:, keep_o], xd.at[last, keep], f_sem.at[7], f_sem.at[7], peer_x)
    f_gather = remote(gd.at[last, keep], yd.at[last, keep], f_sem.at[8], f_sem.at[8], peer_y)
    halves = [Chunk("half", N_LAYER + i) for i in range(N_HALF)]
    h_gather = [remote(gd.at[chunk.rows, chunk.half(dp)], yd.at[chunk.rows, chunk.half(dp)], f_sem.at[9], f_sem.at[9],
                       peer_y) for chunk in halves]
    me = dp * 4 + f
    sqf_copies = [remote(sq_first.at[me], sq_first.at[me], sq_sem.at[0], sq_sem.at[1], peer)
                  for peer in peers]

    def norm_source(q):
        return g_norm.at[0, :, pl.ds(pl.multiple_of(q * NORM[1], 128), NORM[1])]

    n_push_other = remote(norm_source(f_diag), par_no, n_sem.at[1], n_sem.at[0], peer_core)
    n_push_mine = remote(norm_source(f_core), pmn, n_sem.at[1], n_sem.at[0], peer_core)
    n_x = remote(own_no, xn, n_sem.at[2], n_sem.at[2], peer_x)
    n_y = remote(gn, yn, n_sem.at[3], n_sem.at[3], peer_y)
    n_local = [pltpu.make_async_copy(src, dst, n_sem.at[0]) for src, dst in
               ((norm_source(f_x), own_no), (norm_source(f), gn), (norm_w, wn), (norm_m, mn), (norm_v, vn))]

    def n_times(count):
        return fo_par.at[:, pl.ds(0, count * NORM[0] * NORM[1] // 8)]


    barrier = pltpu.get_barrier_semaphore()
    near = (peer_core, peer_x, peer_y)
    for peer in near:
        pl.semaphore_signal(barrier, inc=1, device_id=peer, device_id_type=MESH)
    zero = Chunk("embed", 0)
    ahead = pltpu.make_async_copy(zero.source(grads, f_diag), pre, pre_sem)
    ahead.start()
    for copy in own_loads(0, zero):
        copy.start()
    for copy in f_give + f_local:
        copy.start()
    acc[...] = jnp.zeros_like(acc)
    acc_first[...] = jnp.zeros_like(acc_first)

    take(f_held, f_sem.at[0])
    pl.semaphore_wait(barrier, len(near))
    f_push[0].start()
    ahead.wait()
    push_other(0, zero, pre).start()
    f_push[1].start()
    start(f_push[2:])
    push_mine(0, zero, zero.source(grads, f_core)).start()
    for k in range(1, FETCH - LEAD + 1):
        fetch(k)
    take(f_held, f_sem.at[1])
    take(fo_par.at[:, give_o], f_sem.at[3])
    fo_own[:, give_o] = fo_own[:, give_o] + fo_par[:, give_o]
    f_scatter[0].start()
    sum_chip(0)
    start_x(0)
    take(fo_par.at[:, give_o], f_sem.at[4])
    gd[last, give] = gd[last, give] + pmd[last, give]
    f_scatter[1].start()
    take(fo_par, f_sem.at[5])
    take(f_held, f_sem.at[2])
    fo_own[:, keep_o] = fo_own[:, keep_o] + fo_par[:, keep_o]
    gd[last, keep] = gd[last, keep] + pmd[last, keep]
    start(f_state)

    def step(t, _):
        i = t - FETCH
        fetch(i + FETCH)

        @pl.when(i == 0)
        def _():
            n_push_other.start()
            n_push_mine.start()
            for copy in n_local:
                copy.start()

        sum_x(i)
        sum_chip(i + LEAD)
        start_y(i)
        start_x(i + LEAD)

        @pl.when(i == 3)
        def _():
            take(n_times(7), n_sem.at[0])
            take(n_times(2), n_sem.at[1])
            own_no[...] = own_no[...] + par_no[...]
            n_x.start()

        @pl.when(i == 10)
        def _():
            take(n_times(2), n_sem.at[2])
            gn[...] = (gn[...] + pmn[...]) + xn[...]
            n_y.start()
            take(f_held, f_sem.at[6])
            fo_own[:, keep_o] = fo_own[:, keep_o] + f_y[...]
            gd[last, keep] = gd[last, keep] + yd[last, keep]

        @pl.when(i == 20)
        def _():
            take(n_times(2), n_sem.at[3])
            mean = (gn[...] + yn[...]) * 0.125
            gn[...] = mean
            square = mean * mean
            total = square[:, 0:128]
            for c in range(1, NORM[1] // 128):
                total = total + square[:, c * 128:(c + 1) * 128]
            acc[0:4, :] += total

        @pl.when(i == N - LEAD)
        def _():
            f_cross.start()

        @pl.when(jnp.logical_and(i == N, core == 0))
        def _():
            start(h_gather)

        @pl.when(i == N + LAG - 3)
        def _():
            take(fo_par, f_sem.at[7])
            mean = (gd[last, keep] + xd[last, keep]) * 0.125
            gd[last, keep] = mean
            sq_first[me] = jnp.sum(acc_first[...] + squares(mean, SPLIT), axis=0, keepdims=True)
            f_gather.start()
            start(sqf_copies)

        sum_y(i - LAG)
        return 0

    lax.fori_loop(FETCH - LEAD + 1, FETCH + N + LAG, step, 0)

    sq_all[f] = jnp.sum(acc[...], axis=0, keepdims=True)
    copies = [remote(sq_all.at[f], sq_all.at[f], sq_sem.at[2], sq_sem.at[3], peer)
              for peer in (peer_core, peer_x, peer_diag)]
    for copy in copies:
        copy.start()

    def drain(k, _):
        on_chunk(k, lambda chunk: retire(k, chunk))
        return 0

    lax.fori_loop(N - RING, N, drain, 0)
    for i, ref in enumerate((w7, m7, v7, wd, md, vd)):
        pltpu.make_async_copy(ref, ref, st_sem.at[i // 3]).wait()

    @pl.when(core == 0)
    def _():
        take(gd.at[pl.ds(0, 8), pl.ds(0, N_HALF * PIECE)], f_sem.at[9])
        for chunk in halves:
            gd[chunk.rows, chunk.half(1 - dp)] = yd[chunk.rows, chunk.half(1 - dp)]

    take(fo_par, f_sem.at[8])
    gd[last, give] = yd[last, give]
    take(sq_first.at[pl.ds(0, 7)], sq_sem.at[0])
    take(sq_first.at[pl.ds(0, 7)], sq_sem.at[1])
    total = sq_first[0]
    for i in range(1, 8):
        total = total + sq_first[i]
    take(sq_all.at[pl.ds(0, 3)], sq_sem.at[2])
    take(sq_all.at[pl.ds(0, 3)], sq_sem.at[3])
    sq_out[...] = ((sq_all[0] + sq_all[1]) + (sq_all[2] + sq_all[3])) + total


def update_math(avg_scale, sq_scale, g, w, m, v, decay):
    avg = ADAM_BETA1 * m + avg_scale * g
    root = sq_scale * g
    sq = ADAM_BETA2 * v + root * root
    dev = sq * lax.rsqrt(jnp.maximum(sq, SMALLEST))
    step_dir = avg / (dev + ADAM_EPS * ROOT_TWO)
    new = (1.0 - LEARN_RATE * decay) * w - (LEARN_RATE * ROOT_TWO / BIAS_ONE) * step_dir
    return new, avg, sq, new.astype(jnp.bfloat16)


def update_kernel(sq, g7, gd, gn, w7, m7, v7, wd, md, vd, wn, mn, vn,
                  lw, lm, lv, lb, dw, dm, dv, db, nw, nm, nv, nb, ew, em, ev, eb,
                  s7w, s7m, s7v, s7b, sdw, sdm, sdv, sdb, snw, snm, snv, snb, sem):
    total = jnp.sum(sq[...], keepdims=True)
    clip = jnp.minimum(1.0, 1.0 / (jnp.sqrt(total) + CLIP_EPS))
    scales = ((1.0 - ADAM_BETA1) * clip, math.sqrt(1.0 - ADAM_BETA2) * clip)

    outs = ((lw, lm, lv, lb), (dw, dm, dv, db), (nw, nm, nv, nb), (ew, em, ev, eb))
    seven_staged = (s7w, s7m, s7v, s7b)
    down_staged = (sdw, sdm, sdv, sdb)

    def layer_copies(j, row, rows):
        at = pl.ds(row, rows)
        return [pltpu.make_async_copy(src.at[j, at, :], dst.at[j, at, :], sem.at[0])
                for a, (src, dst) in enumerate(zip(seven_staged, outs[0]))]

    def embed_copies():
        return [pltpu.make_async_copy(src.at[6], dst, sem.at[0])
                for a, (src, dst) in enumerate(zip(seven_staged, outs[3]))]

    def down_copies(t):
        at = pl.ds(pl.multiple_of(t * 16, 16), 16)
        return [pltpu.make_async_copy(src.at[at, :], dst.at[at, :], sem.at[0])
                for a, (src, dst) in enumerate(zip(down_staged, outs[1]))]

    def seven(j, row, decay):
        for c in range(0, WIDTH, 512):
            ix = (j, pl.ds(row, 16), pl.ds(c, 512))
            out = update_math(*scales, g7[ix], w7[ix], m7[ix], v7[ix], decay)
            for ref, val in zip(seven_staged, out):
                ref[ix] = val

    def block(j, decay):
        def rows(t, _):
            seven(j, pl.multiple_of(t * 16, 16), decay)
            return 0

        lax.fori_loop(0, 4, rows, 0)

    def first_step(t, _):
        row = pl.multiple_of(t * 16, 16)
        seven(0, row, WEIGHT_DECAY)
        start(layer_copies(0, row, 16))
        return 0

    def half_step(t, _):
        seven(1, pl.multiple_of(t * 32, 32), WEIGHT_DECAY)
        seven(1, pl.multiple_of(t * 32 + 16, 16), WEIGHT_DECAY)
        start(layer_copies(1, pl.multiple_of(t * 32, 32), 32))
        return 0

    def layer_step(j, _):
        block(j, WEIGHT_DECAY)
        start(layer_copies(j, 0, ROWS))
        return 0

    def down_step(t, _):
        row = pl.multiple_of(t * 16, 16)

        def cols(u, _):
            ix = (pl.ds(row, 16), pl.ds(pl.multiple_of(u * 1024, 1024), 1024))
            out = update_math(*scales, gd[ix], wd[ix], md[ix], vd[ix], WEIGHT_DECAY)
            for ref, val in zip(down_staged, out):
                ref[ix] = val
            return 0

        lax.fori_loop(0, FF // 1024, cols, 0)
        start(down_copies(t))
        return 0

    lax.fori_loop(0, 4, first_step, 0)
    lax.fori_loop(1, 6, layer_step, 0)
    out = update_math(*scales, gn[...], wn[...], mn[...], vn[...], WEIGHT_DECAY)
    for ref, val in zip((snw, snm, snv, snb), out):
        ref[...] = val
    norm_copies = [pltpu.make_async_copy(src, dst, sem.at[0])
                   for a, (src, dst) in enumerate(zip((snw, snm, snv, snb), outs[2]))]
    start(norm_copies)
    block(6, 0.0)
    start(embed_copies())
    lax.fori_loop(0, 4, down_step, 0)

    for a, staged in enumerate(seven_staged):
        pltpu.make_async_copy(staged.at[pl.ds(0, 6)], outs[0][a], sem.at[0]).wait()
    wait(embed_copies())
    wait(norm_copies)
    for a, staged in enumerate(down_staged):
        pltpu.make_async_copy(staged, outs[1][a], sem.at[0]).wait()


def local_update(g_layer, g_down, g_norm, g_embed, layer_w, layer_m, layer_v, down_w, down_m, down_v, norm_w, norm_m,
                 norm_v, embed_w, embed_m, embed_v):
    any_spec = pl.BlockSpec(memory_space=pl.ANY)
    vmem_spec = pl.BlockSpec(memory_space=pltpu.VMEM)
    dma = pltpu.SemaphoreType.DMA
    held = [(1, 128)] + [SEVEN, DOWN, NORM] + [SEVEN] * 3 + [DOWN] * 3 + [NORM] * 3
    reduced = pl.pallas_call(
        reduce_kernel,
        out_shape=[pltpu.VMEM(shape, F32) for shape in held],
        in_specs=[any_spec] * 16,
        out_specs=[vmem_spec] * len(held),
        scratch_shapes=[pltpu.VMEM((RING, 8, max(PART, PIECE)), F32)] * 2
        + [pltpu.VMEM(SEVEN, F32), pltpu.VMEM(DOWN, F32)] * 3
        + [pltpu.VMEM(NORM, F32)] * 5
        + [pltpu.VMEM((8, 128), F32)] * 2 + [pltpu.VMEM((4, 1, 128), F32), pltpu.VMEM((8, 1, 128), F32)]
        + [pltpu.VMEM((8, PART), F32)] + [pltpu.VMEM((FIRST, FIRST_COLS), F32)] * 2
        + [pltpu.VMEM((2, FIRST, FIRST_COLS), F32), pltpu.VMEM((FIRST, SPLIT), F32)]
        + [dma((RING,)), dma((RING,)), dma((M_RING,)), dma((Y_RING,)), dma((2,)), dma((4,)), dma((4,)), dma((10,)), dma,
           pltpu.SemaphoreType.REGULAR],
        compiler_params=pltpu.CompilerParams(collective_id=0, has_side_effects=True,
                                             vmem_limit_bytes=26 * 1024 * 1024),
    )(g_layer, g_down, g_norm, g_embed, layer_w, layer_m, layer_v, down_w, down_m, down_v, norm_w, norm_m, norm_v,
      embed_w, embed_m, embed_v)
    groups = ((6, ROWS, WIDTH), DOWN, NORM, (ROWS, WIDTH))
    out_shape = [jax.ShapeDtypeStruct(s, d) for s in groups for d in (F32, F32, F32, jnp.bfloat16)]
    staged = [pltpu.VMEM(s, d) for s in (SEVEN, DOWN, NORM) for d in (F32, F32, F32, jnp.bfloat16)]
    return pl.pallas_call(
        update_kernel,
        out_shape=out_shape,
        in_specs=[vmem_spec] * len(held),
        out_specs=[any_spec] * 16,
        scratch_shapes=staged + [dma((1,))],
        compiler_params=pltpu.CompilerParams(vmem_limit_bytes=26 * 1024 * 1024),
    )(*[pltpu.with_memory_space_constraint(a, pltpu.VMEM) for a in reduced])


def solution(mesh):
    grad_four = P(("dp", "fsdp"), None, None, None)
    grad_three = P(("dp", "fsdp"), None, None)
    layer_spec = P(None, "fsdp", None)
    down_spec = P("fsdp", None)
    norm_spec = P(None, "fsdp")
    embed_spec = P("fsdp", None)
    in_specs = (grad_four, grad_three, grad_three, grad_three,
                layer_spec, layer_spec, layer_spec, down_spec, down_spec, down_spec,
                norm_spec, norm_spec, norm_spec, embed_spec, embed_spec, embed_spec)
    out_specs = (layer_spec,) * 4 + (down_spec,) * 4 + (norm_spec,) * 4 + (embed_spec,) * 4
    return jax.shard_map(local_update, mesh=mesh, in_specs=in_specs, out_specs=out_specs, check_vma=False)
```
